32 devices in a mesh: gz: 16 (over z, y, x), xy: 2 (over core).
Axes of the slice: x: 2, y: 2, z: 4, core: 2. Of those that a mesh axis runs over, the one named last changes fastest.
Arguments:
- right_side: float32 [2, 16, 16, 2048], P(None, 'gz', 'xy')
- stiff_across: float32 [16, 16, 2048], P('gz', 'xy'), may hold values from 0.3 to 3
- stiff_down: float32 [16, 16, 2048], P('gz', 'xy'), may hold values from 0.3 to 3
- anchor: float32 [16, 16, 2048], P('gz', 'xy'), may hold values from 0.02 to 0.2
- source_node: int32 [16, 2, 1024], P('gz', 'xy'), may hold values from 0 to 16383
- target_cell: int32 [16, 2, 1024], P('gz', 'xy'), may hold values from 0 to 14334, as said below
- corner_weight: float32 [4, 16, 2, 1024], P(None, 'gz', 'xy'), may hold values from 0 to 1, as said below
- block_count: int32 [16, 2], P('gz', 'xy'), may hold values from 1 to 8, as said below
Outputs:
- solution_field: float32 [2, 16, 16, 2048], P(None, 'gz', 'xy')
- residual: float32 [2, 16, 16, 2048], P(None, 'gz', 'xy')
The draws below stay inside these ranges and needn't reach their ends.
Inputs may be any that keep to these rules, and one draw needn't show every extreme that they name: `target_cell`: each target cell's row is below 7 and its column below 2047 within the block, so all four corners lie in the same block. `corner_weight`: the weights of a slot are nonnegative and sum to 1. `block_count`: some device holds exactly 8 used blocks.
All inputs are finite; a program needn't handle non-finite values.
Results may differ from the reference program's by a relative error of at most 0.00013.
Values sent between devices are 32-bit elements; how exact they have to be, the bound alone decides.
No kernel may reach another device: no remote copies, remote signals or barrier semaphores. Data moves between devices by JAX's collectives and lax.ppermute only.
A program may use at most 64 MiB of HBM per device.

```python
import math
import jax
import jax.numpy as jnp

COLS = 2048
R_DEV = 8
BLOCK = 128
MAXB = 8
ITERS = 3
SECTIONS = 16
ROWS = 16
CORR = 1024
N_XY = 2


def draw_right_side(key, part):
    shape = (2, SECTIONS, R_DEV * N_XY, COLS)
    ramp = 1.0 + 2.0 * jnp.arange(SECTIONS, dtype=jnp.float32) / max(SECTIONS - 1, 1)
    values = jnp.clip(jax.random.normal(jax.random.fold_in(key, 12), shape, jnp.float32), -6.0, 6.0)
    values = values * ramp[None, :, None, None]
    return values.astype(jnp.float32)


def draw_target_cell(key, part):
    first, second = jax.random.split(jax.random.fold_in(key, 21))
    shape = (SECTIONS, N_XY, MAXB * BLOCK)
    row = jax.random.randint(first, shape, 0, R_DEV - 1)
    column = jax.random.randint(second, shape, 0, COLS - 1)
    return (row * COLS + column).astype(jnp.int32)


def draw_corner_weight(key, part):
    first, second = jax.random.split(jax.random.fold_in(key, 31))
    shape = (SECTIONS, N_XY, MAXB * BLOCK)
    across = jax.random.uniform(first, shape, jnp.float32)
    down = jax.random.uniform(second, shape, jnp.float32)
    return jnp.stack([(1.0 - across) * (1.0 - down), across * (1.0 - down), (1.0 - across) * down, across * down]).astype(jnp.float32)


def draw_block_count(key, part):
    first, second, third = jax.random.split(jax.random.fold_in(key, 41), 3)
    shape = (SECTIONS * N_XY,)
    one = jax.random.randint(first, shape, 0, MAXB)
    two = jax.random.randint(second, shape, 0, MAXB)
    counts = 1 + one * two // MAXB
    where = jax.random.randint(third, (), 0, SECTIONS * N_XY)
    counts = counts.at[where].set(MAXB)
    return counts.reshape(SECTIONS, N_XY).astype(jnp.int32)


def with_ends(values, key, smallest, largest):
    index_at = [jax.random.randint(jax.random.fold_in(key, axis), (), 0, length) for axis, length in enumerate(values.shape)]
    longest = values.shape.index(max(values.shape))
    neighbour = index_at[:longest] + [(index_at[longest] + 1) % values.shape[longest]] + index_at[longest + 1:]
    return values.at[tuple(index_at)].set(smallest).at[tuple(neighbour)].set(largest)


def block_scale(own_key, shape, pieces, low, high):
    def one(axis_at, shards_of):
        heights = jax.random.uniform(jax.random.fold_in(jax.random.fold_in(own_key, 6), axis_at), (shards_of,), jnp.float32, low / len(pieces), high / len(pieces))
        return jnp.repeat(jnp.exp(heights), shape[axis_at] // shards_of).reshape((-1,) + (1,) * (len(shape) - axis_at - 1))

    level = one(*pieces[0])
    for cut in pieces[1:]:
        level = level * one(*cut)
    return level


def setup_inputs(seed: int = 0) -> dict:
    key_of = jax.random.split(jax.random.key(seed), 9)
    right_side = draw_right_side(jax.random.fold_in(key_of[8], 71), 0)
    stiff_across = jnp.clip(jnp.exp(math.log(3.0) - 2.3025851 * jax.random.uniform(key_of[1], (SECTIONS, ROWS, COLS), jnp.float32) ** block_scale(key_of[1], (SECTIONS, ROWS, COLS), ((0, 16), (1, 2)), -0.2, 0.2)), 0.3, 3.0)
    stiff_down = jnp.clip(jnp.exp(math.log(3.0) - 2.3025851 * jax.random.uniform(key_of[2], (SECTIONS, ROWS, COLS), jnp.float32) ** block_scale(key_of[2], (SECTIONS, ROWS, COLS), ((0, 16), (1, 2)), -0.2, 0.2)), 0.3, 3.0)
    anchor = jnp.clip(jnp.exp(math.log(0.2) - 2.3025851 * jax.random.uniform(key_of[3], (SECTIONS, ROWS, COLS), jnp.float32) ** block_scale(key_of[3], (SECTIONS, ROWS, COLS), ((0, 16), (1, 2)), -0.2, 0.2)), 0.02, 0.2)
    source_node = with_ends(jax.random.randint(key_of[4], (SECTIONS, N_XY, CORR), 0, R_DEV * COLS), jax.random.fold_in(key_of[4], 1), 0, (R_DEV * COLS) - 1).astype(jnp.int32)
    target_cell = draw_target_cell(jax.random.fold_in(key_of[8], 71), 0)
    corner_weight = draw_corner_weight(jax.random.fold_in(key_of[8], 71), 0)
    block_count = draw_block_count(jax.random.fold_in(key_of[8], 71), 0)
    return {"right_side": right_side, "stiff_across": stiff_across, "stiff_down": stiff_down, "anchor": anchor, "source_node": source_node, "target_cell": target_cell, "corner_weight": corner_weight, "block_count": block_count}


def springs(field, across, down, hold):
    zero_col = jnp.zeros(field.shape[:-1] + (1,), field.dtype)
    zero_row = jnp.zeros(field.shape[:-2] + (1, field.shape[-1]), field.dtype)
    right = jnp.concatenate([field[..., 1:], zero_col], -1)
    left = jnp.concatenate([zero_col, field[..., :-1]], -1)
    lower = jnp.concatenate([field[..., 1:, :], zero_row], -2)
    upper = jnp.concatenate([zero_row, field[..., :-1, :]], -2)
    across_left = jnp.concatenate([jnp.zeros(across.shape[:-1] + (1,), across.dtype), across[..., :-1]], -1)
    down_above = jnp.concatenate([jnp.zeros(down.shape[:-2] + (1, down.shape[-1]), down.dtype), down[..., :-1, :]], -2)
    return (across * (field - right) + across_left * (field - left)
            + down * (field - lower) + down_above * (field - upper) + hold * field)


def reference(right_side, stiff_across, stiff_down, anchor, source_node, target_cell, corner_weight, block_count):
    block_size = R_DEV * COLS
    total = SECTIONS * N_XY * block_size
    base = ((jnp.arange(SECTIONS, dtype=jnp.int32)[:, None] * N_XY
             + jnp.arange(N_XY, dtype=jnp.int32)[None, :]) * block_size).astype(jnp.int32)
    source_all = (source_node + base[:, :, None]).reshape(-1).astype(jnp.int32)
    offsets = jnp.array([0, 1, COLS, COLS + 1], dtype=jnp.int32)
    corners_all = (target_cell[None] + offsets[:, None, None, None] + base[None, :, :, None]
                   + N_XY * block_size).astype(jnp.int32)
    corners_all = jnp.minimum(corners_all, total - 1).reshape(4, -1).astype(jnp.int32)
    weights = corner_weight.reshape(4, -1)
    slot = jnp.arange(CORR, dtype=jnp.int32)
    live = (slot[None, None, :] < block_count[:, :, None] * BLOCK) & (jnp.arange(SECTIONS, dtype=jnp.int32) < SECTIONS - 1)[:, None, None]
    live = live.reshape(-1).astype(right_side.dtype)

    def operate(field):
        flat = field.reshape(2, -1)
        interp = jnp.sum(weights[None] * flat[:, corners_all], 1)
        error = (interp - flat[:, source_all]) * live[None]
        result = jnp.zeros_like(flat).at[:, source_all].add(-error)
        result = result.at[:, corners_all.reshape(-1)].add((weights[None] * error[:, None, :]).reshape(2, -1))
        return springs(field, stiff_across, stiff_down, anchor) + result.reshape(field.shape)

    solution_field = jnp.zeros_like(right_side)
    residual, direction = right_side, right_side
    norm_now = jnp.sum(residual * residual)
    for step in range(ITERS):
        image = operate(direction)
        alpha = norm_now / jnp.sum(direction * image)
        solution_field = solution_field + alpha * direction
        residual = residual - alpha * image
        norm_next = jnp.sum(residual * residual)
        direction = residual + (norm_next / norm_now) * direction
        norm_now = norm_next
    return solution_field, residual
```

```python
import functools

import jax
import jax.numpy as jnp
from jax import lax
from jax.experimental import pallas as pl
from jax.experimental.pallas import tpu as pltpu
from jax.sharding import PartitionSpec as P

BLOCK = 128
ITERS = 3
LANES = 128
GAIN = 0.25
SHIFT = 1.25
F32 = jnp.float32
BF16 = jnp.bfloat16
CHUNK = 256


def swapped(block, axis, first):
    count = lax.axis_size(axis)
    route = []
    for i in range(first, count - 1, 2):
        route += [(i, i + 1), (i + 1, i)]
    return lax.ppermute(block, axis, route) if route else None


def split2(x):
    high = x.astype(BF16)
    return high, (x - high.astype(F32)).astype(BF16)


def div_mod(x, d):
    if d & (d - 1) == 0:
        return lax.shift_right_logical(x, jnp.int32(d.bit_length() - 1)), x & (d - 1)
    q = lax.div(x, jnp.int32(d))
    return q, x - q * d


def hi_lo(index, rows, cols):
    row, col = div_mod(index, cols)
    tile, lane = div_mod(col, LANES)
    return tile * rows + row, lane


def row_of(tile, k):
    return tile[k : k + 1, :]


def one_hot(lanes_of):
    nb = lanes_of.shape[0]
    at = lax.broadcasted_iota(jnp.int32, (LANES, LANES), 0)
    return jnp.concatenate(
        [jnp.where(at == row_of(lanes_of, k), 1.0, 0.0).astype(BF16) for k in range(nb)], axis=1
    )


def tall(field):
    n = field.shape[1] // LANES
    return jnp.concatenate([field[:, i * LANES : (i + 1) * LANES] for i in range(n)], axis=0)


def wide(stack, rows):
    n = stack.shape[0] // rows
    return jnp.concatenate([stack[i * rows : (i + 1) * rows, :] for i in range(n)], axis=1)


def operand(fields):
    out = []
    for f in fields:
        high, low = split2(tall(f))
        out.append(jnp.concatenate([high, low], axis=1))
    return jnp.concatenate(out, axis=0)


def right_of(field):
    return pltpu.roll(field, field.shape[1] - 1, 1)


def looked_up(field, slots_hi, hot2):
    high = tall(field[0]).shape[0]
    left = operand([field[0], field[1]])
    nb = slots_hi.shape[0]
    at = lax.broadcasted_iota(jnp.int32, (high, LANES), 0)
    found = ([], [])
    for k in range(nb):
        got = jnp.dot(left, hot2[:, k * LANES : (k + 1) * LANES], preferred_element_type=F32)
        mask = at == row_of(slots_hi, k)
        for c in range(2):
            found[c].append(
                jnp.sum(jnp.where(mask, got[c * high : (c + 1) * high], 0.0), axis=0, keepdims=True)
            )
    return jnp.stack([jnp.concatenate(f, axis=0) for f in found])


def interpolated(field, slots_hi, hot2, weights):
    high = tall(field[0]).shape[0]
    left = operand([field[0], field[1], right_of(field[0]), right_of(field[1])])
    nb = slots_hi.shape[0]
    at = lax.broadcasted_iota(jnp.int32, (high, LANES), 0)
    found = ([], [])
    for k in range(nb):
        got = jnp.dot(left, hot2[:, k * LANES : (k + 1) * LANES], preferred_element_type=F32)
        here = row_of(slots_hi, k)
        upper = at == here
        lower = at == here + 1
        w = [row_of(weights[q], k) for q in range(4)]
        wl = jnp.where(upper, w[0], jnp.where(lower, w[2], 0.0))
        wr = jnp.where(upper, w[1], jnp.where(lower, w[3], 0.0))
        for c in range(2):
            value = wl * got[c * high : (c + 1) * high] + wr * got[(2 + c) * high : (3 + c) * high]
            found[c].append(jnp.sum(value, axis=0, keepdims=True))
    return jnp.stack([jnp.concatenate(f, axis=0) for f in found])


NT = (((1,), (1,)), ((), ()))


def spread_own(values, slots_hi, hot, rows, high):
    nb = slots_hi.shape[0]
    at = lax.broadcasted_iota(jnp.int32, (high, LANES), 0)
    masks = [at == row_of(slots_hi, k) for k in range(nb)]
    parts = []
    for c in range(2):
        high_part = values[c].astype(BF16).astype(F32)
        for part in (high_part, values[c] - high_part):
            parts.append(
                jnp.concatenate(
                    [jnp.where(masks[k], row_of(part, k), 0.0).astype(BF16) for k in range(nb)], axis=1
                )
            )
    out = lax.dot_general(jnp.concatenate(parts, axis=0), hot, NT, preferred_element_type=F32)
    return [
        wide(out[2 * c * high : (2 * c + 1) * high] + out[(2 * c + 1) * high : (2 * c + 2) * high], rows)
        for c in range(2)
    ]


def spread_corners(values, weights, slots_hi, hot, rows, high):
    nb = slots_hi.shape[0]
    at = lax.broadcasted_iota(jnp.int32, (high, LANES), 0)
    upper = [at == row_of(slots_hi, k) for k in range(nb)]
    lower = [at == row_of(slots_hi, k) + 1 for k in range(nb)]
    parts = []
    for c in range(2):
        for side in range(2):
            up = values[c] * weights[side]
            down = values[c] * weights[2 + side]
            up_high = up.astype(BF16).astype(F32)
            down_high = down.astype(BF16).astype(F32)
            for a, b in ((up_high, down_high), (up - up_high, down - down_high)):
                parts.append(
                    jnp.concatenate(
                        [
                            jnp.where(
                                upper[k], row_of(a, k), jnp.where(lower[k], row_of(b, k), 0.0)
                            ).astype(BF16)
                            for k in range(nb)
                        ],
                        axis=1,
                    )
                )
    out = lax.dot_general(jnp.concatenate(parts, axis=0), hot, NT, preferred_element_type=F32)
    result = []
    for c in range(2):
        sides = []
        for side in range(2):
            p = (2 * c + side) * 2
            sides.append(wide(out[p * high : (p + 1) * high] + out[(p + 1) * high : (p + 2) * high], rows))
        result.append(sides[0] + pltpu.roll(sides[1], 1, 1))
    return result


def springs(field, across, down, hold, upper_row, lower_row, rim):
    rows, cols = field.shape
    col = lax.broadcasted_iota(jnp.int32, (rows, cols), 1)
    row = lax.broadcasted_iota(jnp.int32, (rows, cols), 0)
    right = jnp.where(col == cols - 1, 0.0, pltpu.roll(field, cols - 1, 1))
    pull = across * (field - right)
    out = pull - jnp.where(col == 0, 0.0, pltpu.roll(pull, 1, 1))
    lower = jnp.where(row == rows - 1, lower_row, pltpu.roll(field, rows - 1, 0))
    pull = down * (field - lower)
    above = rim * (upper_row - field[0:1, :])
    out = out + pull - jnp.where(row == 0, above, pltpu.roll(pull, 1, 0))
    return out + hold * field


def pick(flag, a, b):
    return jnp.where(flag, a, b)


def edges_of(get_row, rows, even_b, two):
    first = [get_row(c, 0) for c in range(2)]
    last = [get_row(c, rows - 1) for c in range(2)]
    out = [jnp.concatenate([pick(even_b, last[c], first[c]) for c in range(2)], axis=0)]
    if two:
        out.append(jnp.concatenate([pick(even_b, first[c], last[c]) for c in range(2)], axis=0))
    return out


def pack_kernel(two, flags, count, field, down, source, target, weights, pack, *edges):
    rows, cols = down.shape
    even_b = flags[1] == 0
    has_next = flags[2]
    nb = source.shape[0]
    block = lax.broadcasted_iota(jnp.int32, (nb, LANES), 0)
    live = jnp.where(block * LANES < count[0, 0] * BLOCK * has_next, 1.0, 0.0)
    for c in range(2):
        pack[:, c * cols : (c + 1) * cols] = field[c]
    parts = [source[...].astype(F32), target[...].astype(F32)] + [weights[q] * live for q in range(4)]
    for i, part in enumerate(parts):
        pack[:nb, 2 * cols + i * LANES : 2 * cols + (i + 1) * LANES] = part
    messages = edges_of(lambda c, r: field[c, r : r + 1, :], rows, even_b, two)
    for message, edge in zip(messages, edges):
        edge[0:2, :] = message
        edge[2:3, :] = down[rows - 1 : rows, :]


def halves(flags, edge_refs):
    even_b = flags[1] == 0
    zero = edge_refs[0][...]
    if len(edge_refs) == 2:
        other = edge_refs[1][...]
    else:
        other = jnp.zeros_like(zero)
    return pick(even_b, other, zero), pick(even_b, zero, other)


def advance(field, error, error_prev, own, prev, across, down, hold, above, below, rim):
    own_hi, own_hot = own
    prev_hi, prev_hot, prev_weights = prev
    rows, cols = field[0].shape
    high = rows * (cols // LANES)
    pulled = spread_own(error, own_hi, own_hot, rows, high)
    pushed = spread_corners(error_prev, prev_weights, prev_hi, prev_hot, rows, high)
    result = []
    for c in range(2):
        image = springs(field[c], across, down, hold, above[c : c + 1], below[c : c + 1], rim)
        image = image + (pushed[c] - pulled[c])
        result.append(GAIN * image - SHIFT * field[c])
    return result


def step_kernel(
    first, last, two, n_edges, flags, count, field_ref, across, down, hold, source, weights_or_prev, local, *rest
):
    rest = list(rest)
    take = lambda n: [rest.pop(0) for _ in range(n)]
    even = flags[0] == 0
    even_b = flags[1] == 0
    has_next = flags[2]
    nb = source.shape[0]
    rows, cols = across.shape
    block = lax.broadcasted_iota(jnp.int32, (nb, LANES), 0)
    live = jnp.where(block * LANES < count[0, 0] * BLOCK * has_next, 1.0, 0.0)
    field = [field_ref[0], field_ref[1]]
    own_hi, own_lo = hi_lo(source[...], rows, cols)
    own_hot = one_hot(own_lo)
    own_hot2 = jnp.concatenate([own_hot, own_hot], axis=0)
    got0, got1 = take(2)
    edge_refs = take(n_edges)
    above, below = halves(flags, edge_refs)
    if first:
        target = local
        rim = above[2:3, :]
        slot = lambda ref, i: ref[:nb, 2 * cols + i * LANES : 2 * cols + (i + 1) * LANES]
        prev_parts = [pick(even, slot(got1, i), slot(got0, i)) for i in range(6)]
        prev_target = prev_parts[1].astype(jnp.int32)
        prev_weights = prev_parts[2:]
        prev_hi, prev_lo = hi_lo(prev_target, rows, cols)
        prev_hot = one_hot(prev_lo)
        prev_hot2 = jnp.concatenate([prev_hot, prev_hot], axis=0)
        comp = lambda ref, c: ref[:, c * cols : (c + 1) * cols]
        next_field = [pick(even, comp(got0, c), comp(got1, c)) for c in range(2)]
        prev_field = [pick(even, comp(got1, c), comp(got0, c)) for c in range(2)]
        own = looked_up(field, own_hi, own_hot2)
        mid = interpolated(field, prev_hi, prev_hot2, prev_weights)
        t_hi, t_lo = hi_lo(target[...], rows, cols)
        t_hot = one_hot(t_lo)
        own_weights = [weights_or_prev[q] for q in range(4)]
        from_next = interpolated(next_field, t_hi, jnp.concatenate([t_hot, t_hot], axis=0), own_weights)
        p_hi, p_lo = hi_lo(prev_parts[0].astype(jnp.int32), rows, cols)
        p_hot = one_hot(p_lo)
        from_prev = looked_up(prev_field, p_hi, jnp.concatenate([p_hot, p_hot], axis=0))
    else:
        rim = rest.pop(0)[...]
        prev_ref = weights_or_prev
        prev_target = prev_ref[0].astype(jnp.int32)
        prev_weights = [prev_ref[1 + q] for q in range(4)]
        prev_hi, prev_lo = hi_lo(prev_target, rows, cols)
        prev_hot = one_hot(prev_lo)
        prev_hot2 = jnp.concatenate([prev_hot, prev_hot], axis=0)
        own, mid = local[0], local[1]
        from_next = pick(even, got0[...], got1[...])
        from_prev = pick(even, got1[...], got0[...])
    if last:
        earlier = take(2)
    error = [live * (from_next[c] - own[c]) for c in range(2)]
    error_prev = [mid[c] - from_prev[c] for c in range(2)]
    after = advance(
        field,
        error,
        error_prev,
        (own_hi, own_hot),
        (prev_hi, prev_hot, prev_weights),
        across[...],
        down[...],
        hold[...],
        above,
        below,
        rim,
    )
    out = rest.pop(0)
    for c in range(2):
        out[c] = after[c]
    if last:
        moments = rest.pop(0)
        basis = [[ref[0], ref[1]] for ref in earlier] + [field, after]
        lane = lax.broadcasted_iota(jnp.int32, (1, LANES), 1)
        total = jnp.zeros((1, LANES), F32)
        for i in range(2 * ITERS):
            u, w = basis[i // 2], basis[i - i // 2]
            s = u[0] * w[0] + u[1] * w[1]
            s = jnp.sum(jnp.sum(s, axis=0, keepdims=True), axis=1, keepdims=True)
            total = total + jnp.where(lane == i, s, 0.0)
        moments[...] = jnp.broadcast_to(total, moments.shape)
        return
    after_own = looked_up(after, own_hi, own_hot2)
    after_mid = interpolated(after, prev_hi, prev_hot2, prev_weights)
    local_out, send0, send1 = take(3)
    local_out[0] = after_own
    local_out[1] = after_mid
    send0[...] = pick(even, after_own, after_mid)
    send1[...] = pick(even, after_mid, after_own)
    messages = edges_of(lambda c, r: after[c][r : r + 1, :], rows, even_b, two)
    for message, edge in zip(messages, take(len(messages))):
        edge[...] = message
    if first:
        prev_out, rim_out = take(2)
        prev_out[0] = prev_parts[1]
        for q in range(4):
            prev_out[1 + q] = prev_weights[q]
        rim_out[...] = rim


def conjugate(moments):
    def apply(p):
        shifted = [None] + p
        return [
            (SHIFT * p[k] if k < len(p) else 0.0) * (1.0 / GAIN)
            + ((1.0 / GAIN) * shifted[k] if k else 0.0)
            for k in range(len(p) + 1)
        ]

    def product(p, q):
        return sum(p[i] * q[j] * moments[i + j] for i in range(len(p)) for j in range(len(q)))

    def plus(p, factor, q):
        size = max(len(p), len(q))
        pad = lambda a: a + [None] * (size - len(a))
        out = []
        for a, b in zip(pad(p), pad(q)):
            out.append(factor * b if a is None else a if b is None else a + factor * b)
        return out

    one = jnp.ones_like(moments[0])
    solution_field, residual, direction = [], [one], [one]
    norm_now = moments[0]
    for step in range(ITERS):
        image = apply(direction)
        alpha = norm_now / product(direction, image)
        solution_field = plus(solution_field, alpha, direction)
        residual = plus(residual, -alpha, image)
        if step + 1 < ITERS:
            norm_next = product(residual, residual)
            direction = plus(residual, norm_next / norm_now, direction)
            norm_now = norm_next
    return solution_field, residual


def finish_kernel(sums, *refs):
    basis, (solution_ref, residual_ref) = refs[: ITERS + 1], refs[ITERS + 1 :]
    total = jnp.sum(sums[...], axis=0, keepdims=True)
    lane = lax.broadcasted_iota(jnp.int32, (1, LANES), 1)
    moments = [
        jnp.sum(jnp.where(lane == i, total, 0.0), axis=1, keepdims=True) for i in range(2 * ITERS)
    ]
    solution_field, residual = conjugate(moments)
    for c in range(2):
        values = [ref[c] for ref in basis]
        solution_ref[c] = sum(a * v for a, v in zip(solution_field, values))
        residual_ref[c] = sum(a * v for a, v in zip(residual, values))


VMEM = pl.BlockSpec(memory_space=pltpu.VMEM)
SMEM = pl.BlockSpec(memory_space=pltpu.SMEM)


def call(kernel, in_specs, shapes, name):
    shapes = [jax.ShapeDtypeStruct(s, F32) for s in shapes]
    return pl.pallas_call(
        kernel,
        in_specs=in_specs,
        out_specs=[VMEM] * len(shapes),
        out_shape=shapes,
        name=name,
        compiler_params=pltpu.CompilerParams(vmem_limit_bytes=48 * 1024 * 1024),
    )


def body(
    right_side,
    stiff_across,
    stiff_down,
    anchor,
    source_node,
    target_cell,
    corner_weight,
    block_count,
):
    rows, cols = stiff_across.shape[1:]
    rhs = right_side[:, 0]
    across, down, hold = stiff_across[0], stiff_down[0], anchor[0]
    slots = source_node.shape[2]
    nb = slots // LANES
    source = source_node.reshape(nb, LANES)
    target = target_cell.reshape(nb, LANES)
    weights = corner_weight.reshape(4, nb, LANES)
    n_gz, n_xy = lax.axis_size("gz"), lax.axis_size("xy")
    at_gz, at_xy = lax.axis_index("gz"), lax.axis_index("xy")
    two = n_xy > 2
    flags = jnp.stack([at_gz % 2, at_xy % 2, (at_gz < n_gz - 1).astype(jnp.int32)]).astype(jnp.int32)
    n_edges = 2 if two else 1

    pack, *edges = call(
        functools.partial(pack_kernel, two),
        [SMEM, SMEM] + [VMEM] * 5,
        [(rows, 2 * cols + 6 * LANES)] + [(4, cols)] * n_edges,
        "pack",
    )(flags, block_count, rhs, down, source, target, weights)

    def exchange(to0, to1, edges):
        got1 = swapped(to1, "gz", 1)
        got0 = swapped(to0, "gz", 0)
        return got0, got1, [swapped(e, "xy", i) for i, e in enumerate(edges)]

    field_shape = (2, rows, cols)
    message = (2, nb, LANES)
    common = [field_shape, (2,) + message, message, message] + [(2, cols)] * n_edges
    basis = [rhs]

    got0, got1, got_edges = exchange(pack, pack, edges)
    field, local, to0, to1, *tail = call(
        functools.partial(step_kernel, True, False, two, n_edges),
        [SMEM, SMEM] + [VMEM] * (9 + n_edges),
        common + [(5, nb, LANES), (1, cols)],
        "first",
    )(flags, block_count, rhs, across, down, hold, source, weights, target, got0, got1, *got_edges)
    edges, (prev, rim) = tail[:n_edges], tail[n_edges:]

    for step in range(1, ITERS):
        last = step == ITERS - 1
        got0, got1, got_edges = exchange(to0, to1, edges)
        args = [flags, block_count, field, across, down, hold, source, prev, local, got0, got1, *got_edges, rim]
        shapes = common
        if last:
            args += basis
            shapes = [field_shape, (n_gz * n_xy, LANES)]
        basis.append(field)
        field, *tail = call(
            functools.partial(step_kernel, False, last, two, n_edges),
            [SMEM, SMEM] + [VMEM] * (len(args) - 2),
            shapes,
            "last" if last else "step",
        )(*args)
        if not last:
            local, to0, to1, *edges = tail
    basis.append(field)
    sums = tail[0].reshape(n_gz * n_xy, 1, LANES)
    sums = lax.all_to_all(sums, ("gz", "xy"), 0, 0).reshape(n_gz * n_xy, LANES)
    solution_field, residual = call(
        finish_kernel, [VMEM] * (1 + len(basis)), [field_shape] * 2, "finish"
    )(sums, *basis)
    return solution_field[:, None], residual[:, None]


def solution(mesh):
    in_specs = (
        P(None, "gz", "xy", None),
        P("gz", "xy", None),
        P("gz", "xy", None),
        P("gz", "xy", None),
        P("gz", "xy", None),
        P("gz", "xy", None),
        P(None, "gz", "xy", None),
        P("gz", "xy"),
    )
    out_specs = (P(None, "gz", "xy", None), P(None, "gz", "xy", None))
    return jax.shard_map(body, mesh=mesh, in_specs=in_specs, out_specs=out_specs, check_vma=False)
```

```python
import functools

import jax
import jax.numpy as jnp
from jax import lax
from jax.experimental import pallas as pl
from jax.experimental.pallas import tpu as pltpu
from jax.sharding import PartitionSpec as P


BLOCK = 128
ITERS = 3
LANES = 128
GAIN = 0.25
SHIFT = 1.25
F32 = jnp.float32
BF16 = jnp.bfloat16


def swapped(block, axis, first):
    count = lax.axis_size(axis)
    route = []
    for i in range(first, count - 1, 2):
        route += [(i, i + 1), (i + 1, i)]
    return lax.ppermute(block, axis, route) if route else None


def swapped_sections(block, first):
    count, width = lax.axis_size("gz"), lax.axis_size("xy")
    route = []
    for i in range(first, count - 1, 2):
        for j in range(width):
            a, b = i * width + j, (i + 1) * width + j
            route += [(a, b), (b, a)]
    paired = {a for a, _ in route}
    for a in range(0, count * width - 1, 2):
        if a not in paired and a + 1 not in paired and a // width == (a + 1) // width:
            route += [(a, a + 1), (a + 1, a)]
    return lax.ppermute(block, ("gz", "xy"), route)


def split2(x):
    high = x.astype(BF16)
    return high, (x - high.astype(F32)).astype(BF16)


def div_mod(x, d):
    if d & (d - 1) == 0:
        return lax.shift_right_logical(x, jnp.int32(d.bit_length() - 1)), x & (d - 1)
    q = lax.div(x, jnp.int32(d))
    return q, x - q * d


def hi_lo(index, rows, cols):
    row, col = div_mod(index, cols)
    tile, lane = div_mod(col, LANES)
    return tile * rows + row, lane


def row_of(tile, k):
    return tile[k : k + 1, :]


def one_hot(lanes_of):
    nb = lanes_of.shape[0]
    at = lax.broadcasted_iota(jnp.int32, (LANES, LANES), 0)
    return jnp.concatenate(
        [jnp.where(at == row_of(lanes_of, k), 1.0, 0.0).astype(BF16) for k in range(nb)], axis=1
    )


def tall(field):
    n = field.shape[1] // LANES
    return jnp.concatenate([field[:, i * LANES : (i + 1) * LANES] for i in range(n)], axis=0)


def wide(stack, rows):
    n = stack.shape[0] // rows
    return jnp.concatenate([stack[i * rows : (i + 1) * rows, :] for i in range(n)], axis=1)


def operand(fields):
    out = []
    for f in fields:
        high, low = split2(tall(f))
        out.append(jnp.concatenate([high, low], axis=1))
    return jnp.concatenate(out, axis=0)


def right_of(field):
    return pltpu.roll(field, field.shape[1] - 1, 1)


def looked_up(field, slots_hi, hot2):
    high = tall(field[0]).shape[0]
    left = operand([field[0], field[1]])
    nb = slots_hi.shape[0]
    at = lax.broadcasted_iota(jnp.int32, (high, LANES), 0)
    found = ([], [])
    for k in range(nb):
        got = jnp.dot(left, hot2[:, k * LANES : (k + 1) * LANES], preferred_element_type=F32)
        mask = at == row_of(slots_hi, k)
        for c in range(2):
            found[c].append(
                jnp.sum(jnp.where(mask, got[c * high : (c + 1) * high], 0.0), axis=0, keepdims=True)
            )
    return jnp.stack([jnp.concatenate(f, axis=0) for f in found])


def interpolated(field, slots_hi, hot2, weights):
    high = tall(field[0]).shape[0]
    left = operand([field[0], field[1], right_of(field[0]), right_of(field[1])])
    nb = slots_hi.shape[0]
    at = lax.broadcasted_iota(jnp.int32, (high, LANES), 0)
    found = ([], [])
    for k in range(nb):
        got = jnp.dot(left, hot2[:, k * LANES : (k + 1) * LANES], preferred_element_type=F32)
        here = row_of(slots_hi, k)
        upper = at == here
        lower = at == here + 1
        w = [row_of(weights[q], k) for q in range(4)]
        wl = jnp.where(upper, w[0], jnp.where(lower, w[2], 0.0))
        wr = jnp.where(upper, w[1], jnp.where(lower, w[3], 0.0))
        for c in range(2):
            value = wl * got[c * high : (c + 1) * high] + wr * got[(2 + c) * high : (3 + c) * high]
            found[c].append(jnp.sum(value, axis=0, keepdims=True))
    return jnp.stack([jnp.concatenate(f, axis=0) for f in found])


NT = (((1,), (1,)), ((), ()))


def spread_own(values, slots_hi, hot, rows, high):
    nb = slots_hi.shape[0]
    at = lax.broadcasted_iota(jnp.int32, (high, LANES), 0)
    masks = [at == row_of(slots_hi, k) for k in range(nb)]
    parts = []
    for c in range(2):
        high_part = values[c].astype(BF16).astype(F32)
        for part in (high_part, values[c] - high_part):
            parts.append(
                jnp.concatenate(
                    [jnp.where(masks[k], row_of(part, k), 0.0).astype(BF16) for k in range(nb)], axis=1
                )
            )
    out = lax.dot_general(jnp.concatenate(parts, axis=0), hot, NT, preferred_element_type=F32)
    return [
        wide(out[2 * c * high : (2 * c + 1) * high] + out[(2 * c + 1) * high : (2 * c + 2) * high], rows)
        for c in range(2)
    ]


def spread_corners(values, weights, slots_hi, hot, rows, high):
    nb = slots_hi.shape[0]
    at = lax.broadcasted_iota(jnp.int32, (high, LANES), 0)
    upper = [at == row_of(slots_hi, k) for k in range(nb)]
    lower = [at == row_of(slots_hi, k) + 1 for k in range(nb)]
    parts = []
    for c in range(2):
        for side in range(2):
            up = values[c] * weights[side]
            down = values[c] * weights[2 + side]
            up_high = up.astype(BF16).astype(F32)
            down_high = down.astype(BF16).astype(F32)
            for a, b in ((up_high, down_high), (up - up_high, down - down_high)):
                parts.append(
                    jnp.concatenate(
                        [
                            jnp.where(
                                upper[k], row_of(a, k), jnp.where(lower[k], row_of(b, k), 0.0)
                            ).astype(BF16)
                            for k in range(nb)
                        ],
                        axis=1,
                    )
                )
    out = lax.dot_general(jnp.concatenate(parts, axis=0), hot, NT, preferred_element_type=F32)
    result = []
    for c in range(2):
        sides = []
        for side in range(2):
            p = (2 * c + side) * 2
            sides.append(wide(out[p * high : (p + 1) * high] + out[(p + 1) * high : (p + 2) * high], rows))
        result.append(sides[0] + pltpu.roll(sides[1], 1, 1))
    return result


def springs(field, across, down, hold, upper_row, lower_row, rim):
    rows, cols = field.shape
    col = lax.broadcasted_iota(jnp.int32, (rows, cols), 1)
    row = lax.broadcasted_iota(jnp.int32, (rows, cols), 0)
    right = jnp.where(col == cols - 1, 0.0, pltpu.roll(field, cols - 1, 1))
    pull = across * (field - right)
    out = pull - jnp.where(col == 0, 0.0, pltpu.roll(pull, 1, 1))
    lower = jnp.where(row == rows - 1, lower_row, pltpu.roll(field, rows - 1, 0))
    pull = down * (field - lower)
    above = rim * (upper_row - field[0:1, :])
    out = out + pull - jnp.where(row == 0, above, pltpu.roll(pull, 1, 0))
    return out + hold * field


def pick(flag, a, b):
    return jnp.where(flag, a, b)


def edges_of(get_row, rows, even_b, two):
    first = [get_row(c, 0) for c in range(2)]
    last = [get_row(c, rows - 1) for c in range(2)]
    out = [jnp.concatenate([pick(even_b, last[c], first[c]) for c in range(2)], axis=0)]
    if two:
        out.append(jnp.concatenate([pick(even_b, first[c], last[c]) for c in range(2)], axis=0))
    return out


def pack_kernel(two, flags, count, field, down, source, target, weights, *refs):
    rows, cols = down.shape
    even_b = flags[1] == 0
    has_next = flags[2]
    nb = source.shape[0]
    n_edges = 2 if two else 1
    pack, edges, (last_down, ids, held, sems) = refs[0], refs[1 : 1 + n_edges], refs[1 + n_edges :]
    pairs = [(field.at[c], pack.at[:, c * cols : (c + 1) * cols]) for c in range(2)]
    pairs += [(down, last_down), (source, ids.at[0]), (target, ids.at[1]), (weights, held)]
    copies = [pltpu.make_async_copy(a, b, sems.at[i]) for i, (a, b) in enumerate(pairs)]
    for copy in copies:
        copy.start()
    for copy in copies:
        copy.wait()
    block = lax.broadcasted_iota(jnp.int32, (nb, LANES), 0)
    live = jnp.where(block * LANES < count[0, 0] * BLOCK * has_next, 1.0, 0.0)
    parts = [ids[0].astype(F32), ids[1].astype(F32)] + [held[q] * live for q in range(4)]
    for i, part in enumerate(parts):
        pack[:nb, 2 * cols + i * LANES : 2 * cols + (i + 1) * LANES] = part
    messages = edges_of(lambda c, r: pack[r : r + 1, c * cols : (c + 1) * cols], rows, even_b, two)
    for message, edge in zip(messages, edges):
        edge[0:2, :] = message
        edge[2:3, :] = last_down[rows - 1 : rows, :]


def halves(flags, edge_refs):
    even_b = flags[1] == 0
    zero = edge_refs[0][...]
    if len(edge_refs) == 2:
        other = edge_refs[1][...]
    else:
        other = jnp.zeros_like(zero)
    return pick(even_b, other, zero), pick(even_b, zero, other)


def advance(field, error, error_prev, own, prev, across, down, hold, above, below, rim):
    own_hi, own_hot = own
    prev_hi, prev_hot, prev_weights = prev
    rows, cols = field[0].shape
    high = rows * (cols // LANES)
    pulled = spread_own(error, own_hi, own_hot, rows, high)
    pushed = spread_corners(error_prev, prev_weights, prev_hi, prev_hot, rows, high)
    result = []
    for c in range(2):
        image = springs(field[c], across, down, hold, above[c : c + 1], below[c : c + 1], rim)
        image = image + (pushed[c] - pulled[c])
        result.append(GAIN * image - SHIFT * field[c])
    return result


def step_kernel(
    first, last, two, n_edges, flags, count, field_ref, across, down, hold, source, weights_or_prev, local, *rest
):
    rest = list(rest)
    take = lambda n: [rest.pop(0) for _ in range(n)]
    even = flags[0] == 0
    even_b = flags[1] == 0
    has_next = flags[2]
    nb = source.shape[0]
    rows, cols = across.shape
    block = lax.broadcasted_iota(jnp.int32, (nb, LANES), 0)
    live = jnp.where(block * LANES < count[0, 0] * BLOCK * has_next, 1.0, 0.0)
    field = [field_ref[0], field_ref[1]]
    own_hi, own_lo = hi_lo(source[...], rows, cols)
    own_hot = one_hot(own_lo)
    own_hot2 = jnp.concatenate([own_hot, own_hot], axis=0)
    got0, got1 = take(2)
    edge_refs = take(n_edges)
    above, below = halves(flags, edge_refs)
    if first:
        target = local
        rim = above[2:3, :]
        slot = lambda ref, i: ref[:nb, 2 * cols + i * LANES : 2 * cols + (i + 1) * LANES]
        prev_parts = [pick(even, slot(got1, i), slot(got0, i)) for i in range(6)]
        prev_parts[2:] = [jnp.where(flags[3] > 0, w, 0.0) for w in prev_parts[2:]]
        prev_target = prev_parts[1].astype(jnp.int32)
        prev_weights = prev_parts[2:]
        prev_hi, prev_lo = hi_lo(prev_target, rows, cols)
        prev_hot = one_hot(prev_lo)
        prev_hot2 = jnp.concatenate([prev_hot, prev_hot], axis=0)
        comp = lambda ref, c: ref[:, c * cols : (c + 1) * cols]
        next_field = [pick(even, comp(got0, c), comp(got1, c)) for c in range(2)]
        prev_field = [pick(even, comp(got1, c), comp(got0, c)) for c in range(2)]
        own = looked_up(field, own_hi, own_hot2)
        mid = interpolated(field, prev_hi, prev_hot2, prev_weights)
        t_hi, t_lo = hi_lo(target[...], rows, cols)
        t_hot = one_hot(t_lo)
        own_weights = [weights_or_prev[q] for q in range(4)]
        from_next = interpolated(next_field, t_hi, jnp.concatenate([t_hot, t_hot], axis=0), own_weights)
        p_hi, p_lo = hi_lo(prev_parts[0].astype(jnp.int32), rows, cols)
        p_hot = one_hot(p_lo)
        from_prev = looked_up(prev_field, p_hi, jnp.concatenate([p_hot, p_hot], axis=0))
    else:
        rim = rest.pop(0)[...]
        prev_ref = weights_or_prev
        prev_target = prev_ref[0].astype(jnp.int32)
        prev_weights = [prev_ref[1 + q] for q in range(4)]
        prev_hi, prev_lo = hi_lo(prev_target, rows, cols)
        prev_hot = one_hot(prev_lo)
        prev_hot2 = jnp.concatenate([prev_hot, prev_hot], axis=0)
        own, mid = local[0], local[1]
        from_next = pick(even, got0[...], got1[...])
        from_prev = pick(even, got1[...], got0[...])
    if last:
        earlier = take(2)
    error = [live * (from_next[c] - own[c]) for c in range(2)]
    error_prev = [mid[c] - from_prev[c] for c in range(2)]
    after = advance(
        field,
        error,
        error_prev,
        (own_hi, own_hot),
        (prev_hi, prev_hot, prev_weights),
        across[...],
        down[...],
        hold[...],
        above,
        below,
        rim,
    )
    out = rest.pop(0)
    for c in range(2):
        out[c] = after[c]
    if last:
        moments = rest.pop(0)
        basis = [[ref[0], ref[1]] for ref in earlier] + [field, after]
        lane = lax.broadcasted_iota(jnp.int32, (1, LANES), 1)
        total = jnp.zeros((1, LANES), F32)
        for i in range(2 * ITERS):
            u, w = basis[i // 2], basis[i - i // 2]
            s = u[0] * w[0] + u[1] * w[1]
            s = jnp.sum(jnp.sum(s, axis=0, keepdims=True), axis=1, keepdims=True)
            total = total + jnp.where(lane == i, s, 0.0)
        moments[...] = jnp.broadcast_to(total, moments.shape)
        return
    after_own = looked_up(after, own_hi, own_hot2)
    after_mid = interpolated(after, prev_hi, prev_hot2, prev_weights)
    local_out, send0, send1 = take(3)
    local_out[0] = after_own
    local_out[1] = after_mid
    send0[...] = pick(even, after_own, after_mid)
    send1[...] = pick(even, after_mid, after_own)
    messages = edges_of(lambda c, r: after[c][r : r + 1, :], rows, even_b, two)
    for message, edge in zip(messages, take(len(messages))):
        edge[...] = message
    if first:
        prev_out, rim_out = take(2)
        prev_out[0] = prev_parts[1]
        for q in range(4):
            prev_out[1 + q] = prev_weights[q]
        rim_out[...] = rim


def conjugate(moments):
    def apply(p):
        shifted = [None] + p
        return [
            (SHIFT * p[k] if k < len(p) else 0.0) * (1.0 / GAIN)
            + ((1.0 / GAIN) * shifted[k] if k else 0.0)
            for k in range(len(p) + 1)
        ]

    def product(p, q):
        return sum(p[i] * q[j] * moments[i + j] for i in range(len(p)) for j in range(len(q)))

    def plus(p, factor, q):
        size = max(len(p), len(q))
        pad = lambda a: a + [None] * (size - len(a))
        out = []
        for a, b in zip(pad(p), pad(q)):
            out.append(factor * b if a is None else a if b is None else a + factor * b)
        return out

    one = jnp.ones_like(moments[0])
    solution_field, residual, direction = [], [one], [one]
    norm_now = moments[0]
    for step in range(ITERS):
        image = apply(direction)
        alpha = norm_now / product(direction, image)
        solution_field = plus(solution_field, alpha, direction)
        residual = plus(residual, -alpha, image)
        if step + 1 < ITERS:
            norm_next = product(residual, residual)
            direction = plus(residual, norm_next / norm_now, direction)
            norm_now = norm_next
    return solution_field, residual


def finish_kernel(sums, *refs):
    basis, (solution_ref, residual_ref) = refs[: ITERS + 1], refs[ITERS + 1 :]
    total = jnp.sum(sums[...], axis=0, keepdims=True)
    lane = lax.broadcasted_iota(jnp.int32, (1, LANES), 1)
    moments = [
        jnp.sum(jnp.where(lane == i, total, 0.0), axis=1, keepdims=True) for i in range(2 * ITERS)
    ]
    solution_field, residual = conjugate(moments)
    for c in range(2):
        values = [ref[c] for ref in basis]
        solution_ref[c] = sum(a * v for a, v in zip(solution_field, values))
        residual_ref[c] = sum(a * v for a, v in zip(residual, values))


VMEM = pl.BlockSpec(memory_space=pltpu.VMEM)
SMEM = pl.BlockSpec(memory_space=pltpu.SMEM)
HBM = pl.BlockSpec(memory_space=pltpu.HBM)


def call(kernel, in_specs, shapes, scratch=()):
    shapes = [jax.ShapeDtypeStruct(s, F32) for s in shapes]
    return pl.pallas_call(
        kernel,
        in_specs=in_specs,
        out_specs=[VMEM] * len(shapes),
        out_shape=shapes,
        scratch_shapes=list(scratch),
        compiler_params=pltpu.CompilerParams(vmem_limit_bytes=48 * 1024 * 1024),
    )


def body(
    right_side,
    stiff_across,
    stiff_down,
    anchor,
    source_node,
    target_cell,
    corner_weight,
    block_count,
):
    rows, cols = stiff_across.shape[1:]
    rhs = right_side[:, 0]
    across, down, hold = stiff_across[0], stiff_down[0], anchor[0]
    slots = source_node.shape[2]
    nb = slots // LANES
    source = source_node.reshape(nb, LANES)
    target = target_cell.reshape(nb, LANES)
    weights = corner_weight.reshape(4, nb, LANES)
    n_gz, n_xy = lax.axis_size("gz"), lax.axis_size("xy")
    at_gz, at_xy = lax.axis_index("gz"), lax.axis_index("xy")
    two = n_xy > 2
    flags = jnp.stack([at_gz % 2, at_xy % 2, (at_gz < n_gz - 1).astype(jnp.int32), (at_gz > 0).astype(jnp.int32)]).astype(jnp.int32)
    n_edges = 2 if two else 1

    pack, *edges = call(
        functools.partial(pack_kernel, two),
        [SMEM, SMEM] + [HBM] * 5,
        [(rows, 2 * cols + 6 * LANES)] + [(4, cols)] * n_edges,
        [
            pltpu.VMEM((rows, cols), F32),
            pltpu.VMEM((2, nb, LANES), jnp.int32),
            pltpu.VMEM((4, nb, LANES), F32),
            pltpu.SemaphoreType.DMA((6,)),
        ],
    )(flags, block_count, *(pltpu.with_memory_space_constraint(a, pltpu.HBM) for a in (rhs, down, source, target, weights)))

    def exchange(to0, to1, edges):
        got1 = swapped_sections(to1, 1)
        got0 = swapped_sections(to0, 0)
        got_edges = []
        for i, edge in enumerate(edges):
            got_edges.append(swapped(edge, "xy", i))
        return got0, got1, got_edges

    field_shape = (2, rows, cols)
    message = (2, nb, LANES)
    common = [field_shape, (2,) + message, message, message] + [(2, cols)] * n_edges
    basis = [rhs]

    got0, got1, got_edges = exchange(pack, pack, edges)
    field, local, to0, to1, *tail = call(
        functools.partial(step_kernel, True, False, two, n_edges),
        [SMEM, SMEM] + [VMEM] * (9 + n_edges),
        common + [(5, nb, LANES), (1, cols)],
    )(flags, block_count, rhs, across, down, hold, source, weights, target, got0, got1, *got_edges)
    edges, (prev, rim) = tail[:n_edges], tail[n_edges:]

    for step in range(1, ITERS):
        last = step == ITERS - 1
        got0, got1, got_edges = exchange(to0, to1, edges)
        args = [flags, block_count, field, across, down, hold, source, prev, local, got0, got1, *got_edges, rim]
        shapes = common
        if last:
            args += basis
            shapes = [field_shape, (n_gz * n_xy, LANES)]
        basis.append(field)
        field, *tail = call(
            functools.partial(step_kernel, False, last, two, n_edges),
            [SMEM, SMEM] + [VMEM] * (len(args) - 2),
            shapes,
        )(*args)
        if not last:
            local, to0, to1, *edges = tail
    basis.append(field)
    sums = tail[0].reshape(n_gz * n_xy, 1, LANES)
    sums = lax.all_to_all(sums, ("gz", "xy"), 0, 0).reshape(n_gz * n_xy, LANES)
    solution_field, residual = call(
        finish_kernel, [VMEM] * (1 + len(basis)), [field_shape] * 2
    )(sums, *basis)
    return solution_field[:, None], residual[:, None]


def solution(mesh):
    in_specs = (
        P(None, "gz", "xy", None),
        P("gz", "xy", None),
        P("gz", "xy", None),
        P("gz", "xy", None),
        P("gz", "xy", None),
        P("gz", "xy", None),
        P(None, "gz", "xy", None),
        P("gz", "xy"),
    )
    out_specs = (P(None, "gz", "xy", None), P(None, "gz", "xy", None))
    return jax.shard_map(body, mesh=mesh, in_specs=in_specs, out_specs=out_specs, check_vma=False)
```

```python
import functools

import jax
import jax.numpy as jnp
from jax import lax
from jax.experimental import pallas as pl
from jax.experimental.pallas import tpu as pltpu
from jax.sharding import PartitionSpec as P


BLOCK = 128
ITERS = 3
LANES = 128
GAIN = 0.25
SHIFT = 1.25
F32 = jnp.float32
BF16 = jnp.bfloat16
CHUNK = 256


def swapped(block, axis, first):
    count = lax.axis_size(axis)
    route = []
    for i in range(first, count - 1, 2):
        route += [(i, i + 1), (i + 1, i)]
    return lax.ppermute(block, axis, route) if route else None


def swapped_sections(block, first):
    count, width = lax.axis_size("gz"), lax.axis_size("xy")
    route = []
    for i in range(first, count - 1, 2):
        for j in range(width):
            a, b = i * width + j, (i + 1) * width + j
            route += [(a, b), (b, a)]
    paired = {a for a, _ in route}
    for a in range(0, count * width - 1, 2):
        if a not in paired and a + 1 not in paired and a // width == (a + 1) // width:
            route += [(a, a + 1), (a + 1, a)]
    return lax.ppermute(block, ("gz", "xy"), route)


def split2(x):
    high = x.astype(BF16)
    return high, (x - high.astype(F32)).astype(BF16)


def div_mod(x, d):
    if d & (d - 1) == 0:
        return lax.shift_right_logical(x, jnp.int32(d.bit_length() - 1)), x & (d - 1)
    q = lax.div(x, jnp.int32(d))
    return q, x - q * d


def hi_lo(index, rows, cols):
    row, col = div_mod(index, cols)
    tile, lane = div_mod(col, LANES)
    return tile * rows + row, lane


def row_of(tile, k):
    return tile[k : k + 1, :]


def one_hot(index, size, shift=0):
    at = lax.broadcasted_iota(jnp.int32, (size, LANES), 0) - shift
    return jnp.concatenate(
        [jnp.where(at == row_of(index, k), 1.0, 0.0).astype(BF16) for k in range(index.shape[0])],
        axis=1,
    )


def blend(index, size, first, second):
    at = lax.broadcasted_iota(jnp.int32, (size, LANES), 0)
    out = []
    for k in range(index.shape[0]):
        here = row_of(index, k)
        out.append(
            jnp.where(at == here, row_of(first, k), jnp.where(at == here + 1, row_of(second, k), 0.0))
        )
    return jnp.concatenate(out, axis=1)


def store_lanes(lo, lanes_ref):
    hot = one_hot(lo, LANES)
    lanes_ref[0:LANES, :] = hot
    lanes_ref[LANES : 2 * LANES, :] = hot


def tall(field):
    n = field.shape[1] // LANES
    return jnp.concatenate([field[:, i * LANES : (i + 1) * LANES] for i in range(n)], axis=0)


def wide(stack, rows):
    n = stack.shape[0] // rows
    return jnp.concatenate([stack[i * rows : (i + 1) * rows, :] for i in range(n)], axis=1)


def right_of(field):
    return pltpu.roll(field, field.shape[1] - 1, 1)


def load_left(field, left_ref, sides):
    fields = []
    for c in range(2):
        fields += [field[c], right_of(field[c])] if sides == 2 else [field[c]]
    for i, f in enumerate(fields):
        stack = tall(f)
        high, low = split2(stack)
        n = stack.shape[0]
        left_ref[i * n : (i + 1) * n, 0:LANES] = high
        left_ref[i * n : (i + 1) * n, LANES : 2 * LANES] = low


def as_tiles(rows_of):
    return jnp.concatenate(
        [r[:, i * LANES : (i + 1) * LANES] for r in rows_of for i in range(CHUNK // LANES)], axis=0
    )


def looked_up(left_ref, lanes_ref, high_ref):
    high, slots = high_ref.shape
    stride = left_ref.shape[0] // 2
    found = ([], [])
    for k in range(0, slots, CHUNK):
        mask = high_ref[:, k : k + CHUNK].astype(F32)
        for c in range(2):
            got = jnp.dot(
                left_ref[c * stride : c * stride + high, :],
                lanes_ref[:, k : k + CHUNK],
                preferred_element_type=F32,
            )
            found[c].append(jnp.sum(mask * got, axis=0, keepdims=True))
    return jnp.stack([as_tiles(f) for f in found])


def interpolated(left_ref, lanes_ref, blend_ref):
    high, slots = blend_ref.shape[1:]
    found = ([], [])
    for k in range(0, slots, CHUNK):
        wl = blend_ref[0, :, k : k + CHUNK]
        wr = blend_ref[1, :, k : k + CHUNK]
        for c in range(2):
            got = jnp.dot(
                left_ref[2 * c * high : 2 * (c + 1) * high, :],
                lanes_ref[:, k : k + CHUNK],
                preferred_element_type=F32,
            )
            value = wl * got[:high] + wr * got[high:]
            found[c].append(jnp.sum(value, axis=0, keepdims=True))
    return jnp.stack([as_tiles(f) for f in found])


NT = (((1,), (1,)), ((), ()))


def scaled(mask_ref, tile):
    return jnp.concatenate(
        [mask_ref[:, k * LANES : (k + 1) * LANES] * row_of(tile, k) for k in range(tile.shape[0])],
        axis=1,
    )


def spread_own(values, lanes_ref, high_ref, rows):
    high = high_ref.shape[0]
    result = []
    for c in range(2):
        parts = [scaled(high_ref, part) for part in split2(values[c])]
        out = lax.dot_general(
            jnp.concatenate(parts, axis=0), lanes_ref[0:LANES, :], NT, preferred_element_type=F32
        )
        result.append(wide(out[:high] + out[high:], rows))
    return result


def spread_corners(values, weights, lanes_ref, high_ref, below_ref, rows):
    high = high_ref.shape[0]
    result = []
    for c in range(2):
        parts = []
        for side in range(2):
            for up, down in zip(split2(values[c] * weights[side]), split2(values[c] * weights[2 + side])):
                parts.append(scaled(high_ref, up) + scaled(below_ref, down))
        out = lax.dot_general(
            jnp.concatenate(parts, axis=0), lanes_ref[0:LANES, :], NT, preferred_element_type=F32
        )
        sides = [
            wide(out[p * high : (p + 1) * high] + out[(p + 1) * high : (p + 2) * high], rows)
            for p in (0, 2)
        ]
        result.append(sides[0] + pltpu.roll(sides[1], 1, 1))
    return result


def springs(field, across, down, hold, upper_row, lower_row, rim):
    rows, cols = field.shape
    col = lax.broadcasted_iota(jnp.int32, (rows, cols), 1)
    row = lax.broadcasted_iota(jnp.int32, (rows, cols), 0)
    right = jnp.where(col == cols - 1, 0.0, pltpu.roll(field, cols - 1, 1))
    pull = across * (field - right)
    out = pull - jnp.where(col == 0, 0.0, pltpu.roll(pull, 1, 1))
    lower = jnp.where(row == rows - 1, lower_row, pltpu.roll(field, rows - 1, 0))
    pull = down * (field - lower)
    above = rim * (upper_row - field[0:1, :])
    out = out + pull - jnp.where(row == 0, above, pltpu.roll(pull, 1, 0))
    return out + hold * field


def pick(flag, a, b):
    return jnp.where(flag, a, b)


def edges_of(get_row, rows, even_b, two):
    first = [get_row(c, 0) for c in range(2)]
    last = [get_row(c, rows - 1) for c in range(2)]
    out = [jnp.concatenate([pick(even_b, last[c], first[c]) for c in range(2)], axis=0)]
    if two:
        out.append(jnp.concatenate([pick(even_b, first[c], last[c]) for c in range(2)], axis=0))
    return out


def pack_kernel(two, flags, count, field, down, hold, source, target, weights, *refs):
    rows, cols = down.shape
    even_b = flags[1] == 0
    has_next = flags[2]
    nb = source.shape[0]
    n_edges = 2 if two else 1
    pack, edges = refs[0], refs[1 : 1 + n_edges]
    last_down, hold_out, ids, held, sems = refs[1 + n_edges :]
    pairs = [(field.at[c], pack.at[:, c * cols : (c + 1) * cols]) for c in range(2)]
    pairs += [(down, last_down), (source, ids.at[0]), (target, ids.at[1]), (weights, held)]
    pairs += [(hold, hold_out)]
    copies = [pltpu.make_async_copy(a, b, sems.at[i]) for i, (a, b) in enumerate(pairs)]
    for copy in copies:
        copy.start()
    for copy in copies:
        copy.wait()
    block = lax.broadcasted_iota(jnp.int32, (nb, LANES), 0)
    live = jnp.where(block * LANES < count[0, 0] * BLOCK * has_next, 1.0, 0.0)
    parts = [ids[0].astype(F32), ids[1].astype(F32)] + [held[q] * live for q in range(4)]
    for i, part in enumerate(parts):
        pack[:nb, 2 * cols + i * LANES : 2 * cols + (i + 1) * LANES] = part
    messages = edges_of(lambda c, r: pack[r : r + 1, c * cols : (c + 1) * cols], rows, even_b, two)
    for message, edge in zip(messages, edges):
        edge[0:2, :] = message
        edge[2:3, :] = last_down[rows - 1 : rows, :]


def halves(flags, edge_refs):
    even_b = flags[1] == 0
    zero = edge_refs[0][...]
    if len(edge_refs) == 2:
        other = edge_refs[1][...]
    else:
        other = jnp.zeros_like(zero)
    return pick(even_b, other, zero), pick(even_b, zero, other)


def live_slots(flags, count, nb):
    block = lax.broadcasted_iota(jnp.int32, (nb, LANES), 0)
    return jnp.where(block * LANES < count[0, 0] * BLOCK * flags[2], 1.0, 0.0)


def spring_image(field, across, down, hold, above, below, rim):
    return [
        springs(
            field[c], across[...], down[...], hold[...], above[c : c + 1], below[c : c + 1], rim
        )
        for c in range(2)
    ]


def early_kernel(flags, field_ref, across, down, hold, source, target, weights, *refs):
    edge_refs = refs[:-8]
    base, own_ref, rim_ref, own_lanes, own_high, next_lanes, next_blend, left = refs[-8:]
    rows, cols = across.shape
    size = own_high.shape[0]
    field = [field_ref[0], field_ref[1]]
    above, below = halves(flags, edge_refs)
    image = spring_image(field, across, down, hold, above, below, above[2:3, :])
    for c in range(2):
        base[c] = image[c]
    rim_ref[...] = above[2:3, :]
    hi, lo = hi_lo(source[...], rows, cols)
    store_lanes(lo, own_lanes)
    own_high[...] = one_hot(hi, size)
    hi, lo = hi_lo(target[...], rows, cols)
    store_lanes(lo, next_lanes)
    for side in range(2):
        next_blend[side] = blend(hi, size, weights[side], weights[2 + side])
    load_left(field, left, 1)
    own_ref[...] = looked_up(left, own_lanes, own_high)


def send_on(even, even_b, two, field, own_tables, prev_tables, left, local_ref, send0, send1, *edges):
    own_lanes, own_high = own_tables
    prev_lanes, prev_blend = prev_tables
    load_left(field, left, 2)
    own = looked_up(left, own_lanes, own_high)
    mid = interpolated(left, prev_lanes, prev_blend)
    local_ref[0] = own
    local_ref[1] = mid
    send0[...] = pick(even, own, mid)
    send1[...] = pick(even, mid, own)
    messages = edges_of(lambda c, r: field[c][r : r + 1, :], field[0].shape[0], even_b, two)
    for message, edge in zip(messages, edges):
        edge[...] = message


def stepped(field_ref, image):
    return [GAIN * image[c] - SHIFT * field_ref[c] for c in range(2)]


def first_kernel(
    two, flags, count, field_ref, base, own, own_lanes, own_high, next_lanes, next_blend, got0, got1, *refs
):
    refs, (left, next_left, prev_left, lanes, mask) = refs[:-5], refs[-5:]
    out, local_ref, send0, send1, *edges = refs[:-5]
    prev_weights, prev_lanes, prev_high, prev_below, prev_blend = refs[-5:]
    even, even_b = flags[0] == 0, flags[1] == 0
    nb = own.shape[1]
    rows, cols = field_ref.shape[1:]
    size = own_high.shape[0]
    slot = lambda ref, i: ref[:nb, 2 * cols + i * LANES : 2 * cols + (i + 1) * LANES]
    prev = [pick(even, slot(got1, i), slot(got0, i)) for i in range(6)]
    comp = lambda ref, c: ref[:, c * cols : (c + 1) * cols]
    weights = [jnp.where(flags[3] > 0, w, 0.0) for w in prev[2:]]
    for q in range(4):
        prev_weights[q] = weights[q]
    hi, lo = hi_lo(prev[1].astype(jnp.int32), rows, cols)
    store_lanes(lo, prev_lanes)
    prev_high[...] = one_hot(hi, size)
    prev_below[...] = one_hot(hi, size, 1)
    for side in range(2):
        prev_blend[side] = blend(hi, size, weights[side], weights[2 + side])
    load_left([field_ref[0], field_ref[1]], left, 2)
    mid = interpolated(left, prev_lanes, prev_blend)
    load_left([pick(even, comp(got0, c), comp(got1, c)) for c in range(2)], next_left, 2)
    got_next = interpolated(next_left, next_lanes, next_blend)
    hi, lo = hi_lo(prev[0].astype(jnp.int32), rows, cols)
    store_lanes(lo, lanes)
    mask[...] = one_hot(hi, size)
    load_left([pick(even, comp(got1, c), comp(got0, c)) for c in range(2)], prev_left, 1)
    got_prev = looked_up(prev_left, lanes, mask)
    live = live_slots(flags, count, nb)
    pulled = spread_own([live * (own[c] - got_next[c]) for c in range(2)], own_lanes, own_high, rows)
    error = [mid[c] - got_prev[c] for c in range(2)]
    pushed = spread_corners(error, weights, prev_lanes, prev_high, prev_below, rows)
    after = stepped(field_ref, [base[c] + pulled[c] + pushed[c] for c in range(2)])
    for c in range(2):
        out[c] = after[c]
    send_on(
        even,
        even_b,
        two,
        after,
        (own_lanes, own_high),
        (prev_lanes, prev_blend),
        left,
        local_ref,
        send0,
        send1,
        *edges,
    )


def moments_of(pairs):
    lane = lax.broadcasted_iota(jnp.int32, (1, LANES), 1)
    total = jnp.zeros((1, LANES), F32)
    for i, (u, w) in enumerate(pairs):
        s = u[0] * w[0] + u[1] * w[1]
        s = jnp.sum(jnp.sum(s, axis=0, keepdims=True), axis=1, keepdims=True)
        total = total + jnp.where(lane == i, s, 0.0)
    return total


def step_kernel(
    last,
    two,
    n_edges,
    flags,
    count,
    field_ref,
    across,
    down,
    hold,
    own_lanes,
    own_high,
    prev_weights,
    prev_lanes,
    prev_high,
    prev_below,
    prev_blend,
    local,
    rim,
    got0,
    got1,
    *refs,
):
    refs = list(refs)
    edge_refs = [refs.pop(0) for _ in range(n_edges)]
    earlier = [refs.pop(0) for _ in range(ITERS - 1)] if last else []
    out = refs.pop(0)
    even, even_b = flags[0] == 0, flags[1] == 0
    nb = local.shape[2]
    rows, _ = across.shape
    field = [field_ref[0], field_ref[1]]
    live = live_slots(flags, count, nb)
    got_next = pick(even, got0[...], got1[...])
    got_prev = pick(even, got1[...], got0[...])
    pulled = spread_own([live * (local[0, c] - got_next[c]) for c in range(2)], own_lanes, own_high, rows)
    error = [local[1, c] - got_prev[c] for c in range(2)]
    weights = [prev_weights[q] for q in range(4)]
    pushed = spread_corners(error, weights, prev_lanes, prev_high, prev_below, rows)
    above, below = halves(flags, edge_refs)
    image = spring_image(field, across, down, hold, above, below, rim[...])
    after = stepped(field_ref, [image[c] + pulled[c] + pushed[c] for c in range(2)])
    for c in range(2):
        out[c] = after[c]
    if last:
        basis = [(ref[0], ref[1]) for ref in earlier] + [field, after]
        total = moments_of([(basis[i // 2], basis[i - i // 2]) for i in range(2 * ITERS)])
        sums = refs.pop(0)
        sums[...] = jnp.broadcast_to(total, sums.shape)
    else:
        messages, left = refs[:-1], refs[-1]
        send_on(even, even_b, two, after, (own_lanes, own_high), (prev_lanes, prev_blend), left, *messages)


def conjugate(moments):
    def apply(p):
        shifted = [None] + p
        return [
            (SHIFT * p[k] if k < len(p) else 0.0) * (1.0 / GAIN)
            + ((1.0 / GAIN) * shifted[k] if k else 0.0)
            for k in range(len(p) + 1)
        ]

    def product(p, q):
        return sum(p[i] * q[j] * moments[i + j] for i in range(len(p)) for j in range(len(q)))

    def plus(p, factor, q):
        size = max(len(p), len(q))
        pad = lambda a: a + [None] * (size - len(a))
        out = []
        for a, b in zip(pad(p), pad(q)):
            out.append(factor * b if a is None else a if b is None else a + factor * b)
        return out

    one = jnp.ones_like(moments[0])
    solution_field, residual, direction = [], [one], [one]
    norm_now = moments[0]
    for step in range(ITERS):
        image = apply(direction)
        alpha = norm_now / product(direction, image)
        solution_field = plus(solution_field, alpha, direction)
        residual = plus(residual, -alpha, image)
        if step + 1 < ITERS:
            norm_next = product(residual, residual)
            direction = plus(residual, norm_next / norm_now, direction)
            norm_now = norm_next
    return solution_field, residual


def finish_kernel(sums, *refs):
    basis, (solution_ref, residual_ref) = refs[: ITERS + 1], refs[ITERS + 1 :]
    total = jnp.sum(sums[...], axis=0, keepdims=True)
    lane = lax.broadcasted_iota(jnp.int32, (1, LANES), 1)
    moments = [
        jnp.sum(jnp.where(lane == i, total, 0.0), axis=1, keepdims=True) for i in range(2 * ITERS)
    ]
    solution_field, residual = conjugate(moments)
    for c in range(2):
        values = [ref[c] for ref in basis]
        solution_ref[c] = sum(a * v for a, v in zip(solution_field, values))
        residual_ref[c] = sum(a * v for a, v in zip(residual, values))


VMEM = pl.BlockSpec(memory_space=pltpu.VMEM)
SMEM = pl.BlockSpec(memory_space=pltpu.SMEM)
HBM = pl.BlockSpec(memory_space=pltpu.HBM)


def call(kernel, in_specs, shapes, scratch=()):
    shapes = [s if isinstance(s, jax.ShapeDtypeStruct) else jax.ShapeDtypeStruct(s, F32) for s in shapes]
    return pl.pallas_call(
        kernel,
        in_specs=in_specs,
        out_specs=[VMEM] * len(shapes),
        out_shape=shapes,
        scratch_shapes=list(scratch),
        compiler_params=pltpu.CompilerParams(vmem_limit_bytes=48 * 1024 * 1024),
    )


def body(
    right_side,
    stiff_across,
    stiff_down,
    anchor,
    source_node,
    target_cell,
    corner_weight,
    block_count,
):
    rows, cols = stiff_across.shape[1:]
    rhs = right_side[:, 0]
    across, down, hold = stiff_across[0], stiff_down[0], anchor[0]
    slots = source_node.shape[2]
    nb = slots // LANES
    source = source_node.reshape(nb, LANES)
    target = target_cell.reshape(nb, LANES)
    weights = corner_weight.reshape(4, nb, LANES)
    n_gz, n_xy = lax.axis_size("gz"), lax.axis_size("xy")
    at_gz, at_xy = lax.axis_index("gz"), lax.axis_index("xy")
    two = n_xy > 2
    flags = jnp.stack([at_gz % 2, at_xy % 2, (at_gz < n_gz - 1).astype(jnp.int32), (at_gz > 0).astype(jnp.int32)]).astype(jnp.int32)
    n_edges = 2 if two else 1

    in_hbm = lambda *arrays: [pltpu.with_memory_space_constraint(a, pltpu.HBM) for a in arrays]
    pack, *rest = call(
        functools.partial(pack_kernel, two),
        [SMEM, SMEM] + [HBM] * 6,
        [(rows, 2 * cols + 6 * LANES)] + [(4, cols)] * n_edges + [(rows, cols)] * 2,
        [
            pltpu.VMEM((2, nb, LANES), jnp.int32),
            pltpu.VMEM((4, nb, LANES), F32),
            pltpu.SemaphoreType.DMA((7,)),
        ],
    )(flags, block_count, *in_hbm(rhs, down, hold, source, target, weights))
    edges, (down, hold) = rest[:n_edges], rest[n_edges:]

    def exchange(to0, to1, edges):
        got1 = swapped_sections(to1, 1)
        got0 = swapped_sections(to0, 0)
        got_edges = []
        for i, edge in enumerate(edges):
            got_edges.append(swapped(edge, "xy", i))
        return got0, got1, got_edges

    field_shape = (2, rows, cols)
    message = (2, nb, LANES)
    size = rows * cols // LANES
    common = [field_shape, (2,) + message, message, message] + [(2, cols)] * n_edges
    table = lambda *shape: jax.ShapeDtypeStruct(shape, BF16)
    left = lambda sides: pltpu.VMEM((2 * sides * size, 2 * LANES), BF16)
    lanes, mask, blends = (2 * LANES, slots), (size, slots), (2, size, slots)
    run = lambda kernel, shapes, scratch, *args: call(
        kernel, [SMEM, SMEM] + [VMEM] * (len(args) - 2), shapes, scratch
    )(*args)
    stiff = (across, down, hold)
    basis = [rhs]

    got0, got1, got_edges = exchange(pack, pack, edges)
    base, own, rim, own_lanes, own_high, next_lanes, next_blend = call(
        early_kernel,
        [SMEM] + [VMEM] * (7 + n_edges),
        [field_shape, message, (1, cols), table(*lanes), table(*mask), table(*lanes), blends],
        [left(1)],
    )(flags, rhs, *stiff, source, target, weights, *got_edges)
    field, local, to0, to1, *rest = run(
        functools.partial(first_kernel, two),
        common + [(4, nb, LANES), table(*lanes), table(*mask), table(*mask), blends],
        [left(2), left(2), left(1), pltpu.VMEM(lanes, BF16), pltpu.VMEM(mask, BF16)],
        *(flags, block_count, rhs, base, own, own_lanes, own_high, next_lanes, next_blend, got0, got1),
    )
    edges, prev = rest[:n_edges], rest[n_edges:]

    for step in range(1, ITERS):
        last = step == ITERS - 1
        got0, got1, got_edges = exchange(to0, to1, edges)
        field_next, *rest = run(
            functools.partial(step_kernel, last, two, n_edges),
            [field_shape, (n_gz * n_xy, LANES)] if last else common,
            [] if last else [left(2)],
            *(flags, block_count, field, *stiff, own_lanes, own_high, *prev, local, rim),
            *(got0, got1, *got_edges),
            *(basis if last else []),
        )
        basis.append(field)
        field = field_next
        if not last:
            local, to0, to1, *edges = rest
    basis.append(field)
    sums = lax.all_to_all(rest[0].reshape(n_gz * n_xy, 1, LANES), ("gz", "xy"), 0, 0)
    sums = sums.reshape(n_gz * n_xy, LANES)
    solution_field, residual = call(finish_kernel, [VMEM] * (1 + len(basis)), [field_shape] * 2)(sums, *basis)
    return solution_field[:, None], residual[:, None]


def solution(mesh):
    in_specs = (
        P(None, "gz", "xy", None),
        P("gz", "xy", None),
        P("gz", "xy", None),
        P("gz", "xy", None),
        P("gz", "xy", None),
        P("gz", "xy", None),
        P(None, "gz", "xy", None),
        P("gz", "xy"),
    )
    out_specs = (P(None, "gz", "xy", None), P(None, "gz", "xy", None))
    return jax.shard_map(body, mesh=mesh, in_specs=in_specs, out_specs=out_specs, check_vma=False)
```

```python
import functools

import jax
import jax.numpy as jnp
from jax import lax
from jax.experimental import pallas as pl
from jax.experimental.pallas import tpu as pltpu
from jax.sharding import PartitionSpec as P


BLOCK = 128
ITERS = 3
LANES = 128
GAIN = 0.25
SHIFT = 1.25
F32 = jnp.float32
BF16 = jnp.bfloat16
CHUNK = 256


def swapped(block, axis, first):
    count = lax.axis_size(axis)
    route = []
    for i in range(first, count - 1, 2):
        route += [(i, i + 1), (i + 1, i)]
    return lax.ppermute(block, axis, route) if route else None


def swapped_sections(block, first):
    count, width = lax.axis_size("gz"), lax.axis_size("xy")
    route = []
    for i in range(first, count - 1, 2):
        for j in range(width):
            a, b = i * width + j, (i + 1) * width + j
            route += [(a, b), (b, a)]
    paired = {a for a, _ in route}
    for a in range(0, count * width - 1, 2):
        if a not in paired and a + 1 not in paired and a // width == (a + 1) // width:
            route += [(a, a + 1), (a + 1, a)]
    return lax.ppermute(block, ("gz", "xy"), route)


def split2(x):
    high = x.astype(BF16)
    return high, (x - high.astype(F32)).astype(BF16)


def div_mod(x, d):
    if d & (d - 1) == 0:
        return lax.shift_right_logical(x, jnp.int32(d.bit_length() - 1)), x & (d - 1)
    q = lax.div(x, jnp.int32(d))
    return q, x - q * d


def hi_lo(index, rows, cols):
    row, col = div_mod(index, cols)
    tile, lane = div_mod(col, LANES)
    return tile * rows + row, lane


def row_of(tile, k):
    return tile[k : k + 1, :]


def one_hot(index, size, shift=0):
    at = lax.broadcasted_iota(jnp.int32, (size, LANES), 0) - shift
    return jnp.concatenate(
        [jnp.where(at == row_of(index, k), 1.0, 0.0).astype(BF16) for k in range(index.shape[0])],
        axis=1,
    )


def blend(index, size, first, second):
    at = lax.broadcasted_iota(jnp.int32, (size, LANES), 0)
    out = []
    for k in range(index.shape[0]):
        here = row_of(index, k)
        out.append(
            jnp.where(at == here, row_of(first, k), jnp.where(at == here + 1, row_of(second, k), 0.0))
        )
    return jnp.concatenate(out, axis=1)


def store_lanes(lo, lanes_ref):
    hot = one_hot(lo, LANES)
    lanes_ref[0:LANES, :] = hot
    lanes_ref[LANES : 2 * LANES, :] = hot


def tall(field):
    n = field.shape[1] // LANES
    return jnp.concatenate([field[:, i * LANES : (i + 1) * LANES] for i in range(n)], axis=0)


def wide(stack, rows):
    n = stack.shape[0] // rows
    return jnp.concatenate([stack[i * rows : (i + 1) * rows, :] for i in range(n)], axis=1)


def right_of(field):
    return pltpu.roll(field, field.shape[1] - 1, 1)


def load_left(field, left_ref, sides):
    fields = []
    for c in range(2):
        fields += [field[c], right_of(field[c])] if sides == 2 else [field[c]]
    for i, f in enumerate(fields):
        stack = tall(f)
        high, low = split2(stack)
        n = stack.shape[0]
        left_ref[i * n : (i + 1) * n, 0:LANES] = high
        left_ref[i * n : (i + 1) * n, LANES : 2 * LANES] = low


def as_tiles(rows_of):
    return jnp.concatenate(
        [r[:, i * LANES : (i + 1) * LANES] for r in rows_of for i in range(CHUNK // LANES)], axis=0
    )


def looked_up(left_ref, lanes_ref, high_ref):
    high, slots = high_ref.shape
    stride = left_ref.shape[0] // 2
    found = ([], [])
    for k in range(0, slots, CHUNK):
        mask = high_ref[:, k : k + CHUNK].astype(F32)
        for c in range(2):
            got = jnp.dot(
                left_ref[c * stride : c * stride + high, :],
                lanes_ref[:, k : k + CHUNK],
                preferred_element_type=F32,
            )
            found[c].append(jnp.sum(mask * got, axis=0, keepdims=True))
    return jnp.stack([as_tiles(f) for f in found])


def interpolated(left_ref, lanes_ref, blend_ref):
    high, slots = blend_ref.shape[1:]
    found = ([], [])
    for k in range(0, slots, CHUNK):
        wl = blend_ref[0, :, k : k + CHUNK]
        wr = blend_ref[1, :, k : k + CHUNK]
        for c in range(2):
            got = jnp.dot(
                left_ref[2 * c * high : 2 * (c + 1) * high, :],
                lanes_ref[:, k : k + CHUNK],
                preferred_element_type=F32,
            )
            value = wl * got[:high] + wr * got[high:]
            found[c].append(jnp.sum(value, axis=0, keepdims=True))
    return jnp.stack([as_tiles(f) for f in found])


NT = (((1,), (1,)), ((), ()))


def scaled(mask_ref, tile):
    return jnp.concatenate(
        [mask_ref[:, k * LANES : (k + 1) * LANES] * row_of(tile, k) for k in range(tile.shape[0])],
        axis=1,
    )


def spread_own(values, lanes_ref, high_ref, rows):
    high = high_ref.shape[0]
    result = []
    for c in range(2):
        parts = [scaled(high_ref, part) for part in split2(values[c])]
        out = lax.dot_general(
            jnp.concatenate(parts, axis=0), lanes_ref[0:LANES, :], NT, preferred_element_type=F32
        )
        result.append(wide(out[:high] + out[high:], rows))
    return result


def spread_corners(values, weights, lanes_ref, high_ref, below_ref, rows):
    high = high_ref.shape[0]
    result = []
    for c in range(2):
        parts = []
        for side in range(2):
            for up, down in zip(split2(values[c] * weights[side]), split2(values[c] * weights[2 + side])):
                parts.append(scaled(high_ref, up) + scaled(below_ref, down))
        out = lax.dot_general(
            jnp.concatenate(parts, axis=0), lanes_ref[0:LANES, :], NT, preferred_element_type=F32
        )
        sides = [
            wide(out[p * high : (p + 1) * high] + out[(p + 1) * high : (p + 2) * high], rows)
            for p in (0, 2)
        ]
        result.append(sides[0] + pltpu.roll(sides[1], 1, 1))
    return result


def springs(field, across, down, hold, upper_row, lower_row, rim):
    rows, cols = field.shape
    col = lax.broadcasted_iota(jnp.int32, (rows, cols), 1)
    row = lax.broadcasted_iota(jnp.int32, (rows, cols), 0)
    right = jnp.where(col == cols - 1, 0.0, pltpu.roll(field, cols - 1, 1))
    pull = across * (field - right)
    out = pull - jnp.where(col == 0, 0.0, pltpu.roll(pull, 1, 1))
    lower = jnp.where(row == rows - 1, lower_row, pltpu.roll(field, rows - 1, 0))
    pull = down * (field - lower)
    above = rim * (upper_row - field[0:1, :])
    out = out + pull - jnp.where(row == 0, above, pltpu.roll(pull, 1, 0))
    return out + hold * field


def mark(marks, i):
    return marks[i, 0:1, 0:1]


def pick(flag, a, b):
    return jnp.where(jnp.broadcast_to(flag, a.shape) > 0.5, a, b)


def edges_of(get_row, rows, even_b, two):
    first = [get_row(c, 0) for c in range(2)]
    last = [get_row(c, rows - 1) for c in range(2)]
    out = [jnp.concatenate([pick(even_b, last[c], first[c]) for c in range(2)], axis=0)]
    if two:
        out.append(jnp.concatenate([pick(even_b, first[c], last[c]) for c in range(2)], axis=0))
    return out


def pack_kernel(two, flags, count, field, down, hold, source, target, weights, *refs):
    rows, cols = down.shape
    even_b = jnp.full((1, 1), 1 - flags[1]).astype(F32)
    has_next = flags[2]
    nb = source.shape[0]
    n_edges = 2 if two else 1
    pack, edges = refs[0], refs[1 : 1 + n_edges]
    last_down, hold_out, marks, ids, held, sems = refs[1 + n_edges :]
    pairs = [(field.at[c], pack.at[:, c * cols : (c + 1) * cols]) for c in range(2)]
    pairs += [(down, last_down), (source, ids.at[0]), (target, ids.at[1]), (weights, held)]
    pairs += [(hold, hold_out)]
    copies = [pltpu.make_async_copy(a, b, sems.at[i]) for i, (a, b) in enumerate(pairs)]
    for copy in copies:
        copy.start()
    for copy in copies:
        copy.wait()
    block = lax.broadcasted_iota(jnp.int32, (nb, LANES), 0)
    live = jnp.where(block * LANES < count[0, 0] * BLOCK * has_next, 1.0, 0.0)
    parts = [ids[0].astype(F32), ids[1].astype(F32)] + [held[q] * live for q in range(4)]
    for i in range(2):
        marks[i] = jnp.full((nb, LANES), 1 - flags[i]).astype(F32)
    marks[2] = jnp.full((nb, LANES), flags[3]).astype(F32)
    marks[3] = live
    for i, part in enumerate(parts):
        pack[:nb, 2 * cols + i * LANES : 2 * cols + (i + 1) * LANES] = part
    messages = edges_of(lambda c, r: pack[r : r + 1, c * cols : (c + 1) * cols], rows, even_b, two)
    for message, edge in zip(messages, edges):
        edge[0:2, :] = message
        edge[2:3, :] = last_down[rows - 1 : rows, :]


def halves(flags, edge_refs):
    even_b = mark(flags, 1)
    zero = edge_refs[0][...]
    if len(edge_refs) == 2:
        other = edge_refs[1][...]
    else:
        other = jnp.zeros_like(zero)
    return pick(even_b, other, zero), pick(even_b, zero, other)


def spring_image(field, across, down, hold, above, below, rim):
    return [
        springs(
            field[c], across[...], down[...], hold[...], above[c : c + 1], below[c : c + 1], rim
        )
        for c in range(2)
    ]


def early_kernel(flags, field_ref, across, down, hold, source, target, weights, *refs):
    edge_refs = refs[:-8]
    base, own_ref, rim_ref, own_lanes, own_high, next_lanes, next_blend, left = refs[-8:]
    rows, cols = across.shape
    size = own_high.shape[0]
    field = [field_ref[0], field_ref[1]]
    above, below = halves(flags, edge_refs)
    image = spring_image(field, across, down, hold, above, below, above[2:3, :])
    for c in range(2):
        base[c] = image[c]
    rim_ref[...] = above[2:3, :]
    hi, lo = hi_lo(source[...], rows, cols)
    store_lanes(lo, own_lanes)
    own_high[...] = one_hot(hi, size)
    hi, lo = hi_lo(target[...], rows, cols)
    store_lanes(lo, next_lanes)
    for side in range(2):
        next_blend[side] = blend(hi, size, weights[side], weights[2 + side])
    load_left(field, left, 1)
    own_ref[...] = looked_up(left, own_lanes, own_high)


def send_on(even, even_b, two, field, own_tables, prev_tables, left, local_ref, send0, send1, *edges):
    own_lanes, own_high = own_tables
    prev_lanes, prev_blend = prev_tables
    load_left(field, left, 2)
    own = looked_up(left, own_lanes, own_high)
    mid = interpolated(left, prev_lanes, prev_blend)
    local_ref[0] = own
    local_ref[1] = mid
    send0[...] = pick(even, own, mid)
    send1[...] = pick(even, mid, own)
    messages = edges_of(lambda c, r: field[c][r : r + 1, :], field[0].shape[0], even_b, two)
    for message, edge in zip(messages, edges):
        edge[...] = message


def stepped(field_ref, image):
    return [GAIN * image[c] - SHIFT * field_ref[c] for c in range(2)]


def first_kernel(
    two, flags, field_ref, base, own, own_lanes, own_high, next_lanes, next_blend, got0, got1, *refs
):
    refs, (left, next_left, prev_left, lanes, mask) = refs[:-5], refs[-5:]
    out, local_ref, send0, send1, *edges = refs[:-5]
    prev_weights, prev_lanes, prev_high, prev_below, prev_blend = refs[-5:]
    even, even_b = mark(flags, 0), mark(flags, 1)
    nb = own.shape[1]
    rows, cols = field_ref.shape[1:]
    size = own_high.shape[0]
    slot = lambda ref, i: ref[:nb, 2 * cols + i * LANES : 2 * cols + (i + 1) * LANES]
    prev = [pick(even, slot(got1, i), slot(got0, i)) for i in range(6)]
    comp = lambda ref, c: ref[:, c * cols : (c + 1) * cols]
    weights = [w * flags[2] for w in prev[2:]]
    for q in range(4):
        prev_weights[q] = weights[q]
    hi, lo = hi_lo(prev[1].astype(jnp.int32), rows, cols)
    store_lanes(lo, prev_lanes)
    prev_high[...] = one_hot(hi, size)
    prev_below[...] = one_hot(hi, size, 1)
    for side in range(2):
        prev_blend[side] = blend(hi, size, weights[side], weights[2 + side])
    load_left([field_ref[0], field_ref[1]], left, 2)
    mid = interpolated(left, prev_lanes, prev_blend)
    load_left([pick(even, comp(got0, c), comp(got1, c)) for c in range(2)], next_left, 2)
    got_next = interpolated(next_left, next_lanes, next_blend)
    hi, lo = hi_lo(prev[0].astype(jnp.int32), rows, cols)
    store_lanes(lo, lanes)
    mask[...] = one_hot(hi, size)
    load_left([pick(even, comp(got1, c), comp(got0, c)) for c in range(2)], prev_left, 1)
    got_prev = looked_up(prev_left, lanes, mask)
    live = flags[3]
    pulled = spread_own([live * (own[c] - got_next[c]) for c in range(2)], own_lanes, own_high, rows)
    error = [mid[c] - got_prev[c] for c in range(2)]
    pushed = spread_corners(error, weights, prev_lanes, prev_high, prev_below, rows)
    after = stepped(field_ref, [base[c] + pulled[c] + pushed[c] for c in range(2)])
    for c in range(2):
        out[c] = after[c]
    send_on(
        even,
        even_b,
        two,
        after,
        (own_lanes, own_high),
        (prev_lanes, prev_blend),
        left,
        local_ref,
        send0,
        send1,
        *edges,
    )


def moments_of(pairs):
    lane = lax.broadcasted_iota(jnp.int32, (1, LANES), 1)
    total = jnp.zeros((1, LANES), F32)
    for i, (u, w) in enumerate(pairs):
        s = u[0] * w[0] + u[1] * w[1]
        s = jnp.sum(jnp.sum(s, axis=0, keepdims=True), axis=1, keepdims=True)
        total = total + jnp.where(lane == i, s, 0.0)
    return total


def step_kernel(
    last,
    two,
    n_edges,
    flags,
    field_ref,
    across,
    down,
    hold,
    own_lanes,
    own_high,
    prev_weights,
    prev_lanes,
    prev_high,
    prev_below,
    prev_blend,
    local,
    rim,
    got0,
    got1,
    *refs,
):
    refs = list(refs)
    edge_refs = [refs.pop(0) for _ in range(n_edges)]
    earlier = [refs.pop(0) for _ in range(ITERS - 1)] if last else []
    out = refs.pop(0)
    even, even_b = mark(flags, 0), mark(flags, 1)
    rows, _ = across.shape
    field = [field_ref[0], field_ref[1]]
    live = flags[3]
    got_next = pick(even, got0[...], got1[...])
    got_prev = pick(even, got1[...], got0[...])
    pulled = spread_own([live * (local[0, c] - got_next[c]) for c in range(2)], own_lanes, own_high, rows)
    error = [local[1, c] - got_prev[c] for c in range(2)]
    weights = [prev_weights[q] for q in range(4)]
    pushed = spread_corners(error, weights, prev_lanes, prev_high, prev_below, rows)
    above, below = halves(flags, edge_refs)
    image = spring_image(field, across, down, hold, above, below, rim[...])
    after = stepped(field_ref, [image[c] + pulled[c] + pushed[c] for c in range(2)])
    for c in range(2):
        out[c] = after[c]
    if last:
        basis = [(ref[0], ref[1]) for ref in earlier] + [field, after]
        total = moments_of([(basis[i // 2], basis[i - i // 2]) for i in range(2 * ITERS)])
        sums = refs.pop(0)
        sums[...] = jnp.broadcast_to(total, sums.shape)
    else:
        messages, left = refs[:-1], refs[-1]
        send_on(even, even_b, two, after, (own_lanes, own_high), (prev_lanes, prev_blend), left, *messages)


def conjugate(moments):
    def apply(p):
        shifted = [None] + p
        return [
            (SHIFT * p[k] if k < len(p) else 0.0) * (1.0 / GAIN)
            + ((1.0 / GAIN) * shifted[k] if k else 0.0)
            for k in range(len(p) + 1)
        ]

    def product(p, q):
        return sum(p[i] * q[j] * moments[i + j] for i in range(len(p)) for j in range(len(q)))

    def plus(p, factor, q):
        size = max(len(p), len(q))
        pad = lambda a: a + [None] * (size - len(a))
        out = []
        for a, b in zip(pad(p), pad(q)):
            out.append(factor * b if a is None else a if b is None else a + factor * b)
        return out

    one = jnp.ones_like(moments[0])
    solution_field, residual, direction = [], [one], [one]
    norm_now = moments[0]
    for step in range(ITERS):
        image = apply(direction)
        alpha = norm_now / product(direction, image)
        solution_field = plus(solution_field, alpha, direction)
        residual = plus(residual, -alpha, image)
        if step + 1 < ITERS:
            norm_next = product(residual, residual)
            direction = plus(residual, norm_next / norm_now, direction)
            norm_now = norm_next
    return solution_field, residual


def finish_kernel(sums, *refs):
    basis, (solution_ref, residual_ref) = refs[: ITERS + 1], refs[ITERS + 1 :]
    total = jnp.sum(sums[...], axis=0, keepdims=True)
    lane = lax.broadcasted_iota(jnp.int32, (1, LANES), 1)
    moments = [
        jnp.sum(jnp.where(lane == i, total, 0.0), axis=1, keepdims=True) for i in range(2 * ITERS)
    ]
    solution_field, residual = conjugate(moments)
    for c in range(2):
        values = [ref[c] for ref in basis]
        solution_ref[c] = sum(a * v for a, v in zip(solution_field, values))
        residual_ref[c] = sum(a * v for a, v in zip(residual, values))


VMEM = pl.BlockSpec(memory_space=pltpu.VMEM)
SMEM = pl.BlockSpec(memory_space=pltpu.SMEM)
HBM = pl.BlockSpec(memory_space=pltpu.HBM)


def call(kernel, in_specs, shapes, scratch=()):
    shapes = [s if isinstance(s, jax.ShapeDtypeStruct) else jax.ShapeDtypeStruct(s, F32) for s in shapes]
    return pl.pallas_call(
        kernel,
        in_specs=in_specs,
        out_specs=[VMEM] * len(shapes),
        out_shape=shapes,
        scratch_shapes=list(scratch),
        compiler_params=pltpu.CompilerParams(vmem_limit_bytes=48 * 1024 * 1024),
    )


def body(
    right_side,
    stiff_across,
    stiff_down,
    anchor,
    source_node,
    target_cell,
    corner_weight,
    block_count,
):
    rows, cols = stiff_across.shape[1:]
    rhs = right_side[:, 0]
    across, down, hold = stiff_across[0], stiff_down[0], anchor[0]
    slots = source_node.shape[2]
    nb = slots // LANES
    source = source_node.reshape(nb, LANES)
    target = target_cell.reshape(nb, LANES)
    weights = corner_weight.reshape(4, nb, LANES)
    n_gz, n_xy = lax.axis_size("gz"), lax.axis_size("xy")
    at_gz, at_xy = lax.axis_index("gz"), lax.axis_index("xy")
    two = n_xy > 2
    flags = jnp.stack([at_gz % 2, at_xy % 2, (at_gz < n_gz - 1).astype(jnp.int32), (at_gz > 0).astype(jnp.int32)]).astype(jnp.int32)
    n_edges = 2 if two else 1

    in_hbm = lambda *arrays: [pltpu.with_memory_space_constraint(a, pltpu.HBM) for a in arrays]
    pack, *rest = call(
        functools.partial(pack_kernel, two),
        [SMEM, SMEM] + [HBM] * 6,
        [(rows, 2 * cols + 6 * LANES)] + [(4, cols)] * n_edges + [(rows, cols)] * 2 + [(4, nb, LANES)],
        [
            pltpu.VMEM((2, nb, LANES), jnp.int32),
            pltpu.VMEM((4, nb, LANES), F32),
            pltpu.SemaphoreType.DMA((7,)),
        ],
    )(flags, block_count, *in_hbm(rhs, down, hold, source, target, weights))
    edges, (down, hold, marks) = rest[:n_edges], rest[n_edges:]

    def exchange(to0, to1, edges):
        got1 = swapped_sections(to1, 1)
        got0 = swapped_sections(to0, 0)
        got_edges = []
        for i, edge in enumerate(edges):
            got_edges.append(swapped(edge, "xy", i))
        return got0, got1, got_edges

    field_shape = (2, rows, cols)
    message = (2, nb, LANES)
    size = rows * cols // LANES
    common = [field_shape, (2,) + message, message, message] + [(2, cols)] * n_edges
    table = lambda *shape: jax.ShapeDtypeStruct(shape, BF16)
    left = lambda sides: pltpu.VMEM((2 * sides * size, 2 * LANES), BF16)
    lanes, mask, blends = (2 * LANES, slots), (size, slots), (2, size, slots)
    run = lambda kernel, shapes, scratch, *args: call(kernel, [VMEM] * len(args), shapes, scratch)(*args)
    stiff = (across, down, hold)
    basis = [rhs]

    got0, got1, got_edges = exchange(pack, pack, edges)
    base, own, rim, own_lanes, own_high, next_lanes, next_blend = call(
        early_kernel,
        [VMEM] * (8 + n_edges),
        [field_shape, message, (1, cols), table(*lanes), table(*mask), table(*lanes), blends],
        [left(1)],
    )(marks, rhs, *stiff, source, target, weights, *got_edges)
    field, local, to0, to1, *rest = run(
        functools.partial(first_kernel, two),
        common + [(4, nb, LANES), table(*lanes), table(*mask), table(*mask), blends],
        [left(2), left(2), left(1), pltpu.VMEM(lanes, BF16), pltpu.VMEM(mask, BF16)],
        *(marks, rhs, base, own, own_lanes, own_high, next_lanes, next_blend, got0, got1),
    )
    edges, prev = rest[:n_edges], rest[n_edges:]

    for step in range(1, ITERS):
        last = step == ITERS - 1
        got0, got1, got_edges = exchange(to0, to1, edges)
        field_next, *rest = run(
            functools.partial(step_kernel, last, two, n_edges),
            [field_shape, (n_gz * n_xy, LANES)] if last else common,
            [] if last else [left(2)],
            *(marks, field, *stiff, own_lanes, own_high, *prev, local, rim),
            *(got0, got1, *got_edges),
            *(basis if last else []),
        )
        basis.append(field)
        field = field_next
        if not last:
            local, to0, to1, *edges = rest
    basis.append(field)
    sums = lax.all_to_all(rest[0].reshape(n_gz * n_xy, 1, LANES), ("gz", "xy"), 0, 0)
    sums = sums.reshape(n_gz * n_xy, LANES)
    solution_field, residual = call(finish_kernel, [VMEM] * (1 + len(basis)), [field_shape] * 2)(sums, *basis)
    return solution_field[:, None], residual[:, None]


def solution(mesh):
    in_specs = (
        P(None, "gz", "xy", None),
        P("gz", "xy", None),
        P("gz", "xy", None),
        P("gz", "xy", None),
        P("gz", "xy", None),
        P("gz", "xy", None),
        P(None, "gz", "xy", None),
        P("gz", "xy"),
    )
    out_specs = (P(None, "gz", "xy", None), P(None, "gz", "xy", None))
    return jax.shard_map(body, mesh=mesh, in_specs=in_specs, out_specs=out_specs, check_vma=False)
```

```python
import functools

import jax
import jax.numpy as jnp
from jax import lax
from jax.experimental import pallas as pl
from jax.experimental.pallas import tpu as pltpu
from jax.sharding import PartitionSpec as P


BLOCK = 128
ITERS = 3
LANES = 128
GAIN = 0.25
SHIFT = 1.25
F32 = jnp.float32
BF16 = jnp.bfloat16
CHUNK = 256


def swapped(block, axis, first):
    count = lax.axis_size(axis)
    route = []
    for i in range(first, count - 1, 2):
        route += [(i, i + 1), (i + 1, i)]
    return lax.ppermute(block, axis, route) if route else None


def swapped_sections(block, first):
    count, width = lax.axis_size("gz"), lax.axis_size("xy")
    route = []
    for i in range(first, count - 1, 2):
        for j in range(width):
            a, b = i * width + j, (i + 1) * width + j
            route += [(a, b), (b, a)]
    paired = {a for a, _ in route}
    for a in range(0, count * width - 1, 2):
        if a not in paired and a + 1 not in paired and a // width == (a + 1) // width:
            route += [(a, a + 1), (a + 1, a)]
    return lax.ppermute(block, ("gz", "xy"), route)


def split2(x):
    high = x.astype(BF16)
    return high, (x - high.astype(F32)).astype(BF16)


def div_mod(x, d):
    if d & (d - 1) == 0:
        return lax.shift_right_logical(x, jnp.int32(d.bit_length() - 1)), x & (d - 1)
    q = lax.div(x, jnp.int32(d))
    return q, x - q * d


def hi_lo(index, rows, cols):
    row, col = div_mod(index, cols)
    tile, lane = div_mod(col, LANES)
    return tile * rows + row, lane


def row_of(tile, k):
    return tile[k : k + 1, :]


def one_hot(index, size, shift=0):
    at = lax.broadcasted_iota(jnp.int32, (size, LANES), 0) - shift
    return jnp.concatenate(
        [jnp.where(at == row_of(index, k), 1.0, 0.0).astype(BF16) for k in range(index.shape[0])],
        axis=1,
    )


def blend(index, size, first, second):
    at = lax.broadcasted_iota(jnp.int32, (size, LANES), 0)
    out = []
    for k in range(index.shape[0]):
        here = row_of(index, k)
        out.append(
            jnp.where(at == here, row_of(first, k), jnp.where(at == here + 1, row_of(second, k), 0.0))
        )
    return jnp.concatenate(out, axis=1)


def store_lanes(lo, lanes_ref):
    hot = one_hot(lo, LANES)
    lanes_ref[0:LANES, :] = hot
    lanes_ref[LANES : 2 * LANES, :] = hot


def tall(field):
    n = field.shape[1] // LANES
    return jnp.concatenate([field[:, i * LANES : (i + 1) * LANES] for i in range(n)], axis=0)


def wide(stack, rows):
    n = stack.shape[0] // rows
    return jnp.concatenate([stack[i * rows : (i + 1) * rows, :] for i in range(n)], axis=1)


def right_of(field):
    return pltpu.roll(field, field.shape[1] - 1, 1)


def load_left(field, left_ref, sides):
    fields = []
    for c in range(2):
        fields += [field[c], right_of(field[c])] if sides == 2 else [field[c]]
    for i, f in enumerate(fields):
        stack = tall(f)
        high, low = split2(stack)
        n = stack.shape[0]
        left_ref[i * n : (i + 1) * n, 0:LANES] = high
        left_ref[i * n : (i + 1) * n, LANES : 2 * LANES] = low


def as_tiles(rows_of):
    return jnp.concatenate(
        [r[:, i * LANES : (i + 1) * LANES] for r in rows_of for i in range(CHUNK // LANES)], axis=0
    )


def looked_up(left_ref, lanes_ref, high_ref):
    high, slots = high_ref.shape
    stride = left_ref.shape[0] // 2
    found = ([], [])
    for k in range(0, slots, CHUNK):
        mask = high_ref[:, k : k + CHUNK].astype(F32)
        for c in range(2):
            got = jnp.dot(
                left_ref[c * stride : c * stride + high, :],
                lanes_ref[:, k : k + CHUNK],
                preferred_element_type=F32,
            )
            found[c].append(jnp.sum(mask * got, axis=0, keepdims=True))
    return jnp.stack([as_tiles(f) for f in found])


def interpolated(left_ref, lanes_ref, blend_ref):
    high, slots = blend_ref.shape[1:]
    found = ([], [])
    for k in range(0, slots, CHUNK):
        wl = blend_ref[0, :, k : k + CHUNK]
        wr = blend_ref[1, :, k : k + CHUNK]
        for c in range(2):
            got = jnp.dot(
                left_ref[2 * c * high : 2 * (c + 1) * high, :],
                lanes_ref[:, k : k + CHUNK],
                preferred_element_type=F32,
            )
            value = wl * got[:high] + wr * got[high:]
            found[c].append(jnp.sum(value, axis=0, keepdims=True))
    return jnp.stack([as_tiles(f) for f in found])


NT = (((1,), (1,)), ((), ()))


def scaled(mask_ref, tile):
    return jnp.concatenate(
        [mask_ref[:, k * LANES : (k + 1) * LANES] * row_of(tile, k) for k in range(tile.shape[0])],
        axis=1,
    )


def spread_own(values, lanes_ref, high_ref, rows):
    high = high_ref.shape[0]
    result = []
    for c in range(2):
        parts = [scaled(high_ref, part) for part in split2(values[c])]
        out = lax.dot_general(
            jnp.concatenate(parts, axis=0), lanes_ref[0:LANES, :], NT, preferred_element_type=F32
        )
        result.append(wide(out[:high] + out[high:], rows))
    return result


def spread_corners(values, weights, lanes_ref, high_ref, below_ref, rows):
    high = high_ref.shape[0]
    result = []
    for c in range(2):
        parts = []
        for side in range(2):
            for up, down in zip(split2(values[c] * weights[side]), split2(values[c] * weights[2 + side])):
                parts.append(scaled(high_ref, up) + scaled(below_ref, down))
        out = lax.dot_general(
            jnp.concatenate(parts, axis=0), lanes_ref[0:LANES, :], NT, preferred_element_type=F32
        )
        sides = [
            wide(out[p * high : (p + 1) * high] + out[(p + 1) * high : (p + 2) * high], rows)
            for p in (0, 2)
        ]
        result.append(sides[0] + pltpu.roll(sides[1], 1, 1))
    return result


def springs(field, across, down, hold, upper_row, lower_row, rim):
    rows, cols = field.shape
    col = lax.broadcasted_iota(jnp.int32, (rows, cols), 1)
    row = lax.broadcasted_iota(jnp.int32, (rows, cols), 0)
    right = jnp.where(col == cols - 1, 0.0, pltpu.roll(field, cols - 1, 1))
    pull = across * (field - right)
    out = pull - jnp.where(col == 0, 0.0, pltpu.roll(pull, 1, 1))
    lower = jnp.where(row == rows - 1, lower_row, pltpu.roll(field, rows - 1, 0))
    pull = down * (field - lower)
    above = rim * (upper_row - field[0:1, :])
    out = out + pull - jnp.where(row == 0, above, pltpu.roll(pull, 1, 0))
    return out + hold * field


def mark(marks, i):
    return marks[i, 0:1, 0:1]


def pick(flag, a, b):
    return jnp.where(jnp.broadcast_to(flag, a.shape) > 0.5, a, b)


def edges_of(get_row, rows, even_b, two):
    first = [get_row(c, 0) for c in range(2)]
    last = [get_row(c, rows - 1) for c in range(2)]
    out = [jnp.concatenate([pick(even_b, last[c], first[c]) for c in range(2)], axis=0)]
    if two:
        out.append(jnp.concatenate([pick(even_b, first[c], last[c]) for c in range(2)], axis=0))
    return out


def prepare_kernel(two, count, field, across, down, hold, source, target, weights, *refs):
    outs, (left, ids, held, sems) = refs[:-4], refs[-4:]
    field_out, across_out, down_out, hold_out, up, marks, own_lanes, own_high, *edges = outs
    pairs = [(source, ids.at[0]), (field, field_out), (down, down_out)]
    pairs += [(target, ids.at[1]), (weights, held), (across, across_out), (hold, hold_out)]
    copies = [pltpu.make_async_copy(a, b, sems.at[i]) for i, (a, b) in enumerate(pairs)]
    for copy in copies:
        copy.start()
    rows, cols = across_out.shape
    nb, size = ids.shape[1], own_high.shape[0]
    at_gz, at_xy = lax.axis_index("gz"), lax.axis_index("xy")
    as_mark = lambda flag: jnp.full((nb, LANES), flag.astype(jnp.int32)).astype(F32)
    copies[0].wait()
    hi, lo = hi_lo(ids[0], rows, cols)
    store_lanes(lo, own_lanes)
    own_high[...] = one_hot(hi, size)
    copies[1].wait()
    load_left([field_out[0], field_out[1]], left, 1)
    own = looked_up(left, own_lanes, own_high)
    for copy in copies[2:]:
        copy.wait()
    has_next = (at_gz < lax.axis_size("gz") - 1).astype(jnp.int32)
    block = lax.broadcasted_iota(jnp.int32, (nb, LANES), 0)
    live = jnp.where(block * LANES < count[0, 0] * BLOCK * has_next, 1.0, 0.0)
    marks[0] = as_mark(1 - lax.rem(at_gz, 2))
    marks[1] = as_mark(1 - lax.rem(at_xy, 2))
    marks[2] = as_mark(at_gz > 0)
    marks[3] = live
    parts = [own[0], own[1], ids[1].astype(F32)] + [held[q] * live for q in range(4)]
    for i, part in enumerate(parts):
        up[:, i * LANES : (i + 1) * LANES] = part
    even_b = mark(marks, 1)
    messages = edges_of(lambda c, r: field_out[c, r : r + 1, :], rows, even_b, two)
    for message, edge in zip(messages, edges):
        edge[0:2, :] = message
        edge[2:3, :] = down_out[rows - 1 : rows, :]


def tile_of(up, i):
    return up[:, i * LANES : (i + 1) * LANES]


def halves(flags, edge_refs):
    even_b = mark(flags, 1)
    zero = edge_refs[0][...]
    if len(edge_refs) == 2:
        other = edge_refs[1][...]
    else:
        other = jnp.zeros_like(zero)
    return pick(even_b, other, zero), pick(even_b, zero, other)


def spring_image(field, across, down, hold, above, below, rim):
    return [
        springs(
            field[c], across[...], down[...], hold[...], above[c : c + 1], below[c : c + 1], rim
        )
        for c in range(2)
    ]


def early_kernel(flags, field_ref, across, down, hold, up, *refs):
    edge_refs, (base, rim_ref, next_lanes, next_blend) = refs[:-4], refs[-4:]
    rows, cols = across.shape
    field = [field_ref[0], field_ref[1]]
    above, below = halves(flags, edge_refs)
    image = spring_image(field, across, down, hold, above, below, above[2:3, :])
    for c in range(2):
        base[c] = image[c]
    rim_ref[...] = above[2:3, :]
    hi, lo = hi_lo(tile_of(up, 2).astype(jnp.int32), rows, cols)
    store_lanes(lo, next_lanes)
    for side in range(2):
        next_blend[side] = blend(hi, next_blend.shape[1], tile_of(up, 3 + side), tile_of(up, 5 + side))


def send_on(even, even_b, two, field, own_tables, prev_tables, left, local_ref, send0, send1, *edges):
    own_lanes, own_high = own_tables
    prev_lanes, prev_blend = prev_tables
    load_left(field, left, 2)
    own = looked_up(left, own_lanes, own_high)
    mid = interpolated(left, prev_lanes, prev_blend)
    local_ref[0] = own
    local_ref[1] = mid
    send0[...] = pick(even, own, mid)
    send1[...] = pick(even, mid, own)
    messages = edges_of(lambda c, r: field[c][r : r + 1, :], field[0].shape[0], even_b, two)
    for message, edge in zip(messages, edges):
        edge[...] = message


def stepped(field_ref, image):
    return [GAIN * image[c] - SHIFT * field_ref[c] for c in range(2)]


def first_kernel(
    two, flags, field_ref, base, up, own_lanes, own_high, next_lanes, next_blend, next_field, up0, up1, *refs
):
    refs, (left, next_left) = refs[:-2], refs[-2:]
    out, local_ref, send0, send1, *edges = refs[:-5]
    prev_weights, prev_lanes, prev_high, prev_below, prev_blend = refs[-5:]
    even, even_b = mark(flags, 0), mark(flags, 1)
    rows, cols = field_ref.shape[1:]
    size = own_high.shape[0]
    got_up = pick(even, up1[...], up0[...])
    weights = [tile_of(got_up, 3 + q) * flags[2] for q in range(4)]
    for q in range(4):
        prev_weights[q] = weights[q]
    hi, lo = hi_lo(tile_of(got_up, 2).astype(jnp.int32), rows, cols)
    store_lanes(lo, prev_lanes)
    prev_high[...] = one_hot(hi, size)
    prev_below[...] = one_hot(hi, size, 1)
    for side in range(2):
        prev_blend[side] = blend(hi, size, weights[side], weights[2 + side])
    load_left([field_ref[0], field_ref[1]], left, 2)
    mid = interpolated(left, prev_lanes, prev_blend)
    load_left([next_field[0], next_field[1]], next_left, 2)
    got_next = interpolated(next_left, next_lanes, next_blend)
    own = [tile_of(up, c) for c in range(2)]
    got_prev = [tile_of(got_up, c) for c in range(2)]
    live = flags[3]
    pulled = spread_own([live * (own[c] - got_next[c]) for c in range(2)], own_lanes, own_high, rows)
    error = [mid[c] - got_prev[c] for c in range(2)]
    pushed = spread_corners(error, weights, prev_lanes, prev_high, prev_below, rows)
    after = stepped(field_ref, [base[c] + pulled[c] + pushed[c] for c in range(2)])
    for c in range(2):
        out[c] = after[c]
    send_on(
        even,
        even_b,
        two,
        after,
        (own_lanes, own_high),
        (prev_lanes, prev_blend),
        left,
        local_ref,
        send0,
        send1,
        *edges,
    )


def moments_of(pairs, start=0):
    lane = lax.broadcasted_iota(jnp.int32, (1, LANES), 1)
    total = jnp.zeros((1, LANES), F32)
    for i, (u, w) in enumerate(pairs):
        s = u[0] * w[0] + u[1] * w[1]
        s = jnp.sum(jnp.sum(s, axis=0, keepdims=True), axis=1, keepdims=True)
        total = total + jnp.where(lane == start + i, s, 0.0)
    return total


def between_kernel(last, n_edges, flags, field_ref, across, down, hold, rim, *refs):
    refs = list(refs)
    edge_refs = [refs.pop(0) for _ in range(n_edges)]
    earlier = [refs.pop(0) for _ in range(ITERS - 1)] if last else []
    field = [field_ref[0], field_ref[1]]
    above, below = halves(flags, edge_refs)
    image = spring_image(field, across, down, hold, above, below, rim[...])
    base = refs.pop(0)
    for c in range(2):
        base[c] = image[c]
    if last:
        basis = [(ref[0], ref[1]) for ref in earlier] + [field]
        refs.pop(0)[...] = moments_of([(basis[i // 2], basis[i - i // 2]) for i in range(2 * ITERS - 1)])


def step_kernel(
    last,
    two,
    flags,
    field_ref,
    base,
    own_lanes,
    own_high,
    prev_weights,
    prev_lanes,
    prev_high,
    prev_below,
    prev_blend,
    local,
    got0,
    got1,
    *refs,
):
    refs = list(refs)
    partial = refs.pop(0) if last else None
    out = refs.pop(0)
    even, even_b = mark(flags, 0), mark(flags, 1)
    rows = field_ref.shape[1]
    live = flags[3]
    got_next = pick(even, got0[...], got1[...])
    got_prev = pick(even, got1[...], got0[...])
    pulled = spread_own([live * (local[0, c] - got_next[c]) for c in range(2)], own_lanes, own_high, rows)
    error = [local[1, c] - got_prev[c] for c in range(2)]
    weights = [prev_weights[q] for q in range(4)]
    pushed = spread_corners(error, weights, prev_lanes, prev_high, prev_below, rows)
    after = stepped(field_ref, [base[c] + pulled[c] + pushed[c] for c in range(2)])
    for c in range(2):
        out[c] = after[c]
    if last:
        lane = lax.broadcasted_iota(jnp.int32, (1, LANES), 1)
        end = 2 * ITERS - 1
        newest = moments_of([((field_ref[0], field_ref[1]), after)], end)
        sums = refs.pop(0)
        sums[...] = jnp.broadcast_to(jnp.where(lane == end, newest, partial[...]), sums.shape)
    else:
        messages, left = refs[:-1], refs[-1]
        send_on(even, even_b, two, after, (own_lanes, own_high), (prev_lanes, prev_blend), left, *messages)


def conjugate(moments):
    def apply(p):
        shifted = [None] + p
        return [
            (SHIFT * p[k] if k < len(p) else 0.0) * (1.0 / GAIN)
            + ((1.0 / GAIN) * shifted[k] if k else 0.0)
            for k in range(len(p) + 1)
        ]

    def product(p, q):
        return sum(p[i] * q[j] * moments[i + j] for i in range(len(p)) for j in range(len(q)))

    def plus(p, factor, q):
        size = max(len(p), len(q))
        pad = lambda a: a + [None] * (size - len(a))
        out = []
        for a, b in zip(pad(p), pad(q)):
            out.append(factor * b if a is None else a if b is None else a + factor * b)
        return out

    one = jnp.ones_like(moments[0])
    solution_field, residual, direction = [], [one], [one]
    norm_now = moments[0]
    for step in range(ITERS):
        image = apply(direction)
        alpha = norm_now / product(direction, image)
        solution_field = plus(solution_field, alpha, direction)
        residual = plus(residual, -alpha, image)
        if step + 1 < ITERS:
            norm_next = product(residual, residual)
            direction = plus(residual, norm_next / norm_now, direction)
            norm_now = norm_next
    return solution_field, residual


def finish_kernel(sums, *refs):
    basis, (solution_ref, residual_ref) = refs[: ITERS + 1], refs[ITERS + 1 :]
    total = jnp.sum(sums[...], axis=0, keepdims=True)
    lane = lax.broadcasted_iota(jnp.int32, (1, LANES), 1)
    moments = [
        jnp.sum(jnp.where(lane == i, total, 0.0), axis=1, keepdims=True) for i in range(2 * ITERS)
    ]
    solution_field, residual = conjugate(moments)
    for c in range(2):
        values = [ref[c] for ref in basis]
        solution_ref[c] = sum(a * v for a, v in zip(solution_field, values))
        residual_ref[c] = sum(a * v for a, v in zip(residual, values))


VMEM = pl.BlockSpec(memory_space=pltpu.VMEM)
SMEM = pl.BlockSpec(memory_space=pltpu.SMEM)
HBM = pl.BlockSpec(memory_space=pltpu.HBM)


def call(kernel, in_specs, shapes, scratch=()):
    shapes = [s if isinstance(s, jax.ShapeDtypeStruct) else jax.ShapeDtypeStruct(s, F32) for s in shapes]
    return pl.pallas_call(
        kernel,
        in_specs=in_specs,
        out_specs=[VMEM] * len(shapes),
        out_shape=shapes,
        scratch_shapes=list(scratch),
        compiler_params=pltpu.CompilerParams(vmem_limit_bytes=48 * 1024 * 1024),
    )


def body(
    right_side,
    stiff_across,
    stiff_down,
    anchor,
    source_node,
    target_cell,
    corner_weight,
    block_count,
):
    rows, cols = stiff_across.shape[1:]
    rhs = right_side[:, 0]
    across, down, hold = stiff_across[0], stiff_down[0], anchor[0]
    slots = source_node.shape[2]
    nb = slots // LANES
    source = source_node.reshape(nb, LANES)
    target = target_cell.reshape(nb, LANES)
    weights = corner_weight.reshape(4, nb, LANES)
    n_gz, n_xy = lax.axis_size("gz"), lax.axis_size("xy")
    two = n_xy > 2
    n_edges = 2 if two else 1

    def exchange(to0, to1, edges):
        got1 = swapped_sections(to1, 1)
        got0 = swapped_sections(to0, 0)
        got_edges = []
        for i, edge in enumerate(edges):
            got_edges.append(swapped(edge, "xy", i))
        return got0, got1, got_edges

    field_shape = (2, rows, cols)
    message = (2, nb, LANES)
    size = rows * cols // LANES
    common = [field_shape, (2,) + message, message, message] + [(2, cols)] * n_edges
    table = lambda *shape: jax.ShapeDtypeStruct(shape, BF16)
    left = lambda sides: pltpu.VMEM((2 * sides * size, 2 * LANES), BF16)
    lanes, mask, blends = (2 * LANES, slots), (size, slots), (2, size, slots)
    run = lambda kernel, shapes, scratch, *args: call(kernel, [VMEM] * len(args), shapes, scratch)(*args)
    next_field = lax.ppermute(rhs, "gz", [(i, (i - 1) % n_gz) for i in range(n_gz)])
    in_hbm = lambda *arrays: [pltpu.with_memory_space_constraint(a, pltpu.HBM) for a in arrays]
    grid = (rows, cols)
    rhs, across, down, hold, up, marks, own_lanes, own_high, *edges = call(
        functools.partial(prepare_kernel, two),
        [SMEM] + [HBM] * 7,
        [field_shape, grid, grid, grid, (nb, 7 * LANES), (4, nb, LANES), table(*lanes), table(*mask)]
        + [(4, cols)] * n_edges,
        [
            left(1),
            pltpu.VMEM((2, nb, LANES), jnp.int32),
            pltpu.VMEM((4, nb, LANES), F32),
            pltpu.SemaphoreType.DMA((7,)),
        ],
    )(block_count, *in_hbm(rhs, across, down, hold, source, target, weights))
    stiff = (across, down, hold)
    basis = [rhs]
    up1 = swapped_sections(up, 1)
    up0 = swapped_sections(up, 0)
    got_edges = []
    for i, edge in enumerate(edges):
        got_edges.append(swapped(edge, "xy", i))
    base, rim, next_lanes, next_blend = run(
        early_kernel, [field_shape, (1, cols), table(*lanes), blends], [], *(marks, rhs, *stiff, up, *got_edges)
    )
    field, local, to0, to1, *rest = run(
        functools.partial(first_kernel, two),
        common + [(4, nb, LANES), table(*lanes), table(*mask), table(*mask), blends],
        [left(2), left(2)],
        *(marks, rhs, base, up, own_lanes, own_high, next_lanes, next_blend, next_field, up0, up1),
    )
    edges, prev = rest[:n_edges], rest[n_edges:]

    for step in range(1, ITERS):
        last = step == ITERS - 1
        got0, got1, got_edges = exchange(to0, to1, edges)
        base, *partial = run(
            functools.partial(between_kernel, last, n_edges),
            [field_shape] + ([(1, LANES)] if last else []),
            [],
            *(marks, field, *stiff, rim, *got_edges, *(basis if last else [])),
        )
        field_next, *rest = run(
            functools.partial(step_kernel, last, two),
            [field_shape, (n_gz * n_xy, LANES)] if last else common,
            [] if last else [left(2)],
            *(marks, field, base, own_lanes, own_high, *prev, local, got0, got1, *partial),
        )
        basis.append(field)
        field = field_next
        if not last:
            local, to0, to1, *edges = rest
    basis.append(field)
    sums = lax.all_to_all(rest[0].reshape(n_gz * n_xy, 1, LANES), ("gz", "xy"), 0, 0)
    sums = sums.reshape(n_gz * n_xy, LANES)
    solution_field, residual = call(finish_kernel, [VMEM] * (1 + len(basis)), [field_shape] * 2)(sums, *basis)
    return solution_field[:, None], residual[:, None]


def solution(mesh):
    in_specs = (
        P(None, "gz", "xy", None),
        P("gz", "xy", None),
        P("gz", "xy", None),
        P("gz", "xy", None),
        P("gz", "xy", None),
        P("gz", "xy", None),
        P(None, "gz", "xy", None),
        P("gz", "xy"),
    )
    out_specs = (P(None, "gz", "xy", None), P(None, "gz", "xy", None))
    return jax.shard_map(body, mesh=mesh, in_specs=in_specs, out_specs=out_specs, check_vma=False)
```

```python
import functools

import jax
import jax.numpy as jnp
from jax import lax
from jax.experimental import pallas as pl
from jax.experimental.pallas import tpu as pltpu
from jax.sharding import PartitionSpec as P


BLOCK = 128
ITERS = 3
LANES = 128
WIDE = 256
GAIN = 0.25
SHIFT = 1.25
F32 = jnp.float32
BF16 = jnp.bfloat16
CHUNK = 256


def swapped(block, axis, first):
    count = lax.axis_size(axis)
    route = []
    for i in range(first, count - 1, 2):
        route += [(i, i + 1), (i + 1, i)]
    return lax.ppermute(block, axis, route) if route else None


def swapped_sections(block, first):
    count, width = lax.axis_size("gz"), lax.axis_size("xy")
    route = []
    for i in range(first, count - 1, 2):
        for j in range(width):
            a, b = i * width + j, (i + 1) * width + j
            route += [(a, b), (b, a)]
    paired = {a for a, _ in route}
    for a in range(0, count * width - 1, 2):
        if a not in paired and a + 1 not in paired and a // width == (a + 1) // width:
            route += [(a, a + 1), (a + 1, a)]
    return lax.ppermute(block, ("gz", "xy"), route)


def split2(x):
    high = x.astype(BF16)
    return high, (x - high.astype(F32)).astype(BF16)


def div_mod(x, d):
    if d & (d - 1) == 0:
        return lax.shift_right_logical(x, jnp.int32(d.bit_length() - 1)), x & (d - 1)
    q = lax.div(x, jnp.int32(d))
    return q, x - q * d


def hi_lo(index, rows, cols):
    row, col = div_mod(index, cols)
    tile, lane = div_mod(col, WIDE)
    return tile * rows + row, lane


def row_of(tile, k):
    return tile[k : k + 1, :]


def one_hot(index, size, shift=0):
    at = lax.broadcasted_iota(jnp.int32, (size, LANES), 0) - shift
    return jnp.concatenate(
        [jnp.where(at == row_of(index, k), 1.0, 0.0).astype(BF16) for k in range(index.shape[0])],
        axis=1,
    )


def blend(index, size, first, second):
    at = lax.broadcasted_iota(jnp.int32, (size, LANES), 0)
    out = []
    for k in range(index.shape[0]):
        here = row_of(index, k)
        out.append(
            jnp.where(at == here, row_of(first, k), jnp.where(at == here + 1, row_of(second, k), 0.0))
        )
    return jnp.concatenate(out, axis=1)


def store_lanes(lo, lanes_ref):
    lanes_ref[...] = one_hot(lo, WIDE)


def tall(field):
    n = field.shape[1] // WIDE
    return jnp.concatenate([field[:, i * WIDE : (i + 1) * WIDE] for i in range(n)], axis=0)


def wide(stack, rows):
    n = stack.shape[0] // rows
    return jnp.concatenate([stack[i * rows : (i + 1) * rows, :] for i in range(n)], axis=1)


def right_of(field):
    return pltpu.roll(field, field.shape[1] - 1, 1)


def load_left(field, left_ref, sides):
    fields = []
    for c in range(2):
        fields += [field[c], right_of(field[c])] if sides == 2 else [field[c]]
    for i, f in enumerate(fields):
        stack = tall(f)
        high, low = split2(stack)
        n = stack.shape[0]
        left_ref[2 * i * n : (2 * i + 1) * n, :] = high
        left_ref[(2 * i + 1) * n : (2 * i + 2) * n, :] = low


def as_tiles(rows_of):
    return jnp.concatenate(
        [r[:, i * LANES : (i + 1) * LANES] for r in rows_of for i in range(CHUNK // LANES)], axis=0
    )


def looked_up(left_ref, lanes_ref, high_ref):
    high, slots = high_ref.shape
    stride = left_ref.shape[0] // 2
    found = ([], [])
    for k in range(0, slots, CHUNK):
        hot = lanes_ref[:, k : k + CHUNK]
        mask = high_ref[:, k : k + CHUNK]
        for c in range(2):
            got = jnp.dot(
                left_ref[c * stride : c * stride + 2 * high, :],
                hot,
                preferred_element_type=F32,
            )
            value = mask * (got[:high] + got[high:])
            found[c].append(jnp.sum(value, axis=0, keepdims=True))
    return jnp.stack([as_tiles(f) for f in found])


def interpolated(left_ref, lanes_ref, blend_ref):
    high, slots = blend_ref.shape[1:]
    found = ([], [])
    for k in range(0, slots, CHUNK):
        hot = lanes_ref[:, k : k + CHUNK]
        wl = blend_ref[0, :, k : k + CHUNK]
        wr = blend_ref[1, :, k : k + CHUNK]
        for c in range(2):
            got = jnp.dot(
                left_ref[4 * c * high : 4 * (c + 1) * high, :],
                hot,
                preferred_element_type=F32,
            )
            value = wl * (got[:high] + got[high : 2 * high]) + wr * (got[2 * high : 3 * high] + got[3 * high :])
            found[c].append(jnp.sum(value, axis=0, keepdims=True))
    return jnp.stack([as_tiles(f) for f in found])


NT = (((1,), (1,)), ((), ()))


def scaled(mask_ref, tile):
    return jnp.concatenate(
        [mask_ref[:, k * LANES : (k + 1) * LANES] * row_of(tile, k) for k in range(tile.shape[0])],
        axis=1,
    )


def spread_own(values, lanes_ref, high_ref, rows):
    high = high_ref.shape[0]
    result = []
    for c in range(2):
        parts = [scaled(high_ref, part.astype(F32)).astype(BF16) for part in split2(values[c])]
        out = lax.dot_general(
            jnp.concatenate(parts, axis=0), lanes_ref[...], NT, preferred_element_type=F32
        )
        result.append(wide(out[:high] + out[high:], rows))
    return result


def spread_corners(values, weights, lanes_ref, high_ref, below_ref, rows):
    high = high_ref.shape[0]
    result = []
    for c in range(2):
        parts = []
        for side in range(2):
            for up, down in zip(split2(values[c] * weights[side]), split2(values[c] * weights[2 + side])):
                part = scaled(high_ref, up.astype(F32)) + scaled(below_ref, down.astype(F32))
                parts.append(part.astype(BF16))
        out = lax.dot_general(
            jnp.concatenate(parts, axis=0), lanes_ref[...], NT, preferred_element_type=F32
        )
        sides = [
            wide(out[p * high : (p + 1) * high] + out[(p + 1) * high : (p + 2) * high], rows)
            for p in (0, 2)
        ]
        result.append(sides[0] + pltpu.roll(sides[1], 1, 1))
    return result


def springs(field, across, down, hold, upper_row, lower_row, rim):
    rows, cols = field.shape
    col = lax.broadcasted_iota(jnp.int32, (rows, cols), 1)
    row = lax.broadcasted_iota(jnp.int32, (rows, cols), 0)
    right = jnp.where(col == cols - 1, 0.0, pltpu.roll(field, cols - 1, 1))
    pull = across * (field - right)
    out = pull - jnp.where(col == 0, 0.0, pltpu.roll(pull, 1, 1))
    lower = jnp.where(row == rows - 1, lower_row, pltpu.roll(field, rows - 1, 0))
    pull = down * (field - lower)
    above = rim * (upper_row - field[0:1, :])
    out = out + pull - jnp.where(row == 0, above, pltpu.roll(pull, 1, 0))
    return out + hold * field


def mark(marks, i):
    return marks[i, 0:1, 0:1]


def pick(flag, a, b):
    return jnp.where(jnp.broadcast_to(flag, a.shape) > 0.5, a, b)


def edges_of(get_row, rows, even_b, two):
    first = [get_row(c, 0) for c in range(2)]
    last = [get_row(c, rows - 1) for c in range(2)]
    out = [jnp.concatenate([pick(even_b, last[c], first[c]) for c in range(2)], axis=0)]
    if two:
        out.append(jnp.concatenate([pick(even_b, first[c], last[c]) for c in range(2)], axis=0))
    return out


def prepare_kernel(two, count, field, across, down, hold, source, target, weights, *refs):
    outs, (left, ids, held, sems) = refs[:-4], refs[-4:]
    field_out, across_out, down_out, hold_out, up, marks, own_lanes, own_high, *edges = outs
    pairs = [(source, ids.at[0]), (field, field_out), (down, down_out)]
    pairs += [(target, ids.at[1]), (weights, held), (across, across_out), (hold, hold_out)]
    copies = [pltpu.make_async_copy(a, b, sems.at[i]) for i, (a, b) in enumerate(pairs)]
    for copy in copies:
        copy.start()
    rows, cols = across_out.shape
    nb, size = ids.shape[1], own_high.shape[0]
    at_gz, at_xy = lax.axis_index("gz"), lax.axis_index("xy")
    as_mark = lambda flag: jnp.full((nb, LANES), flag.astype(jnp.int32)).astype(F32)
    copies[0].wait()
    hi, lo = hi_lo(ids[0], rows, cols)
    store_lanes(lo, own_lanes)
    own_high[...] = one_hot(hi, size).astype(F32)
    copies[1].wait()
    load_left([field_out[0], field_out[1]], left, 1)
    own = looked_up(left, own_lanes, own_high)
    for copy in copies[2:]:
        copy.wait()
    has_next = (at_gz < lax.axis_size("gz") - 1).astype(jnp.int32)
    block = lax.broadcasted_iota(jnp.int32, (nb, LANES), 0)
    live = jnp.where(block * LANES < count[0, 0] * BLOCK * has_next, 1.0, 0.0)
    marks[0] = as_mark(1 - lax.rem(at_gz, 2))
    marks[1] = as_mark(1 - lax.rem(at_xy, 2))
    marks[2] = as_mark(at_gz > 0)
    marks[3] = live
    parts = [own[0], own[1], ids[1].astype(F32)] + [held[q] * live for q in range(4)]
    for i, part in enumerate(parts):
        up[:, i * LANES : (i + 1) * LANES] = part
    even_b = mark(marks, 1)
    messages = edges_of(lambda c, r: field_out[c, r : r + 1, :], rows, even_b, two)
    for message, edge in zip(messages, edges):
        edge[0:2, :] = message
        edge[2:3, :] = down_out[rows - 1 : rows, :]


def tile_of(up, i):
    return up[:, i * LANES : (i + 1) * LANES]


def halves(flags, edge_refs):
    even_b = mark(flags, 1)
    zero = edge_refs[0][...]
    if len(edge_refs) == 2:
        other = edge_refs[1][...]
    else:
        other = jnp.zeros_like(zero)
    return pick(even_b, other, zero), pick(even_b, zero, other)


def spring_image(field, across, down, hold, above, below, rim):
    return [
        springs(
            field[c], across[...], down[...], hold[...], above[c : c + 1], below[c : c + 1], rim
        )
        for c in range(2)
    ]


def early_kernel(flags, field_ref, across, down, hold, up, *refs):
    edge_refs, (base, rim_ref, next_lanes, next_blend) = refs[:-4], refs[-4:]
    rows, cols = across.shape
    field = [field_ref[0], field_ref[1]]
    above, below = halves(flags, edge_refs)
    image = spring_image(field, across, down, hold, above, below, above[2:3, :])
    for c in range(2):
        base[c] = image[c]
    rim_ref[...] = above[2:3, :]
    hi, lo = hi_lo(tile_of(up, 2).astype(jnp.int32), rows, cols)
    store_lanes(lo, next_lanes)
    for side in range(2):
        next_blend[side] = blend(hi, next_blend.shape[1], tile_of(up, 3 + side), tile_of(up, 5 + side))


def ahead_kernel(next_lanes, next_blend, next_field, out, left):
    load_left([next_field[0], next_field[1]], left, 2)
    out[...] = interpolated(left, next_lanes, next_blend)


def send_on(even, even_b, two, field, own_tables, prev_tables, left, local_ref, send0, send1, *edges):
    own_lanes, own_high = own_tables
    prev_lanes, prev_blend = prev_tables
    load_left(field, left, 2)
    own = looked_up(left, own_lanes, own_high)
    mid = interpolated(left, prev_lanes, prev_blend)
    local_ref[0] = own
    local_ref[1] = mid
    send0[...] = pick(even, own, mid)
    send1[...] = pick(even, mid, own)
    messages = edges_of(lambda c, r: field[c][r : r + 1, :], field[0].shape[0], even_b, two)
    for message, edge in zip(messages, edges):
        edge[...] = message


def stepped(field_ref, image):
    return [GAIN * image[c] - SHIFT * field_ref[c] for c in range(2)]


def first_kernel(
    two, flags, field_ref, base, up, own_lanes, own_high, got_next, up0, up1, *refs
):
    refs, left = refs[:-1], refs[-1]
    out, local_ref, send0, send1, *edges = refs[:-5]
    prev_weights, prev_lanes, prev_high, prev_below, prev_blend = refs[-5:]
    even, even_b = mark(flags, 0), mark(flags, 1)
    rows, cols = field_ref.shape[1:]
    size = own_high.shape[0]
    got_up = pick(even, up1[...], up0[...])
    weights = [tile_of(got_up, 3 + q) * flags[2] for q in range(4)]
    for q in range(4):
        prev_weights[q] = weights[q]
    hi, lo = hi_lo(tile_of(got_up, 2).astype(jnp.int32), rows, cols)
    store_lanes(lo, prev_lanes)
    prev_high[...] = one_hot(hi, size).astype(F32)
    prev_below[...] = one_hot(hi, size, 1).astype(F32)
    for side in range(2):
        prev_blend[side] = blend(hi, size, weights[side], weights[2 + side])
    load_left([field_ref[0], field_ref[1]], left, 2)
    mid = interpolated(left, prev_lanes, prev_blend)
    own = [tile_of(up, c) for c in range(2)]
    got_prev = [tile_of(got_up, c) for c in range(2)]
    live = flags[3]
    pulled = spread_own([live * (own[c] - got_next[c]) for c in range(2)], own_lanes, own_high, rows)
    error = [mid[c] - got_prev[c] for c in range(2)]
    pushed = spread_corners(error, weights, prev_lanes, prev_high, prev_below, rows)
    after = stepped(field_ref, [base[c] + pulled[c] + pushed[c] for c in range(2)])
    for c in range(2):
        out[c] = after[c]
    send_on(
        even,
        even_b,
        two,
        after,
        (own_lanes, own_high),
        (prev_lanes, prev_blend),
        left,
        local_ref,
        send0,
        send1,
        *edges,
    )


def moments_of(pairs, start=0):
    lane = lax.broadcasted_iota(jnp.int32, (1, LANES), 1)
    total = jnp.zeros((1, LANES), F32)
    for i, (u, w) in enumerate(pairs):
        s = u[0] * w[0] + u[1] * w[1]
        s = jnp.sum(jnp.sum(s, axis=0, keepdims=True), axis=1, keepdims=True)
        total = total + jnp.where(lane == start + i, s, 0.0)
    return total


def between_kernel(last, n_edges, flags, field_ref, across, down, hold, rim, *refs):
    refs = list(refs)
    edge_refs = [refs.pop(0) for _ in range(n_edges)]
    earlier = [refs.pop(0) for _ in range(ITERS - 1)] if last else []
    field = [field_ref[0], field_ref[1]]
    above, below = halves(flags, edge_refs)
    image = spring_image(field, across, down, hold, above, below, rim[...])
    base = refs.pop(0)
    for c in range(2):
        base[c] = image[c]
    if last:
        basis = [(ref[0], ref[1]) for ref in earlier] + [field, image]
        refs.pop(0)[...] = moments_of([(basis[i // 2], basis[i - i // 2]) for i in range(2 * ITERS)])


def errors_of(flags, local, got0, got1):
    even, live = mark(flags, 0), flags[3]
    got_next = pick(even, got0[...], got1[...])
    got_prev = pick(even, got1[...], got0[...])
    return (
        [live * (local[0, c] - got_next[c]) for c in range(2)],
        [local[1, c] - got_prev[c] for c in range(2)],
    )


def sum_kernel(flags, partial, local, got0, got1, sums):
    own, prev = errors_of(flags, local, got0, got1)
    s = own[0] * local[0, 0] + own[1] * local[0, 1] + prev[0] * local[1, 0] + prev[1] * local[1, 1]
    s = jnp.sum(jnp.sum(s, axis=0, keepdims=True), axis=1, keepdims=True)
    lane = lax.broadcasted_iota(jnp.int32, (1, LANES), 1)
    at = 2 * ITERS - 1
    before = jnp.sum(jnp.where(lane == at - 1, partial[...], 0.0), axis=1, keepdims=True)
    total = jnp.where(lane == at, GAIN * (partial[...] + s) - SHIFT * before, partial[...])
    sums[...] = jnp.broadcast_to(total, sums.shape)


def step_kernel(
    last,
    two,
    flags,
    field_ref,
    base,
    own_lanes,
    own_high,
    prev_weights,
    prev_lanes,
    prev_high,
    prev_below,
    prev_blend,
    local,
    got0,
    got1,
    out,
    *refs,
):
    rows = field_ref.shape[1]
    error, error_prev = errors_of(flags, local, got0, got1)
    pulled = spread_own(error, own_lanes, own_high, rows)
    weights = [prev_weights[q] for q in range(4)]
    pushed = spread_corners(error_prev, weights, prev_lanes, prev_high, prev_below, rows)
    after = stepped(field_ref, [base[c] + pulled[c] + pushed[c] for c in range(2)])
    for c in range(2):
        out[c] = after[c]
    if not last:
        even, even_b = mark(flags, 0), mark(flags, 1)
        messages, left = refs[:-1], refs[-1]
        send_on(even, even_b, two, after, (own_lanes, own_high), (prev_lanes, prev_blend), left, *messages)


def conjugate(moments):
    def apply(p):
        shifted = [None] + p
        return [
            (SHIFT * p[k] if k < len(p) else 0.0) * (1.0 / GAIN)
            + ((1.0 / GAIN) * shifted[k] if k else 0.0)
            for k in range(len(p) + 1)
        ]

    def product(p, q):
        return sum(p[i] * q[j] * moments[i + j] for i in range(len(p)) for j in range(len(q)))

    def plus(p, factor, q):
        size = max(len(p), len(q))
        pad = lambda a: a + [None] * (size - len(a))
        out = []
        for a, b in zip(pad(p), pad(q)):
            out.append(factor * b if a is None else a if b is None else a + factor * b)
        return out

    one = jnp.ones_like(moments[0])
    solution_field, residual, direction = [], [one], [one]
    norm_now = moments[0]
    for step in range(ITERS):
        image = apply(direction)
        alpha = norm_now / product(direction, image)
        solution_field = plus(solution_field, alpha, direction)
        residual = plus(residual, -alpha, image)
        if step + 1 < ITERS:
            norm_next = product(residual, residual)
            direction = plus(residual, norm_next / norm_now, direction)
            norm_now = norm_next
    return solution_field, residual


def finish_kernel(sums, *refs):
    basis, (solution_ref, residual_ref) = refs[: ITERS + 1], refs[ITERS + 1 :]
    total = jnp.sum(sums[...], axis=0, keepdims=True)
    lane = lax.broadcasted_iota(jnp.int32, (1, LANES), 1)
    moments = [
        jnp.sum(jnp.where(lane == i, total, 0.0), axis=1, keepdims=True) for i in range(2 * ITERS)
    ]
    solution_field, residual = conjugate(moments)
    for c in range(2):
        values = [ref[c] for ref in basis]
        solution_ref[c] = sum(a * v for a, v in zip(solution_field, values))
        residual_ref[c] = sum(a * v for a, v in zip(residual, values))


VMEM = pl.BlockSpec(memory_space=pltpu.VMEM)
SMEM = pl.BlockSpec(memory_space=pltpu.SMEM)
HBM = pl.BlockSpec(memory_space=pltpu.HBM)


def call(kernel, in_specs, shapes, scratch=()):
    shapes = [s if isinstance(s, jax.ShapeDtypeStruct) else jax.ShapeDtypeStruct(s, F32) for s in shapes]
    return pl.pallas_call(
        kernel,
        in_specs=in_specs,
        out_specs=[VMEM] * len(shapes),
        out_shape=shapes,
        scratch_shapes=list(scratch),
        compiler_params=pltpu.CompilerParams(vmem_limit_bytes=48 * 1024 * 1024),
    )


def body(
    right_side,
    stiff_across,
    stiff_down,
    anchor,
    source_node,
    target_cell,
    corner_weight,
    block_count,
):
    rows, cols = stiff_across.shape[1:]
    rhs = right_side[:, 0]
    across, down, hold = stiff_across[0], stiff_down[0], anchor[0]
    slots = source_node.shape[2]
    nb = slots // LANES
    source = source_node.reshape(nb, LANES)
    target = target_cell.reshape(nb, LANES)
    weights = corner_weight.reshape(4, nb, LANES)
    n_gz, n_xy = lax.axis_size("gz"), lax.axis_size("xy")
    two = n_xy > 2
    n_edges = 2 if two else 1

    def exchange(to0, to1, edges):
        got1 = swapped_sections(to1, 1)
        got0 = swapped_sections(to0, 0)
        got_edges = []
        for i, edge in enumerate(edges):
            got_edges.append(swapped(edge, "xy", i))
        return got0, got1, got_edges

    field_shape = (2, rows, cols)
    message = (2, nb, LANES)
    size = rows * cols // WIDE
    common = [field_shape, (2,) + message, message, message] + [(2, cols)] * n_edges
    table = lambda *shape: jax.ShapeDtypeStruct(shape, BF16)
    left = lambda sides: pltpu.VMEM((4 * sides * size, WIDE), BF16)
    lanes, mask, blends = (WIDE, slots), (size, slots), (2, size, slots)
    run = lambda kernel, shapes, scratch, *args: call(kernel, [VMEM] * len(args), shapes, scratch)(*args)
    next_field = lax.ppermute(rhs, "gz", [(i, (i - 1) % n_gz) for i in range(n_gz)])
    in_hbm = lambda *arrays: [pltpu.with_memory_space_constraint(a, pltpu.HBM) for a in arrays]
    grid = (rows, cols)
    rhs, across, down, hold, up, marks, own_lanes, own_high, *edges = call(
        functools.partial(prepare_kernel, two),
        [SMEM] + [HBM] * 7,
        [field_shape, grid, grid, grid, (nb, 7 * LANES), (4, nb, LANES), table(*lanes), mask]
        + [(4, cols)] * n_edges,
        [
            left(1),
            pltpu.VMEM((2, nb, LANES), jnp.int32),
            pltpu.VMEM((4, nb, LANES), F32),
            pltpu.SemaphoreType.DMA((7,)),
        ],
    )(block_count, *in_hbm(rhs, across, down, hold, source, target, weights))
    stiff = (across, down, hold)
    basis = [rhs]
    up1 = swapped_sections(up, 1)
    up0 = swapped_sections(up, 0)
    got_edges = []
    for i, edge in enumerate(edges):
        got_edges.append(swapped(edge, "xy", i))
    base, rim, next_lanes, next_blend = run(
        early_kernel, [field_shape, (1, cols), table(*lanes), blends], [], *(marks, rhs, *stiff, up, *got_edges)
    )
    (got_next,) = run(ahead_kernel, [message], [left(2)], next_lanes, next_blend, next_field)
    field, local, to0, to1, *rest = run(
        functools.partial(first_kernel, two),
        common + [(4, nb, LANES), table(*lanes), mask, mask, blends],
        [left(2)],
        *(marks, rhs, base, up, own_lanes, own_high, got_next, up0, up1),
    )
    edges, prev = rest[:n_edges], rest[n_edges:]

    for step in range(1, ITERS):
        last = step == ITERS - 1
        got0, got1, got_edges = exchange(to0, to1, edges)
        base, *partial = run(
            functools.partial(between_kernel, last, n_edges),
            [field_shape] + ([(1, LANES)] if last else []),
            [],
            *(marks, field, *stiff, rim, *got_edges, *(basis if last else [])),
        )
        if last:
            (sums,) = run(sum_kernel, [(n_gz * n_xy, LANES)], [], marks, *partial, local, got0, got1)
            sums = lax.all_to_all(sums.reshape(n_gz * n_xy, 1, LANES), ("gz", "xy"), 0, 0)
            sums = sums.reshape(n_gz * n_xy, LANES)
        field_next, *rest = run(
            functools.partial(step_kernel, last, two),
            [field_shape] if last else common,
            [] if last else [left(2)],
            *(marks, field, base, own_lanes, own_high, *prev, local, got0, got1),
        )
        basis.append(field)
        field = field_next
        if not last:
            local, to0, to1, *edges = rest
    basis.append(field)
    solution_field, residual = call(finish_kernel, [VMEM] * (1 + len(basis)), [field_shape] * 2)(sums, *basis)
    return solution_field[:, None], residual[:, None]


def solution(mesh):
    in_specs = (
        P(None, "gz", "xy", None),
        P("gz", "xy", None),
        P("gz", "xy", None),
        P("gz", "xy", None),
        P("gz", "xy", None),
        P("gz", "xy", None),
        P(None, "gz", "xy", None),
        P("gz", "xy"),
    )
    out_specs = (P(None, "gz", "xy", None), P(None, "gz", "xy", None))
    return jax.shard_map(body, mesh=mesh, in_specs=in_specs, out_specs=out_specs, check_vma=False)
```

```python
import functools
import math

import jax
import jax.numpy as jnp
from jax import lax
from jax.experimental import pallas as pl
from jax.experimental.pallas import tpu as pltpu
from jax.sharding import PartitionSpec as P


BLOCK = 128
ITERS = 3
LANES = 128
WIDE = 256
GAIN = 0.25
SHIFT = 1.25
F32 = jnp.float32
BF16 = jnp.bfloat16
CHUNK = 256


def swapped(block, axis, first):
    count = lax.axis_size(axis)
    route = []
    for i in range(first, count - 1, 2):
        route += [(i, i + 1), (i + 1, i)]
    return lax.ppermute(block, axis, route) if route else None


def swapped_sections(block, first):
    count, width = lax.axis_size("gz"), lax.axis_size("xy")
    route = []
    for i in range(first, count - 1, 2):
        for j in range(width):
            a, b = i * width + j, (i + 1) * width + j
            route += [(a, b), (b, a)]
    paired = {a for a, _ in route}
    for a in range(0, count * width - 1, 2):
        if a not in paired and a + 1 not in paired and a // width == (a + 1) // width:
            route += [(a, a + 1), (a + 1, a)]
    return lax.ppermute(block, ("gz", "xy"), route)


def split2(x):
    high = x.astype(BF16)
    return high, (x - high.astype(F32)).astype(BF16)


def div_mod(x, d):
    if d & (d - 1) == 0:
        return lax.shift_right_logical(x, jnp.int32(d.bit_length() - 1)), x & (d - 1)
    q = lax.div(x, jnp.int32(d))
    return q, x - q * d


def hi_lo(index, rows, cols):
    row, col = div_mod(index, cols)
    tile, lane = div_mod(col, WIDE)
    return tile * rows + row, lane


def row_of(tile, k):
    return tile[k : k + 1, :]


def one_hot(index, size, shift=0):
    at = lax.broadcasted_iota(jnp.int32, (size, LANES), 0) - shift
    return jnp.concatenate(
        [jnp.where(at == row_of(index, k), 1.0, 0.0).astype(BF16) for k in range(index.shape[0])],
        axis=1,
    )


def blend(index, size, first, second):
    at = lax.broadcasted_iota(jnp.int32, (size, LANES), 0)
    out = []
    for k in range(index.shape[0]):
        here = row_of(index, k)
        out.append(
            jnp.where(at == here, row_of(first, k), jnp.where(at == here + 1, row_of(second, k), 0.0))
        )
    return jnp.concatenate(out, axis=1)


def store_lanes(lo, lanes_ref):
    lanes_ref[...] = one_hot(lo, WIDE)


def tall(field):
    n = field.shape[1] // WIDE
    return jnp.concatenate([field[:, i * WIDE : (i + 1) * WIDE] for i in range(n)], axis=0)


def wide(stack, rows):
    n = stack.shape[0] // rows
    return jnp.concatenate([stack[i * rows : (i + 1) * rows, :] for i in range(n)], axis=1)


def right_of(field):
    return pltpu.roll(field, field.shape[1] - 1, 1)


def load_left(field, left_ref, sides):
    fields = []
    for c in range(2):
        fields += [field[c], right_of(field[c])] if sides == 2 else [field[c]]
    for i, f in enumerate(fields):
        stack = tall(f)
        high, low = split2(stack)
        n = stack.shape[0]
        left_ref[2 * i * n : (2 * i + 1) * n, :] = high
        left_ref[(2 * i + 1) * n : (2 * i + 2) * n, :] = low


def as_tiles(rows_of):
    return jnp.concatenate(
        [r[:, i * LANES : (i + 1) * LANES] for r in rows_of for i in range(CHUNK // LANES)], axis=0
    )


def looked_up(left_ref, lanes_ref, high_ref):
    high, slots = high_ref.shape
    stride = left_ref.shape[0] // 2
    found = ([], [])
    for k in range(0, slots, CHUNK):
        hot = lanes_ref[:, k : k + CHUNK]
        mask = high_ref[:, k : k + CHUNK]
        for c in range(2):
            got = jnp.dot(
                left_ref[c * stride : c * stride + 2 * high, :],
                hot,
                preferred_element_type=F32,
            )
            value = mask * (got[:high] + got[high:])
            found[c].append(jnp.sum(value, axis=0, keepdims=True))
    return jnp.stack([as_tiles(f) for f in found])


def interpolated(left_ref, lanes_ref, blend_ref):
    high, slots = blend_ref.shape[1:]
    found = ([], [])
    for k in range(0, slots, CHUNK):
        hot = lanes_ref[:, k : k + CHUNK]
        wl = blend_ref[0, :, k : k + CHUNK]
        wr = blend_ref[1, :, k : k + CHUNK]
        for c in range(2):
            got = jnp.dot(
                left_ref[4 * c * high : 4 * (c + 1) * high, :],
                hot,
                preferred_element_type=F32,
            )
            value = wl * (got[:high] + got[high : 2 * high]) + wr * (got[2 * high : 3 * high] + got[3 * high :])
            found[c].append(jnp.sum(value, axis=0, keepdims=True))
    return jnp.stack([as_tiles(f) for f in found])


NT = (((1,), (1,)), ((), ()))


def scaled(mask_ref, tile):
    return jnp.concatenate(
        [mask_ref[:, k * LANES : (k + 1) * LANES] * row_of(tile, k) for k in range(tile.shape[0])],
        axis=1,
    )


def spread_own(values, lanes_ref, high_ref, rows):
    high = high_ref.shape[0]
    result = []
    for c in range(2):
        parts = [scaled(high_ref, part.astype(F32)).astype(BF16) for part in split2(values[c])]
        out = lax.dot_general(
            jnp.concatenate(parts, axis=0), lanes_ref[...], NT, preferred_element_type=F32
        )
        result.append(wide(out[:high] + out[high:], rows))
    return result


def spread_corners(values, weights, lanes_ref, high_ref, below_ref, rows):
    high = high_ref.shape[0]
    result = []
    for c in range(2):
        parts = []
        for side in range(2):
            for up, down in zip(split2(values[c] * weights[side]), split2(values[c] * weights[2 + side])):
                part = scaled(high_ref, up.astype(F32)) + scaled(below_ref, down.astype(F32))
                parts.append(part.astype(BF16))
        out = lax.dot_general(
            jnp.concatenate(parts, axis=0), lanes_ref[...], NT, preferred_element_type=F32
        )
        sides = [
            wide(out[p * high : (p + 1) * high] + out[(p + 1) * high : (p + 2) * high], rows)
            for p in (0, 2)
        ]
        result.append(sides[0] + pltpu.roll(sides[1], 1, 1))
    return result


def springs(field, across, down, hold, upper_row, lower_row, rim):
    rows, cols = field.shape
    col = lax.broadcasted_iota(jnp.int32, (rows, cols), 1)
    row = lax.broadcasted_iota(jnp.int32, (rows, cols), 0)
    right = jnp.where(col == cols - 1, 0.0, pltpu.roll(field, cols - 1, 1))
    pull = across * (field - right)
    out = pull - jnp.where(col == 0, 0.0, pltpu.roll(pull, 1, 1))
    lower = jnp.where(row == rows - 1, lower_row, pltpu.roll(field, rows - 1, 0))
    pull = down * (field - lower)
    above = rim * (upper_row - field[0:1, :])
    out = out + pull - jnp.where(row == 0, above, pltpu.roll(pull, 1, 0))
    return out + hold * field


def mark(marks, i):
    return marks[i, 0:1, 0:1]


def pick(flag, a, b):
    return jnp.where(jnp.broadcast_to(flag, a.shape) > 0.5, a, b)


def edges_of(get_row, rows, even_b, two):
    first = [get_row(c, 0) for c in range(2)]
    last = [get_row(c, rows - 1) for c in range(2)]
    out = [jnp.concatenate([pick(even_b, last[c], first[c]) for c in range(2)], axis=0)]
    if two:
        out.append(jnp.concatenate([pick(even_b, first[c], last[c]) for c in range(2)], axis=0))
    return out


def prepare_kernel(two, count, field, across, down, hold, source, target, weights, *refs):
    outs, (left, ids, held, sems) = refs[:-4], refs[-4:]
    field_out, across_out, down_out, hold_out, up, marks, own_lanes, own_high, *edges = outs
    pairs = [(source, ids.at[0]), (field, field_out), (down, down_out)]
    pairs += [(target, ids.at[1]), (weights, held), (across, across_out), (hold, hold_out)]
    copies = [pltpu.make_async_copy(a, b, sems.at[i]) for i, (a, b) in enumerate(pairs)]
    for copy in copies:
        copy.start()
    rows, cols = across_out.shape
    nb, size = ids.shape[1], own_high.shape[0]
    at_gz, at_xy = lax.axis_index("gz"), lax.axis_index("xy")
    as_mark = lambda flag: jnp.full((nb, LANES), flag.astype(jnp.int32)).astype(F32)
    copies[0].wait()
    hi, lo = hi_lo(ids[0], rows, cols)
    store_lanes(lo, own_lanes)
    own_high[...] = one_hot(hi, size).astype(F32)
    copies[1].wait()
    load_left([field_out[0], field_out[1]], left, 1)
    own = looked_up(left, own_lanes, own_high)
    for copy in copies[2:]:
        copy.wait()
    has_next = (at_gz < lax.axis_size("gz") - 1).astype(jnp.int32)
    block = lax.broadcasted_iota(jnp.int32, (nb, LANES), 0)
    live = jnp.where(block * LANES < count[0, 0] * BLOCK * has_next, 1.0, 0.0)
    marks[0] = as_mark(1 - lax.rem(at_gz, 2))
    marks[1] = as_mark(1 - lax.rem(at_xy, 2))
    marks[2] = as_mark(at_gz > 0)
    marks[3] = live
    parts = [own[0], own[1], ids[1].astype(F32)] + [held[q] * live for q in range(4)]
    for i, part in enumerate(parts):
        up[:, i * LANES : (i + 1) * LANES] = part
    even_b = mark(marks, 1)
    messages = edges_of(lambda c, r: field_out[c, r : r + 1, :], rows, even_b, two)
    for message, edge in zip(messages, edges):
        edge[0:2, :] = message
        edge[2:3, :] = down_out[rows - 1 : rows, :]


def tile_of(up, i):
    return up[:, i * LANES : (i + 1) * LANES]


def halves(flags, edge_refs):
    even_b = mark(flags, 1)
    zero = edge_refs[0][...]
    if len(edge_refs) == 2:
        other = edge_refs[1][...]
    else:
        other = jnp.zeros_like(zero)
    return pick(even_b, other, zero), pick(even_b, zero, other)


def spring_image(field, across, down, hold, above, below, rim):
    return [
        springs(
            field[c], across[...], down[...], hold[...], above[c : c + 1], below[c : c + 1], rim
        )
        for c in range(2)
    ]


def early_kernel(flags, field_ref, across, down, hold, up, *refs):
    edge_refs, (base, rim_ref, next_lanes, next_blend) = refs[:-4], refs[-4:]
    rows, cols = across.shape
    field = [field_ref[0], field_ref[1]]
    above, below = halves(flags, edge_refs)
    image = spring_image(field, across, down, hold, above, below, above[2:3, :])
    for c in range(2):
        base[c] = image[c]
    rim_ref[...] = above[2:3, :]
    hi, lo = hi_lo(tile_of(up, 2).astype(jnp.int32), rows, cols)
    store_lanes(lo, next_lanes)
    for side in range(2):
        next_blend[side] = blend(hi, next_blend.shape[1], tile_of(up, 3 + side), tile_of(up, 5 + side))


def ahead_kernel(next_lanes, next_blend, next_field, out, left):
    load_left([next_field[0], next_field[1]], left, 2)
    out[...] = interpolated(left, next_lanes, next_blend)


def send_on(even, even_b, two, field, own_tables, prev_tables, left, local_ref, send0, send1, *edges):
    own_lanes, own_high = own_tables
    prev_lanes, prev_blend = prev_tables
    load_left(field, left, 2)
    own = looked_up(left, own_lanes, own_high)
    mid = interpolated(left, prev_lanes, prev_blend)
    local_ref[0] = own
    local_ref[1] = mid
    send0[...] = pick(even, own, mid)
    send1[...] = pick(even, mid, own)
    messages = edges_of(lambda c, r: field[c][r : r + 1, :], field[0].shape[0], even_b, two)
    for message, edge in zip(messages, edges):
        edge[...] = message


def stepped(field_ref, image):
    return [GAIN * image[c] - SHIFT * field_ref[c] for c in range(2)]


def first_kernel(
    two, flags, field_ref, base, up, own_lanes, own_high, got_next, up0, up1, *refs
):
    refs, left = refs[:-1], refs[-1]
    out, local_ref, send0, send1, *edges = refs[:-5]
    prev_weights, prev_lanes, prev_high, prev_below, prev_blend = refs[-5:]
    even, even_b = mark(flags, 0), mark(flags, 1)
    rows, cols = field_ref.shape[1:]
    size = own_high.shape[0]
    got_up = pick(even, up1[...], up0[...])
    weights = [tile_of(got_up, 3 + q) * flags[2] for q in range(4)]
    for q in range(4):
        prev_weights[q] = weights[q]
    hi, lo = hi_lo(tile_of(got_up, 2).astype(jnp.int32), rows, cols)
    store_lanes(lo, prev_lanes)
    prev_high[...] = one_hot(hi, size).astype(F32)
    prev_below[...] = one_hot(hi, size, 1).astype(F32)
    for side in range(2):
        prev_blend[side] = blend(hi, size, weights[side], weights[2 + side])
    load_left([field_ref[0], field_ref[1]], left, 2)
    mid = interpolated(left, prev_lanes, prev_blend)
    own = [tile_of(up, c) for c in range(2)]
    got_prev = [tile_of(got_up, c) for c in range(2)]
    live = flags[3]
    pulled = spread_own([live * (own[c] - got_next[c]) for c in range(2)], own_lanes, own_high, rows)
    error = [mid[c] - got_prev[c] for c in range(2)]
    pushed = spread_corners(error, weights, prev_lanes, prev_high, prev_below, rows)
    after = stepped(field_ref, [base[c] + pulled[c] + pushed[c] for c in range(2)])
    for c in range(2):
        out[c] = after[c]
    send_on(
        even,
        even_b,
        two,
        after,
        (own_lanes, own_high),
        (prev_lanes, prev_blend),
        left,
        local_ref,
        send0,
        send1,
        *edges,
    )


def moment_scale(slots):
    bound = GAIN * (8 * 3.0 + 0.2 + 4 * slots) + SHIFT
    return 0.5 ** math.ceil(2.5 * math.log2(bound))


def moments_of(pairs, scale, start=0):
    lane = lax.broadcasted_iota(jnp.int32, (1, LANES), 1)
    total = jnp.zeros((1, LANES), F32)
    for i, (u, w) in enumerate(pairs):
        s = (u[0] * scale) * (w[0] * scale) + (u[1] * scale) * (w[1] * scale)
        s = jnp.sum(jnp.sum(s, axis=0, keepdims=True), axis=1, keepdims=True)
        total = total + jnp.where(lane == start + i, s, 0.0)
    return total


def between_kernel(last, n_edges, scale, flags, field_ref, across, down, hold, rim, *refs):
    refs = list(refs)
    edge_refs = [refs.pop(0) for _ in range(n_edges)]
    earlier = [refs.pop(0) for _ in range(ITERS - 1)] if last else []
    field = [field_ref[0], field_ref[1]]
    above, below = halves(flags, edge_refs)
    image = spring_image(field, across, down, hold, above, below, rim[...])
    base = refs.pop(0)
    for c in range(2):
        base[c] = image[c]
    if last:
        basis = [(ref[0], ref[1]) for ref in earlier] + [field, image]
        refs.pop(0)[...] = moments_of(
            [(basis[i // 2], basis[i - i // 2]) for i in range(2 * ITERS)], scale
        )


def errors_of(flags, local, got0, got1):
    even, live = mark(flags, 0), flags[3]
    got_next = pick(even, got0[...], got1[...])
    got_prev = pick(even, got1[...], got0[...])
    return (
        [live * (local[0, c] - got_next[c]) for c in range(2)],
        [local[1, c] - got_prev[c] for c in range(2)],
    )


def sum_kernel(scale, flags, partial, local, got0, got1, sums):
    own, prev = errors_of(flags, local, got0, got1)
    pairs = [(own[c], local[0, c]) for c in range(2)] + [(prev[c], local[1, c]) for c in range(2)]
    s = sum((a * scale) * (b * scale) for a, b in pairs)
    s = jnp.sum(jnp.sum(s, axis=0, keepdims=True), axis=1, keepdims=True)
    lane = lax.broadcasted_iota(jnp.int32, (1, LANES), 1)
    at = 2 * ITERS - 1
    before = jnp.sum(jnp.where(lane == at - 1, partial[...], 0.0), axis=1, keepdims=True)
    total = jnp.where(lane == at, GAIN * (partial[...] + s) - SHIFT * before, partial[...])
    sums[...] = jnp.broadcast_to(total, sums.shape)


def step_kernel(
    last,
    two,
    flags,
    field_ref,
    base,
    own_lanes,
    own_high,
    prev_weights,
    prev_lanes,
    prev_high,
    prev_below,
    prev_blend,
    local,
    got0,
    got1,
    out,
    *refs,
):
    rows = field_ref.shape[1]
    error, error_prev = errors_of(flags, local, got0, got1)
    pulled = spread_own(error, own_lanes, own_high, rows)
    weights = [prev_weights[q] for q in range(4)]
    pushed = spread_corners(error_prev, weights, prev_lanes, prev_high, prev_below, rows)
    after = stepped(field_ref, [base[c] + pulled[c] + pushed[c] for c in range(2)])
    for c in range(2):
        out[c] = after[c]
    if not last:
        even, even_b = mark(flags, 0), mark(flags, 1)
        messages, left = refs[:-1], refs[-1]
        send_on(even, even_b, two, after, (own_lanes, own_high), (prev_lanes, prev_blend), left, *messages)


def conjugate(moments):
    def apply(p):
        shifted = [None] + p
        return [
            (SHIFT * p[k] if k < len(p) else 0.0) * (1.0 / GAIN)
            + ((1.0 / GAIN) * shifted[k] if k else 0.0)
            for k in range(len(p) + 1)
        ]

    def product(p, q):
        return sum(p[i] * q[j] * moments[i + j] for i in range(len(p)) for j in range(len(q)))

    def plus(p, factor, q):
        size = max(len(p), len(q))
        pad = lambda a: a + [None] * (size - len(a))
        out = []
        for a, b in zip(pad(p), pad(q)):
            out.append(factor * b if a is None else a if b is None else a + factor * b)
        return out

    one = jnp.ones_like(moments[0])
    solution_field, residual, direction = [], [one], [one]
    norm_now = moments[0]
    for step in range(ITERS):
        image = apply(direction)
        alpha = norm_now / product(direction, image)
        solution_field = plus(solution_field, alpha, direction)
        residual = plus(residual, -alpha, image)
        if step + 1 < ITERS:
            norm_next = product(residual, residual)
            direction = plus(residual, norm_next / norm_now, direction)
            norm_now = norm_next
    return solution_field, residual


def finish_kernel(sums, *refs):
    basis, (solution_ref, residual_ref) = refs[: ITERS + 1], refs[ITERS + 1 :]
    total = jnp.sum(sums[...], axis=0, keepdims=True)
    lane = lax.broadcasted_iota(jnp.int32, (1, LANES), 1)
    moments = [
        jnp.sum(jnp.where(lane == i, total, 0.0), axis=1, keepdims=True) for i in range(2 * ITERS)
    ]
    solution_field, residual = conjugate(moments)
    for c in range(2):
        values = [ref[c] for ref in basis]
        solution_ref[c] = sum(a * v for a, v in zip(solution_field, values))
        residual_ref[c] = sum(a * v for a, v in zip(residual, values))


VMEM = pl.BlockSpec(memory_space=pltpu.VMEM)
SMEM = pl.BlockSpec(memory_space=pltpu.SMEM)
HBM = pl.BlockSpec(memory_space=pltpu.HBM)


def call(kernel, in_specs, shapes, scratch=()):
    shapes = [s if isinstance(s, jax.ShapeDtypeStruct) else jax.ShapeDtypeStruct(s, F32) for s in shapes]
    return pl.pallas_call(
        kernel,
        in_specs=in_specs,
        out_specs=[VMEM] * len(shapes),
        out_shape=shapes,
        scratch_shapes=list(scratch),
        compiler_params=pltpu.CompilerParams(vmem_limit_bytes=48 * 1024 * 1024),
    )


def body(
    right_side,
    stiff_across,
    stiff_down,
    anchor,
    source_node,
    target_cell,
    corner_weight,
    block_count,
):
    rows, cols = stiff_across.shape[1:]
    rhs = right_side[:, 0]
    across, down, hold = stiff_across[0], stiff_down[0], anchor[0]
    slots = source_node.shape[2]
    nb = slots // LANES
    source = source_node.reshape(nb, LANES)
    target = target_cell.reshape(nb, LANES)
    weights = corner_weight.reshape(4, nb, LANES)
    n_gz, n_xy = lax.axis_size("gz"), lax.axis_size("xy")
    two = n_xy > 2
    n_edges = 2 if two else 1

    def exchange(to0, to1, edges):
        got1 = swapped_sections(to1, 1)
        got0 = swapped_sections(to0, 0)
        got_edges = []
        for i, edge in enumerate(edges):
            got_edges.append(swapped(edge, "xy", i))
        return got0, got1, got_edges

    field_shape = (2, rows, cols)
    message = (2, nb, LANES)
    scale = moment_scale(slots)
    size = rows * cols // WIDE
    common = [field_shape, (2,) + message, message, message] + [(2, cols)] * n_edges
    table = lambda *shape: jax.ShapeDtypeStruct(shape, BF16)
    left = lambda sides: pltpu.VMEM((4 * sides * size, WIDE), BF16)
    lanes, mask, blends = (WIDE, slots), (size, slots), (2, size, slots)
    run = lambda kernel, shapes, scratch, *args: call(kernel, [VMEM] * len(args), shapes, scratch)(*args)
    next_field = lax.ppermute(rhs, "gz", [(i, (i - 1) % n_gz) for i in range(n_gz)])
    in_hbm = lambda *arrays: [pltpu.with_memory_space_constraint(a, pltpu.HBM) for a in arrays]
    grid = (rows, cols)
    rhs, across, down, hold, up, marks, own_lanes, own_high, *edges = call(
        functools.partial(prepare_kernel, two),
        [SMEM] + [HBM] * 7,
        [field_shape, grid, grid, grid, (nb, 7 * LANES), (4, nb, LANES), table(*lanes), mask]
        + [(4, cols)] * n_edges,
        [
            left(1),
            pltpu.VMEM((2, nb, LANES), jnp.int32),
            pltpu.VMEM((4, nb, LANES), F32),
            pltpu.SemaphoreType.DMA((7,)),
        ],
    )(block_count, *in_hbm(rhs, across, down, hold, source, target, weights))
    stiff = (across, down, hold)
    basis = [rhs]
    up1 = swapped_sections(up, 1)
    up0 = swapped_sections(up, 0)
    got_edges = []
    for i, edge in enumerate(edges):
        got_edges.append(swapped(edge, "xy", i))
    base, rim, next_lanes, next_blend = run(
        early_kernel, [field_shape, (1, cols), table(*lanes), blends], [], *(marks, rhs, *stiff, up, *got_edges)
    )
    (got_next,) = run(ahead_kernel, [message], [left(2)], next_lanes, next_blend, next_field)
    field, local, to0, to1, *rest = run(
        functools.partial(first_kernel, two),
        common + [(4, nb, LANES), table(*lanes), mask, mask, blends],
        [left(2)],
        *(marks, rhs, base, up, own_lanes, own_high, got_next, up0, up1),
    )
    edges, prev = rest[:n_edges], rest[n_edges:]

    for step in range(1, ITERS):
        last = step == ITERS - 1
        got0, got1, got_edges = exchange(to0, to1, edges)
        base, *partial = run(
            functools.partial(between_kernel, last, n_edges, scale),
            [field_shape] + ([(1, LANES)] if last else []),
            [],
            *(marks, field, *stiff, rim, *got_edges, *(basis if last else [])),
        )
        if last:
            (sums,) = run(
                functools.partial(sum_kernel, scale),
                [(n_gz * n_xy, LANES)],
                [],
                marks, *partial,
                local,
                got0,
                got1,
            )
            sums = lax.all_to_all(sums.reshape(n_gz * n_xy, 1, LANES), ("gz", "xy"), 0, 0)
            sums = sums.reshape(n_gz * n_xy, LANES)
        field_next, *rest = run(
            functools.partial(step_kernel, last, two),
            [field_shape] if last else common,
            [] if last else [left(2)],
            *(marks, field, base, own_lanes, own_high, *prev, local, got0, got1),
        )
        basis.append(field)
        field = field_next
        if not last:
            local, to0, to1, *edges = rest
    basis.append(field)
    solution_field, residual = call(finish_kernel, [VMEM] * (1 + len(basis)), [field_shape] * 2)(sums, *basis)
    return solution_field[:, None], residual[:, None]


def solution(mesh):
    in_specs = (
        P(None, "gz", "xy", None),
        P("gz", "xy", None),
        P("gz", "xy", None),
        P("gz", "xy", None),
        P("gz", "xy", None),
        P("gz", "xy", None),
        P(None, "gz", "xy", None),
        P("gz", "xy"),
    )
    out_specs = (P(None, "gz", "xy", None), P(None, "gz", "xy", None))
    return jax.shard_map(body, mesh=mesh, in_specs=in_specs, out_specs=out_specs, check_vma=False)
```

```python
import functools
import math

import jax
import jax.numpy as jnp
from jax import lax
from jax.experimental import pallas as pl
from jax.experimental.pallas import tpu as pltpu
from jax.sharding import PartitionSpec as P


BLOCK = 128
ITERS = 3
LANES = 128
WIDE = 256
GAIN = 0.25
SHIFT = 1.25
F32 = jnp.float32
BF16 = jnp.bfloat16
CHUNK = 256


def swapped(block, axis, first):
    count = lax.axis_size(axis)
    route = []
    for i in range(first, count - 1, 2):
        route += [(i, i + 1), (i + 1, i)]
    return lax.ppermute(block, axis, route) if route else None


def swapped_sections(block, first):
    count, width = lax.axis_size("gz"), lax.axis_size("xy")
    route = []
    for i in range(first, count - 1, 2):
        for j in range(width):
            a, b = i * width + j, (i + 1) * width + j
            route += [(a, b), (b, a)]
    paired = {a for a, _ in route}
    for a in range(0, count * width - 1, 2):
        if a not in paired and a + 1 not in paired and a // width == (a + 1) // width:
            route += [(a, a + 1), (a + 1, a)]
    return lax.ppermute(block, ("gz", "xy"), route)


def split2(x):
    high = x.astype(BF16)
    return high, (x - high.astype(F32)).astype(BF16)


def div_mod(x, d):
    if d & (d - 1) == 0:
        return lax.shift_right_logical(x, jnp.int32(d.bit_length() - 1)), x & (d - 1)
    q = lax.div(x, jnp.int32(d))
    return q, x - q * d


def hi_lo(index, rows, cols):
    row, col = div_mod(index, cols)
    tile, lane = div_mod(col, WIDE)
    return tile * rows + row, lane


def row_of(tile, k):
    return tile[k : k + 1, :]


def one_hot(index, size, shift=0):
    at = lax.broadcasted_iota(jnp.int32, (size, LANES), 0) - shift
    return jnp.concatenate(
        [jnp.where(at == row_of(index, k), 1.0, 0.0).astype(BF16) for k in range(index.shape[0])],
        axis=1,
    )


def blend(index, size, first, second):
    at = lax.broadcasted_iota(jnp.int32, (size, LANES), 0)
    out = []
    for k in range(index.shape[0]):
        here = row_of(index, k)
        out.append(
            jnp.where(at == here, row_of(first, k), jnp.where(at == here + 1, row_of(second, k), 0.0))
        )
    return jnp.concatenate(out, axis=1)


def store_lanes(lo, lanes_ref):
    lanes_ref[...] = one_hot(lo, WIDE)


def tall(field):
    n = field.shape[1] // WIDE
    return jnp.concatenate([field[:, i * WIDE : (i + 1) * WIDE] for i in range(n)], axis=0)


def wide(stack, rows):
    n = stack.shape[0] // rows
    return jnp.concatenate([stack[i * rows : (i + 1) * rows, :] for i in range(n)], axis=1)


def right_of(field):
    return pltpu.roll(field, field.shape[1] - 1, 1)


def load_left(field, left_ref, sides):
    fields = []
    for c in range(2):
        fields += [field[c], right_of(field[c])] if sides == 2 else [field[c]]
    for i, f in enumerate(fields):
        stack = tall(f)
        high, low = split2(stack)
        n = stack.shape[0]
        left_ref[2 * i * n : (2 * i + 1) * n, :] = high
        left_ref[(2 * i + 1) * n : (2 * i + 2) * n, :] = low


def as_tiles(rows_of):
    return jnp.concatenate(
        [r[:, i * LANES : (i + 1) * LANES] for r in rows_of for i in range(CHUNK // LANES)], axis=0
    )


def looked_up(left_ref, lanes_ref, high_ref):
    high, slots = high_ref.shape
    stride = left_ref.shape[0] // 2
    found = ([], [])
    for k in range(0, slots, CHUNK):
        hot = lanes_ref[:, k : k + CHUNK]
        mask = high_ref[:, k : k + CHUNK]
        for c in range(2):
            got = jnp.dot(
                left_ref[c * stride : c * stride + 2 * high, :],
                hot,
                preferred_element_type=F32,
            )
            value = mask * (got[:high] + got[high:])
            found[c].append(jnp.sum(value, axis=0, keepdims=True))
    return jnp.stack([as_tiles(f) for f in found])


def interpolated(left_ref, lanes_ref, blend_ref):
    high, slots = blend_ref.shape[1:]
    found = ([], [])
    for k in range(0, slots, CHUNK):
        hot = lanes_ref[:, k : k + CHUNK]
        wl = blend_ref[0, :, k : k + CHUNK]
        wr = blend_ref[1, :, k : k + CHUNK]
        for c in range(2):
            got = jnp.dot(
                left_ref[4 * c * high : 4 * (c + 1) * high, :],
                hot,
                preferred_element_type=F32,
            )
            value = wl * (got[:high] + got[high : 2 * high]) + wr * (got[2 * high : 3 * high] + got[3 * high :])
            found[c].append(jnp.sum(value, axis=0, keepdims=True))
    return jnp.stack([as_tiles(f) for f in found])


NT = (((1,), (1,)), ((), ()))


def scaled(mask_ref, tile):
    return jnp.concatenate(
        [mask_ref[:, k * LANES : (k + 1) * LANES] * row_of(tile, k) for k in range(tile.shape[0])],
        axis=1,
    )


def spread_own(values, lanes_ref, high_ref, rows):
    high = high_ref.shape[0]
    parts = [scaled(high_ref, part.astype(F32)).astype(BF16) for c in range(2) for part in split2(values[c])]
    out = lax.dot_general(jnp.concatenate(parts, axis=0), lanes_ref[...], NT, preferred_element_type=F32)
    return [
        wide(out[2 * c * high : (2 * c + 1) * high] + out[(2 * c + 1) * high : (2 * c + 2) * high], rows)
        for c in range(2)
    ]


def spread_own_apart(values, lanes_ref, high_ref, rows):
    high = high_ref.shape[0]
    result = []
    for c in range(2):
        parts = [scaled(high_ref, part.astype(F32)).astype(BF16) for part in split2(values[c])]
        out = lax.dot_general(
            jnp.concatenate(parts, axis=0), lanes_ref[...], NT, preferred_element_type=F32
        )
        result.append(wide(out[:high] + out[high:], rows))
    return result


def spread_corners(values, weights, lanes_ref, high_ref, below_ref, rows):
    high = high_ref.shape[0]
    result = []
    for c in range(2):
        parts = []
        for side in range(2):
            for up, down in zip(split2(values[c] * weights[side]), split2(values[c] * weights[2 + side])):
                part = scaled(high_ref, up.astype(F32)) + scaled(below_ref, down.astype(F32))
                parts.append(part.astype(BF16))
        out = lax.dot_general(
            jnp.concatenate(parts, axis=0), lanes_ref[...], NT, preferred_element_type=F32
        )
        sides = [
            wide(out[p * high : (p + 1) * high] + out[(p + 1) * high : (p + 2) * high], rows)
            for p in (0, 2)
        ]
        result.append(sides[0] + pltpu.roll(sides[1], 1, 1))
    return result


def springs(field, across, down, hold, upper_row, lower_row, rim):
    rows, cols = field.shape
    col = lax.broadcasted_iota(jnp.int32, (rows, cols), 1)
    row = lax.broadcasted_iota(jnp.int32, (rows, cols), 0)
    right = jnp.where(col == cols - 1, 0.0, pltpu.roll(field, cols - 1, 1))
    pull = across * (field - right)
    out = pull - jnp.where(col == 0, 0.0, pltpu.roll(pull, 1, 1))
    lower = jnp.where(row == rows - 1, lower_row, pltpu.roll(field, rows - 1, 0))
    pull = down * (field - lower)
    above = rim * (upper_row - field[0:1, :])
    out = out + pull - jnp.where(row == 0, above, pltpu.roll(pull, 1, 0))
    return out + hold * field


def mark(marks, i):
    return marks[i, 0:1, 0:1]


def pick(flag, a, b):
    return jnp.where(jnp.broadcast_to(flag, a.shape) > 0.5, a, b)


def edges_of(get_row, rows, even_b, two):
    first = [get_row(c, 0) for c in range(2)]
    last = [get_row(c, rows - 1) for c in range(2)]
    out = [jnp.concatenate([pick(even_b, last[c], first[c]) for c in range(2)], axis=0)]
    if two:
        out.append(jnp.concatenate([pick(even_b, first[c], last[c]) for c in range(2)], axis=0))
    return out


def prepare_kernel(two, count, field, across, down, hold, source, target, weights, *refs):
    outs, (left, ids, held, sems) = refs[:-4], refs[-4:]
    field_out, across_out, down_out, hold_out, up, marks, own_lanes, own_high, *edges = outs
    pairs = [(source, ids.at[0]), (field, field_out), (down, down_out)]
    pairs += [(target, ids.at[1]), (weights, held), (across, across_out), (hold, hold_out)]
    copies = [pltpu.make_async_copy(a, b, sems.at[i]) for i, (a, b) in enumerate(pairs)]
    for copy in copies:
        copy.start()
    rows, cols = across_out.shape
    nb, size = ids.shape[1], own_high.shape[0]
    at_gz, at_xy = lax.axis_index("gz"), lax.axis_index("xy")
    as_mark = lambda flag: jnp.full((nb, LANES), flag.astype(jnp.int32)).astype(F32)
    copies[0].wait()
    hi, lo = hi_lo(ids[0], rows, cols)
    store_lanes(lo, own_lanes)
    own_high[...] = one_hot(hi, size).astype(F32)
    copies[1].wait()
    load_left([field_out[0], field_out[1]], left, 1)
    own = looked_up(left, own_lanes, own_high)
    for copy in copies[2:]:
        copy.wait()
    has_next = (at_gz < lax.axis_size("gz") - 1).astype(jnp.int32)
    block = lax.broadcasted_iota(jnp.int32, (nb, LANES), 0)
    live = jnp.where(block * LANES < count[0, 0] * BLOCK * has_next, 1.0, 0.0)
    marks[0] = as_mark(1 - lax.rem(at_gz, 2))
    marks[1] = as_mark(1 - lax.rem(at_xy, 2))
    marks[2] = as_mark(at_gz > 0)
    marks[3] = live
    parts = [own[0], own[1], ids[1].astype(F32)] + [held[q] * live for q in range(4)]
    for i, part in enumerate(parts):
        up[:, i * LANES : (i + 1) * LANES] = part
    even_b = mark(marks, 1)
    messages = edges_of(lambda c, r: field_out[c, r : r + 1, :], rows, even_b, two)
    for message, edge in zip(messages, edges):
        edge[0:2, :] = message
        edge[2:3, :] = down_out[rows - 1 : rows, :]


def tile_of(up, i):
    return up[:, i * LANES : (i + 1) * LANES]


def halves(flags, edge_refs):
    even_b = mark(flags, 1)
    zero = edge_refs[0][...]
    if len(edge_refs) == 2:
        other = edge_refs[1][...]
    else:
        other = jnp.zeros_like(zero)
    return pick(even_b, other, zero), pick(even_b, zero, other)


def spring_image(field, across, down, hold, above, below, rim):
    return [
        springs(
            field[c], across[...], down[...], hold[...], above[c : c + 1], below[c : c + 1], rim
        )
        for c in range(2)
    ]


def early_kernel(flags, field_ref, across, down, hold, up, *refs):
    edge_refs, (base, rim_ref, next_lanes, next_blend) = refs[:-4], refs[-4:]
    rows, cols = across.shape
    field = [field_ref[0], field_ref[1]]
    above, below = halves(flags, edge_refs)
    image = spring_image(field, across, down, hold, above, below, above[2:3, :])
    for c in range(2):
        base[c] = image[c]
    rim_ref[...] = above[2:3, :]
    hi, lo = hi_lo(tile_of(up, 2).astype(jnp.int32), rows, cols)
    store_lanes(lo, next_lanes)
    for side in range(2):
        next_blend[side] = blend(hi, next_blend.shape[1], tile_of(up, 3 + side), tile_of(up, 5 + side))


def ahead_kernel(next_lanes, next_blend, next_field, out, left):
    load_left([next_field[0], next_field[1]], left, 2)
    out[...] = interpolated(left, next_lanes, next_blend)


def send_on(even, even_b, two, field, own_tables, prev_tables, left, local_ref, send0, send1, *edges):
    own_lanes, own_high = own_tables
    prev_lanes, prev_blend = prev_tables
    load_left(field, left, 2)
    own = looked_up(left, own_lanes, own_high)
    mid = interpolated(left, prev_lanes, prev_blend)
    local_ref[0] = own
    local_ref[1] = mid
    send0[...] = pick(even, own, mid)
    send1[...] = pick(even, mid, own)
    messages = edges_of(lambda c, r: field[c][r : r + 1, :], field[0].shape[0], even_b, two)
    for message, edge in zip(messages, edges):
        edge[...] = message


def stepped(field_ref, image):
    return [GAIN * image[c] - SHIFT * field_ref[c] for c in range(2)]


def first_kernel(
    two, flags, field_ref, base, up, own_lanes, own_high, got_next, up0, up1, *refs
):
    refs, left = refs[:-1], refs[-1]
    out, local_ref, send0, send1, *edges = refs[:-5]
    prev_weights, prev_lanes, prev_high, prev_below, prev_blend = refs[-5:]
    even, even_b = mark(flags, 0), mark(flags, 1)
    rows, cols = field_ref.shape[1:]
    size = own_high.shape[0]
    got_up = pick(even, up1[...], up0[...])
    weights = [tile_of(got_up, 3 + q) * flags[2] for q in range(4)]
    for q in range(4):
        prev_weights[q] = weights[q]
    hi, lo = hi_lo(tile_of(got_up, 2).astype(jnp.int32), rows, cols)
    store_lanes(lo, prev_lanes)
    prev_high[...] = one_hot(hi, size).astype(F32)
    prev_below[...] = one_hot(hi, size, 1).astype(F32)
    for side in range(2):
        prev_blend[side] = blend(hi, size, weights[side], weights[2 + side])
    load_left([field_ref[0], field_ref[1]], left, 2)
    mid = interpolated(left, prev_lanes, prev_blend)
    own = [tile_of(up, c) for c in range(2)]
    got_prev = [tile_of(got_up, c) for c in range(2)]
    live = flags[3]
    pulled = spread_own_apart([live * (own[c] - got_next[c]) for c in range(2)], own_lanes, own_high, rows)
    error = [mid[c] - got_prev[c] for c in range(2)]
    pushed = spread_corners(error, weights, prev_lanes, prev_high, prev_below, rows)
    after = stepped(field_ref, [base[c] + pulled[c] + pushed[c] for c in range(2)])
    for c in range(2):
        out[c] = after[c]
    send_on(
        even,
        even_b,
        two,
        after,
        (own_lanes, own_high),
        (prev_lanes, prev_blend),
        left,
        local_ref,
        send0,
        send1,
        *edges,
    )


def moment_scale(slots):
    bound = GAIN * (8 * 3.0 + 0.2 + 4 * slots) + SHIFT
    return 0.5 ** math.ceil(2.5 * math.log2(bound))


def moments_of(pairs, scale, start=0):
    lane = lax.broadcasted_iota(jnp.int32, (1, LANES), 1)
    total = jnp.zeros((1, LANES), F32)
    for i, (u, w) in enumerate(pairs):
        s = (u[0] * scale) * (w[0] * scale) + (u[1] * scale) * (w[1] * scale)
        s = jnp.sum(jnp.sum(s, axis=0, keepdims=True), axis=1, keepdims=True)
        total = total + jnp.where(lane == start + i, s, 0.0)
    return total


def between_kernel(last, n_edges, scale, flags, field_ref, across, down, hold, rim, *refs):
    refs = list(refs)
    edge_refs = [refs.pop(0) for _ in range(n_edges)]
    earlier = [refs.pop(0) for _ in range(ITERS - 1)] if last else []
    field = [field_ref[0], field_ref[1]]
    above, below = halves(flags, edge_refs)
    image = spring_image(field, across, down, hold, above, below, rim[...])
    base = refs.pop(0)
    for c in range(2):
        base[c] = image[c]
    if last:
        basis = [(ref[0], ref[1]) for ref in earlier] + [field, image]
        refs.pop(0)[...] = moments_of(
            [(basis[i // 2], basis[i - i // 2]) for i in range(2 * ITERS)], scale
        )


def errors_of(flags, local, got0, got1):
    even, live = mark(flags, 0), flags[3]
    got_next = pick(even, got0[...], got1[...])
    got_prev = pick(even, got1[...], got0[...])
    return (
        [live * (local[0, c] - got_next[c]) for c in range(2)],
        [local[1, c] - got_prev[c] for c in range(2)],
    )


def sum_kernel(scale, flags, partial, local, got0, got1, sums):
    own, prev = errors_of(flags, local, got0, got1)
    pairs = [(own[c], local[0, c]) for c in range(2)] + [(prev[c], local[1, c]) for c in range(2)]
    s = sum((a * scale) * (b * scale) for a, b in pairs)
    s = jnp.sum(jnp.sum(s, axis=0, keepdims=True), axis=1, keepdims=True)
    lane = lax.broadcasted_iota(jnp.int32, (1, LANES), 1)
    at = 2 * ITERS - 1
    before = jnp.sum(jnp.where(lane == at - 1, partial[...], 0.0), axis=1, keepdims=True)
    total = jnp.where(lane == at, GAIN * (partial[...] + s) - SHIFT * before, partial[...])
    sums[...] = jnp.broadcast_to(total, sums.shape)


def step_kernel(
    flags,
    field_ref,
    base,
    own_lanes,
    own_high,
    prev_weights,
    prev_lanes,
    prev_high,
    prev_below,
    prev_blend,
    local,
    got0,
    got1,
    out,
):
    rows = field_ref.shape[1]
    error, error_prev = errors_of(flags, local, got0, got1)
    pulled = spread_own(error, own_lanes, own_high, rows)
    weights = [prev_weights[q] for q in range(4)]
    pushed = spread_corners(error_prev, weights, prev_lanes, prev_high, prev_below, rows)
    after = stepped(field_ref, [base[c] + pulled[c] + pushed[c] for c in range(2)])
    for c in range(2):
        out[c] = after[c]


def send_kernel(two, flags, field_ref, own_lanes, own_high, prev_lanes, prev_blend, *refs):
    messages, left = refs[:-1], refs[-1]
    send_on(
        mark(flags, 0),
        mark(flags, 1),
        two,
        [field_ref[0], field_ref[1]],
        (own_lanes, own_high),
        (prev_lanes, prev_blend),
        left,
        *messages,
    )


def conjugate(moments):
    def apply(p):
        shifted = [None] + p
        return [
            (SHIFT * p[k] if k < len(p) else 0.0) * (1.0 / GAIN)
            + ((1.0 / GAIN) * shifted[k] if k else 0.0)
            for k in range(len(p) + 1)
        ]

    def product(p, q):
        return sum(p[i] * q[j] * moments[i + j] for i in range(len(p)) for j in range(len(q)))

    def plus(p, factor, q):
        size = max(len(p), len(q))
        pad = lambda a: a + [None] * (size - len(a))
        out = []
        for a, b in zip(pad(p), pad(q)):
            out.append(factor * b if a is None else a if b is None else a + factor * b)
        return out

    one = jnp.ones_like(moments[0])
    solution_field, residual, direction = [], [one], [one]
    norm_now = moments[0]
    for step in range(ITERS):
        image = apply(direction)
        alpha = norm_now / product(direction, image)
        solution_field = plus(solution_field, alpha, direction)
        residual = plus(residual, -alpha, image)
        if step + 1 < ITERS:
            norm_next = product(residual, residual)
            direction = plus(residual, norm_next / norm_now, direction)
            norm_now = norm_next
    return solution_field, residual


def finish_kernel(sums, *refs):
    basis, (solution_ref, residual_ref) = refs[: ITERS + 1], refs[ITERS + 1 :]
    total = jnp.sum(sums[...], axis=0, keepdims=True)
    lane = lax.broadcasted_iota(jnp.int32, (1, LANES), 1)
    moments = [
        jnp.sum(jnp.where(lane == i, total, 0.0), axis=1, keepdims=True) for i in range(2 * ITERS)
    ]
    solution_field, residual = conjugate(moments)
    for c in range(2):
        values = [ref[c] for ref in basis]
        solution_ref[c] = sum(a * v for a, v in zip(solution_field, values))
        residual_ref[c] = sum(a * v for a, v in zip(residual, values))


VMEM = pl.BlockSpec(memory_space=pltpu.VMEM)
SMEM = pl.BlockSpec(memory_space=pltpu.SMEM)
HBM = pl.BlockSpec(memory_space=pltpu.HBM)


def call(kernel, in_specs, shapes, scratch=()):
    shapes = [s if isinstance(s, jax.ShapeDtypeStruct) else jax.ShapeDtypeStruct(s, F32) for s in shapes]
    return pl.pallas_call(
        kernel,
        in_specs=in_specs,
        out_specs=[VMEM] * len(shapes),
        out_shape=shapes,
        scratch_shapes=list(scratch),
        compiler_params=pltpu.CompilerParams(vmem_limit_bytes=48 * 1024 * 1024),
    )


def body(
    right_side,
    stiff_across,
    stiff_down,
    anchor,
    source_node,
    target_cell,
    corner_weight,
    block_count,
):
    rows, cols = stiff_across.shape[1:]
    rhs = right_side[:, 0]
    across, down, hold = stiff_across[0], stiff_down[0], anchor[0]
    slots = source_node.shape[2]
    nb = slots // LANES
    source = source_node.reshape(nb, LANES)
    target = target_cell.reshape(nb, LANES)
    weights = corner_weight.reshape(4, nb, LANES)
    n_gz, n_xy = lax.axis_size("gz"), lax.axis_size("xy")
    two = n_xy > 2
    n_edges = 2 if two else 1

    def exchange(to0, to1, edges):
        got1 = swapped_sections(to1, 1)
        got0 = swapped_sections(to0, 0)
        got_edges = []
        for i, edge in enumerate(edges):
            got_edges.append(swapped(edge, "xy", i))
        return got0, got1, got_edges

    field_shape = (2, rows, cols)
    message = (2, nb, LANES)
    scale = moment_scale(slots)
    size = rows * cols // WIDE
    common = [field_shape, (2,) + message, message, message] + [(2, cols)] * n_edges
    table = lambda *shape: jax.ShapeDtypeStruct(shape, BF16)
    left = lambda sides: pltpu.VMEM((4 * sides * size, WIDE), BF16)
    lanes, mask, blends = (WIDE, slots), (size, slots), (2, size, slots)
    run = lambda kernel, shapes, scratch, *args: call(kernel, [VMEM] * len(args), shapes, scratch)(*args)
    next_field = lax.ppermute(rhs, "gz", [(i, (i - 1) % n_gz) for i in range(n_gz)])
    in_hbm = lambda *arrays: [pltpu.with_memory_space_constraint(a, pltpu.HBM) for a in arrays]
    grid = (rows, cols)
    rhs, across, down, hold, up, marks, own_lanes, own_high, *edges = call(
        functools.partial(prepare_kernel, two),
        [SMEM] + [HBM] * 7,
        [field_shape, grid, grid, grid, (nb, 7 * LANES), (4, nb, LANES), table(*lanes), mask]
        + [(4, cols)] * n_edges,
        [
            left(1),
            pltpu.VMEM((2, nb, LANES), jnp.int32),
            pltpu.VMEM((4, nb, LANES), F32),
            pltpu.SemaphoreType.DMA((7,)),
        ],
    )(block_count, *in_hbm(rhs, across, down, hold, source, target, weights))
    stiff = (across, down, hold)
    basis = [rhs]
    up1 = swapped_sections(up, 1)
    up0 = swapped_sections(up, 0)
    got_edges = []
    for i, edge in enumerate(edges):
        got_edges.append(swapped(edge, "xy", i))
    base, rim, next_lanes, next_blend = run(
        early_kernel, [field_shape, (1, cols), table(*lanes), blends], [], *(marks, rhs, *stiff, up, *got_edges)
    )
    (got_next,) = run(ahead_kernel, [message], [left(2)], next_lanes, next_blend, next_field)
    field, local, to0, to1, *rest = run(
        functools.partial(first_kernel, two),
        common + [(4, nb, LANES), table(*lanes), mask, mask, blends],
        [left(2)],
        *(marks, rhs, base, up, own_lanes, own_high, got_next, up0, up1),
    )
    edges, prev = rest[:n_edges], rest[n_edges:]

    for step in range(1, ITERS):
        last = step == ITERS - 1
        got0, got1, got_edges = exchange(to0, to1, edges)
        base, *partial = run(
            functools.partial(between_kernel, last, n_edges, scale),
            [field_shape] + ([(1, LANES)] if last else []),
            [],
            *(marks, field, *stiff, rim, *got_edges, *(basis if last else [])),
        )
        if last:
            (sums,) = run(
                functools.partial(sum_kernel, scale),
                [(n_gz * n_xy, LANES)],
                [],
                marks, *partial,
                local,
                got0,
                got1,
            )
            sums = lax.all_to_all(sums.reshape(n_gz * n_xy, 1, LANES), ("gz", "xy"), 0, 0)
            sums = sums.reshape(n_gz * n_xy, LANES)
        (field_next,) = run(
            step_kernel, [field_shape], [], *(marks, field, base, own_lanes, own_high, *prev, local, got0, got1)
        )
        basis.append(field)
        field = field_next
        if not last:
            local, to0, to1, *edges = run(
                functools.partial(send_kernel, two),
                common[1:],
                [left(2)],
                *(marks, field, own_lanes, own_high, prev[1], prev[4]),
            )
    basis.append(field)
    solution_field, residual = call(finish_kernel, [VMEM] * (1 + len(basis)), [field_shape] * 2)(sums, *basis)
    return solution_field[:, None], residual[:, None]


def solution(mesh):
    in_specs = (
        P(None, "gz", "xy", None),
        P("gz", "xy", None),
        P("gz", "xy", None),
        P("gz", "xy", None),
        P("gz", "xy", None),
        P("gz", "xy", None),
        P(None, "gz", "xy", None),
        P("gz", "xy"),
    )
    out_specs = (P(None, "gz", "xy", None), P(None, "gz", "xy", None))
    return jax.shard_map(body, mesh=mesh, in_specs=in_specs, out_specs=out_specs, check_vma=False)
```

```python
import functools
import math

import jax
import jax.numpy as jnp
from jax import lax
from jax.experimental import pallas as pl
from jax.experimental.pallas import tpu as pltpu
from jax.sharding import PartitionSpec as P


BLOCK = 128
ITERS = 3
LANES = 128
WIDE = 256
GAIN = 0.25
SHIFT = 1.25
F32 = jnp.float32
BF16 = jnp.bfloat16
CHUNK = 256


def swapped(block, axis, first):
    count = lax.axis_size(axis)
    route = []
    for i in range(first, count - 1, 2):
        route += [(i, i + 1), (i + 1, i)]
    return lax.ppermute(block, axis, route) if route else None


def swapped_sections(block, first):
    count, width = lax.axis_size("gz"), lax.axis_size("xy")
    route = []
    for i in range(first, count - 1, 2):
        for j in range(width):
            a, b = i * width + j, (i + 1) * width + j
            route += [(a, b), (b, a)]
    paired = {a for a, _ in route}
    for a in range(0, count * width - 1, 2):
        if a not in paired and a + 1 not in paired and a // width == (a + 1) // width:
            route += [(a, a + 1), (a + 1, a)]
    return lax.ppermute(block, ("gz", "xy"), route)


def split2(x):
    high = x.astype(BF16)
    return high, (x - high.astype(F32)).astype(BF16)


def div_mod(x, d):
    if d & (d - 1) == 0:
        return lax.shift_right_logical(x, jnp.int32(d.bit_length() - 1)), x & (d - 1)
    q = lax.div(x, jnp.int32(d))
    return q, x - q * d


def hi_lo(index, rows, cols):
    row, col = div_mod(index, cols)
    tile, lane = div_mod(col, WIDE)
    return tile * rows + row, lane


def row_of(tile, k):
    return tile[k : k + 1, :]


def one_hot(index, size, shift=0):
    at = lax.broadcasted_iota(jnp.int32, (size, LANES), 0) - shift
    return jnp.concatenate(
        [jnp.where(at == row_of(index, k), 1.0, 0.0).astype(BF16) for k in range(index.shape[0])],
        axis=1,
    )


def blend(index, size, first, second):
    at = lax.broadcasted_iota(jnp.int32, (size, LANES), 0)
    out = []
    for k in range(index.shape[0]):
        here = row_of(index, k)
        out.append(
            jnp.where(at == here, row_of(first, k), jnp.where(at == here + 1, row_of(second, k), 0.0))
        )
    return jnp.concatenate(out, axis=1)


def store_lanes(lo, lanes_ref):
    lanes_ref[...] = one_hot(lo, WIDE)


def tall(field):
    n = field.shape[1] // WIDE
    return jnp.concatenate([field[:, i * WIDE : (i + 1) * WIDE] for i in range(n)], axis=0)


def wide(stack, rows):
    n = stack.shape[0] // rows
    return jnp.concatenate([stack[i * rows : (i + 1) * rows, :] for i in range(n)], axis=1)


def right_of(field):
    return pltpu.roll(field, field.shape[1] - 1, 1)


def load_left(field, left_ref, sides):
    fields = []
    for c in range(2):
        fields += [field[c], right_of(field[c])] if sides == 2 else [field[c]]
    for i, f in enumerate(fields):
        stack = tall(f)
        high, low = split2(stack)
        n = stack.shape[0]
        left_ref[2 * i * n : (2 * i + 1) * n, :] = high
        left_ref[(2 * i + 1) * n : (2 * i + 2) * n, :] = low


def as_tiles(rows_of):
    return jnp.concatenate(
        [r[:, i * LANES : (i + 1) * LANES] for r in rows_of for i in range(CHUNK // LANES)], axis=0
    )


def looked_up(left_ref, lanes_ref, high_ref):
    high, slots = high_ref.shape
    stride = left_ref.shape[0] // 2
    found = ([], [])
    for k in range(0, slots, CHUNK):
        hot = lanes_ref[:, k : k + CHUNK]
        mask = high_ref[:, k : k + CHUNK]
        rows_of = [left_ref[c * stride : c * stride + 2 * high, :] for c in range(2)]
        got = jnp.dot(jnp.concatenate(rows_of, axis=0), hot, preferred_element_type=F32)
        for c in range(2):
            part = got[2 * c * high : 2 * (c + 1) * high]
            found[c].append(jnp.sum(mask * (part[:high] + part[high:]), axis=0, keepdims=True))
    return jnp.stack([as_tiles(f) for f in found])


def interpolated(left_ref, lanes_ref, blend_ref):
    high, slots = blend_ref.shape[1:]
    found = ([], [])
    for k in range(0, slots, CHUNK):
        hot = lanes_ref[:, k : k + CHUNK]
        wl = blend_ref[0, :, k : k + CHUNK]
        wr = blend_ref[1, :, k : k + CHUNK]
        for c in range(2):
            got = jnp.dot(
                left_ref[4 * c * high : 4 * (c + 1) * high, :],
                hot,
                preferred_element_type=F32,
            )
            value = wl * (got[:high] + got[high : 2 * high]) + wr * (got[2 * high : 3 * high] + got[3 * high :])
            found[c].append(jnp.sum(value, axis=0, keepdims=True))
    return jnp.stack([as_tiles(f) for f in found])


NT = (((1,), (1,)), ((), ()))


def scaled(mask_ref, tile):
    return jnp.concatenate(
        [mask_ref[:, k * LANES : (k + 1) * LANES] * row_of(tile, k) for k in range(tile.shape[0])],
        axis=1,
    )


def spread_own(values, lanes_ref, high_ref, rows):
    high = high_ref.shape[0]
    parts = [scaled(high_ref, part.astype(F32)).astype(BF16) for c in range(2) for part in split2(values[c])]
    out = lax.dot_general(jnp.concatenate(parts, axis=0), lanes_ref[...], NT, preferred_element_type=F32)
    return [
        wide(out[2 * c * high : (2 * c + 1) * high] + out[(2 * c + 1) * high : (2 * c + 2) * high], rows)
        for c in range(2)
    ]


def spread_own_apart(values, lanes_ref, high_ref, rows):
    high = high_ref.shape[0]
    result = []
    for c in range(2):
        parts = [scaled(high_ref, part.astype(F32)).astype(BF16) for part in split2(values[c])]
        out = lax.dot_general(
            jnp.concatenate(parts, axis=0), lanes_ref[...], NT, preferred_element_type=F32
        )
        result.append(wide(out[:high] + out[high:], rows))
    return result


def spread_corners(values, weights, lanes_ref, high_ref, below_ref, rows):
    high = high_ref.shape[0]
    result = []
    for c in range(2):
        parts = []
        for side in range(2):
            for up, down in zip(split2(values[c] * weights[side]), split2(values[c] * weights[2 + side])):
                part = scaled(high_ref, up.astype(F32)) + scaled(below_ref, down.astype(F32))
                parts.append(part.astype(BF16))
        out = lax.dot_general(
            jnp.concatenate(parts, axis=0), lanes_ref[...], NT, preferred_element_type=F32
        )
        sides = [
            wide(out[p * high : (p + 1) * high] + out[(p + 1) * high : (p + 2) * high], rows)
            for p in (0, 2)
        ]
        result.append(sides[0] + pltpu.roll(sides[1], 1, 1))
    return result


def springs(field, across, down, hold, upper_row, lower_row, rim):
    rows, cols = field.shape
    col = lax.broadcasted_iota(jnp.int32, (rows, cols), 1)
    row = lax.broadcasted_iota(jnp.int32, (rows, cols), 0)
    right = jnp.where(col == cols - 1, 0.0, pltpu.roll(field, cols - 1, 1))
    pull = across * (field - right)
    out = pull - jnp.where(col == 0, 0.0, pltpu.roll(pull, 1, 1))
    lower = jnp.where(row == rows - 1, lower_row, pltpu.roll(field, rows - 1, 0))
    pull = down * (field - lower)
    above = rim * (upper_row - field[0:1, :])
    out = out + pull - jnp.where(row == 0, above, pltpu.roll(pull, 1, 0))
    return out + hold * field


def mark(marks, i):
    return marks[i, 0:1, 0:1]


def pick(flag, a, b):
    return jnp.where(jnp.broadcast_to(flag, a.shape) > 0.5, a, b)


def edges_of(get_row, rows, even_b, two):
    first = [get_row(c, 0) for c in range(2)]
    last = [get_row(c, rows - 1) for c in range(2)]
    out = [jnp.concatenate([pick(even_b, last[c], first[c]) for c in range(2)], axis=0)]
    if two:
        out.append(jnp.concatenate([pick(even_b, first[c], last[c]) for c in range(2)], axis=0))
    return out


def prepare_kernel(two, count, field, across, down, hold, source, target, weights, *refs):
    outs, (left, ids, held, sems) = refs[:-4], refs[-4:]
    field_out, across_out, down_out, hold_out, up, marks, own_lanes, own_high, *edges = outs
    pairs = [(source, ids.at[0]), (field, field_out), (down, down_out)]
    pairs += [(target, ids.at[1]), (weights, held), (across, across_out), (hold, hold_out)]
    copies = [pltpu.make_async_copy(a, b, sems.at[i]) for i, (a, b) in enumerate(pairs)]
    for copy in copies:
        copy.start()
    rows, cols = across_out.shape
    nb, size = ids.shape[1], own_high.shape[0]
    at_gz, at_xy = lax.axis_index("gz"), lax.axis_index("xy")
    as_mark = lambda flag: jnp.full((nb, LANES), flag.astype(jnp.int32)).astype(F32)
    copies[0].wait()
    hi, lo = hi_lo(ids[0], rows, cols)
    store_lanes(lo, own_lanes)
    own_high[...] = one_hot(hi, size).astype(F32)
    copies[1].wait()
    load_left([field_out[0], field_out[1]], left, 1)
    own = looked_up(left, own_lanes, own_high)
    for copy in copies[2:]:
        copy.wait()
    has_next = (at_gz < lax.axis_size("gz") - 1).astype(jnp.int32)
    block = lax.broadcasted_iota(jnp.int32, (nb, LANES), 0)
    live = jnp.where(block * LANES < count[0, 0] * BLOCK * has_next, 1.0, 0.0)
    marks[0] = as_mark(1 - lax.rem(at_gz, 2))
    marks[1] = as_mark(1 - lax.rem(at_xy, 2))
    marks[2] = as_mark(at_gz > 0)
    marks[3] = live
    parts = [own[0], own[1], ids[1].astype(F32)] + [held[q] * live for q in range(4)]
    for i, part in enumerate(parts):
        up[:, i * LANES : (i + 1) * LANES] = part
    even_b = mark(marks, 1)
    messages = edges_of(lambda c, r: field_out[c, r : r + 1, :], rows, even_b, two)
    for message, edge in zip(messages, edges):
        edge[0:2, :] = message
        edge[2:3, :] = down_out[rows - 1 : rows, :]


def tile_of(up, i):
    return up[:, i * LANES : (i + 1) * LANES]


def halves(flags, edge_refs):
    even_b = mark(flags, 1)
    zero = edge_refs[0][...]
    if len(edge_refs) == 2:
        other = edge_refs[1][...]
    else:
        other = jnp.zeros_like(zero)
    return pick(even_b, other, zero), pick(even_b, zero, other)


def spring_image(field, across, down, hold, above, below, rim):
    return [
        springs(
            field[c], across[...], down[...], hold[...], above[c : c + 1], below[c : c + 1], rim
        )
        for c in range(2)
    ]


def early_kernel(flags, field_ref, across, down, hold, up, *refs):
    edge_refs, (base, rim_ref, next_lanes, next_blend) = refs[:-4], refs[-4:]
    rows, cols = across.shape
    field = [field_ref[0], field_ref[1]]
    above, below = halves(flags, edge_refs)
    image = spring_image(field, across, down, hold, above, below, above[2:3, :])
    for c in range(2):
        base[c] = image[c]
    rim_ref[...] = above[2:3, :]
    hi, lo = hi_lo(tile_of(up, 2).astype(jnp.int32), rows, cols)
    store_lanes(lo, next_lanes)
    for side in range(2):
        next_blend[side] = blend(hi, next_blend.shape[1], tile_of(up, 3 + side), tile_of(up, 5 + side))


def ahead_kernel(next_lanes, next_blend, next_field, out, left):
    load_left([next_field[0], next_field[1]], left, 2)
    out[...] = interpolated(left, next_lanes, next_blend)


def send_on(even, even_b, two, field, own_tables, prev_tables, left, local_ref, send0, send1, *edges):
    own_lanes, own_high = own_tables
    prev_lanes, prev_blend = prev_tables
    load_left(field, left, 2)
    own = looked_up(left, own_lanes, own_high)
    mid = interpolated(left, prev_lanes, prev_blend)
    local_ref[0] = own
    local_ref[1] = mid
    send0[...] = pick(even, own, mid)
    send1[...] = pick(even, mid, own)
    messages = edges_of(lambda c, r: field[c][r : r + 1, :], field[0].shape[0], even_b, two)
    for message, edge in zip(messages, edges):
        edge[...] = message


def stepped(field_ref, image):
    return [GAIN * image[c] - SHIFT * field_ref[c] for c in range(2)]


def first_kernel(
    two, flags, field_ref, base, up, own_lanes, own_high, got_next, up0, up1, *refs
):
    refs, left = refs[:-1], refs[-1]
    out, local_ref, send0, send1, *edges = refs[:-5]
    prev_weights, prev_lanes, prev_high, prev_below, prev_blend = refs[-5:]
    even, even_b = mark(flags, 0), mark(flags, 1)
    rows, cols = field_ref.shape[1:]
    size = own_high.shape[0]
    got_up = pick(even, up1[...], up0[...])
    weights = [tile_of(got_up, 3 + q) * flags[2] for q in range(4)]
    for q in range(4):
        prev_weights[q] = weights[q]
    hi, lo = hi_lo(tile_of(got_up, 2).astype(jnp.int32), rows, cols)
    store_lanes(lo, prev_lanes)
    prev_high[...] = one_hot(hi, size).astype(F32)
    prev_below[...] = one_hot(hi, size, 1).astype(F32)
    for side in range(2):
        prev_blend[side] = blend(hi, size, weights[side], weights[2 + side])
    load_left([field_ref[0], field_ref[1]], left, 2)
    mid = interpolated(left, prev_lanes, prev_blend)
    own = [tile_of(up, c) for c in range(2)]
    got_prev = [tile_of(got_up, c) for c in range(2)]
    live = flags[3]
    pulled = spread_own_apart([live * (own[c] - got_next[c]) for c in range(2)], own_lanes, own_high, rows)
    error = [mid[c] - got_prev[c] for c in range(2)]
    pushed = spread_corners(error, weights, prev_lanes, prev_high, prev_below, rows)
    after = stepped(field_ref, [base[c] + pulled[c] + pushed[c] for c in range(2)])
    for c in range(2):
        out[c] = after[c]
    send_on(
        even,
        even_b,
        two,
        after,
        (own_lanes, own_high),
        (prev_lanes, prev_blend),
        left,
        local_ref,
        send0,
        send1,
        *edges,
    )


def moment_scale(slots):
    bound = GAIN * (8 * 3.0 + 0.2 + 4 * slots) + SHIFT
    return 0.5 ** math.ceil(2.5 * math.log2(bound))


def moments_of(pairs, scale, start=0):
    lane = lax.broadcasted_iota(jnp.int32, (1, LANES), 1)
    total = jnp.zeros((1, LANES), F32)
    for i, (u, w) in enumerate(pairs):
        s = (u[0] * scale) * (w[0] * scale) + (u[1] * scale) * (w[1] * scale)
        s = jnp.sum(jnp.sum(s, axis=0, keepdims=True), axis=1, keepdims=True)
        total = total + jnp.where(lane == start + i, s, 0.0)
    return total


def between_kernel(last, n_edges, scale, flags, field_ref, across, down, hold, rim, *refs):
    refs = list(refs)
    edge_refs = [refs.pop(0) for _ in range(n_edges)]
    earlier = [refs.pop(0) for _ in range(ITERS - 1)] if last else []
    field = [field_ref[0], field_ref[1]]
    above, below = halves(flags, edge_refs)
    image = spring_image(field, across, down, hold, above, below, rim[...])
    base = refs.pop(0)
    for c in range(2):
        base[c] = image[c]
    if last:
        basis = [(ref[0], ref[1]) for ref in earlier] + [field, image]
        refs.pop(0)[...] = moments_of(
            [(basis[i // 2], basis[i - i // 2]) for i in range(2 * ITERS)], scale
        )


def errors_of(flags, local, got0, got1):
    even, live = mark(flags, 0), flags[3]
    got_next = pick(even, got0[...], got1[...])
    got_prev = pick(even, got1[...], got0[...])
    return (
        [live * (local[0, c] - got_next[c]) for c in range(2)],
        [local[1, c] - got_prev[c] for c in range(2)],
    )


def sum_kernel(scale, flags, partial, local, got0, got1, sums):
    own, prev = errors_of(flags, local, got0, got1)
    pairs = [(own[c], local[0, c]) for c in range(2)] + [(prev[c], local[1, c]) for c in range(2)]
    s = sum((a * scale) * (b * scale) for a, b in pairs)
    s = jnp.sum(jnp.sum(s, axis=0, keepdims=True), axis=1, keepdims=True)
    lane = lax.broadcasted_iota(jnp.int32, (1, LANES), 1)
    at = 2 * ITERS - 1
    before = jnp.sum(jnp.where(lane == at - 1, partial[...], 0.0), axis=1, keepdims=True)
    total = jnp.where(lane == at, GAIN * (partial[...] + s) - SHIFT * before, partial[...])
    sums[...] = jnp.broadcast_to(total, sums.shape)


def step_kernel(
    flags,
    field_ref,
    base,
    own_lanes,
    own_high,
    prev_weights,
    prev_lanes,
    prev_high,
    prev_below,
    prev_blend,
    local,
    got0,
    got1,
    out,
):
    rows = field_ref.shape[1]
    error, error_prev = errors_of(flags, local, got0, got1)
    pulled = spread_own(error, own_lanes, own_high, rows)
    weights = [prev_weights[q] for q in range(4)]
    pushed = spread_corners(error_prev, weights, prev_lanes, prev_high, prev_below, rows)
    after = stepped(field_ref, [base[c] + pulled[c] + pushed[c] for c in range(2)])
    for c in range(2):
        out[c] = after[c]


def send_kernel(two, flags, field_ref, own_lanes, own_high, prev_lanes, prev_blend, *refs):
    messages, left = refs[:-1], refs[-1]
    send_on(
        mark(flags, 0),
        mark(flags, 1),
        two,
        [field_ref[0], field_ref[1]],
        (own_lanes, own_high),
        (prev_lanes, prev_blend),
        left,
        *messages,
    )


def conjugate(moments):
    def apply(p):
        shifted = [None] + p
        return [
            (SHIFT * p[k] if k < len(p) else 0.0) * (1.0 / GAIN)
            + ((1.0 / GAIN) * shifted[k] if k else 0.0)
            for k in range(len(p) + 1)
        ]

    def product(p, q):
        return sum(p[i] * q[j] * moments[i + j] for i in range(len(p)) for j in range(len(q)))

    def plus(p, factor, q):
        size = max(len(p), len(q))
        pad = lambda a: a + [None] * (size - len(a))
        out = []
        for a, b in zip(pad(p), pad(q)):
            out.append(factor * b if a is None else a if b is None else a + factor * b)
        return out

    one = jnp.ones_like(moments[0])
    solution_field, residual, direction = [], [one], [one]
    norm_now = moments[0]
    for step in range(ITERS):
        image = apply(direction)
        alpha = norm_now / product(direction, image)
        solution_field = plus(solution_field, alpha, direction)
        residual = plus(residual, -alpha, image)
        if step + 1 < ITERS:
            norm_next = product(residual, residual)
            direction = plus(residual, norm_next / norm_now, direction)
            norm_now = norm_next
    return solution_field, residual


def finish_kernel(sums, *refs):
    basis, (solution_ref, residual_ref) = refs[: ITERS + 1], refs[ITERS + 1 :]
    total = jnp.sum(sums[...], axis=0, keepdims=True)
    lane = lax.broadcasted_iota(jnp.int32, (1, LANES), 1)
    moments = [
        jnp.sum(jnp.where(lane == i, total, 0.0), axis=1, keepdims=True) for i in range(2 * ITERS)
    ]
    solution_field, residual = conjugate(moments)
    for c in range(2):
        values = [ref[c] for ref in basis]
        solution_ref[c] = sum(a * v for a, v in zip(solution_field, values))
        residual_ref[c] = sum(a * v for a, v in zip(residual, values))


VMEM = pl.BlockSpec(memory_space=pltpu.VMEM)
SMEM = pl.BlockSpec(memory_space=pltpu.SMEM)
HBM = pl.BlockSpec(memory_space=pltpu.HBM)


def call(kernel, in_specs, shapes, scratch=()):
    shapes = [s if isinstance(s, jax.ShapeDtypeStruct) else jax.ShapeDtypeStruct(s, F32) for s in shapes]
    return pl.pallas_call(
        kernel,
        in_specs=in_specs,
        out_specs=[VMEM] * len(shapes),
        out_shape=shapes,
        scratch_shapes=list(scratch),
        compiler_params=pltpu.CompilerParams(vmem_limit_bytes=48 * 1024 * 1024),
    )


def body(
    right_side,
    stiff_across,
    stiff_down,
    anchor,
    source_node,
    target_cell,
    corner_weight,
    block_count,
):
    rows, cols = stiff_across.shape[1:]
    rhs = right_side[:, 0]
    across, down, hold = stiff_across[0], stiff_down[0], anchor[0]
    slots = source_node.shape[2]
    nb = slots // LANES
    source = source_node.reshape(nb, LANES)
    target = target_cell.reshape(nb, LANES)
    weights = corner_weight.reshape(4, nb, LANES)
    n_gz, n_xy = lax.axis_size("gz"), lax.axis_size("xy")
    two = n_xy > 2
    n_edges = 2 if two else 1

    def exchange(to0, to1, edges):
        got1 = swapped_sections(to1, 1)
        got0 = swapped_sections(to0, 0)
        got_edges = []
        for i, edge in enumerate(edges):
            got_edges.append(swapped(edge, "xy", i))
        return got0, got1, got_edges

    field_shape = (2, rows, cols)
    message = (2, nb, LANES)
    scale = moment_scale(slots)
    size = rows * cols // WIDE
    common = [field_shape, (2,) + message, message, message] + [(2, cols)] * n_edges
    table = lambda *shape: jax.ShapeDtypeStruct(shape, BF16)
    left = lambda sides: pltpu.VMEM((4 * sides * size, WIDE), BF16)
    lanes, mask, blends = (WIDE, slots), (size, slots), (2, size, slots)
    run = lambda kernel, shapes, scratch, *args: call(kernel, [VMEM] * len(args), shapes, scratch)(*args)
    next_field = lax.ppermute(rhs, "gz", [(i, (i - 1) % n_gz) for i in range(n_gz)])
    in_hbm = lambda *arrays: [pltpu.with_memory_space_constraint(a, pltpu.HBM) for a in arrays]
    grid = (rows, cols)
    rhs, across, down, hold, up, marks, own_lanes, own_high, *edges = call(
        functools.partial(prepare_kernel, two),
        [SMEM] + [HBM] * 7,
        [field_shape, grid, grid, grid, (nb, 7 * LANES), (4, nb, LANES), table(*lanes), mask]
        + [(4, cols)] * n_edges,
        [
            left(1),
            pltpu.VMEM((2, nb, LANES), jnp.int32),
            pltpu.VMEM((4, nb, LANES), F32),
            pltpu.SemaphoreType.DMA((7,)),
        ],
    )(block_count, *in_hbm(rhs, across, down, hold, source, target, weights))
    stiff = (across, down, hold)
    basis = [rhs]
    up1 = swapped_sections(up, 1)
    up0 = swapped_sections(up, 0)
    got_edges = []
    for i, edge in enumerate(edges):
        got_edges.append(swapped(edge, "xy", i))
    base, rim, next_lanes, next_blend = run(
        early_kernel, [field_shape, (1, cols), table(*lanes), blends], [], *(marks, rhs, *stiff, up, *got_edges)
    )
    (got_next,) = run(ahead_kernel, [message], [left(2)], next_lanes, next_blend, next_field)
    field, local, to0, to1, *rest = run(
        functools.partial(first_kernel, two),
        common + [(4, nb, LANES), table(*lanes), mask, mask, blends],
        [left(2)],
        *(marks, rhs, base, up, own_lanes, own_high, got_next, up0, up1),
    )
    edges, prev = rest[:n_edges], rest[n_edges:]

    for step in range(1, ITERS):
        last = step == ITERS - 1
        got0, got1, got_edges = exchange(to0, to1, edges)
        base, *partial = run(
            functools.partial(between_kernel, last, n_edges, scale),
            [field_shape] + ([(1, LANES)] if last else []),
            [],
            *(marks, field, *stiff, rim, *got_edges, *(basis if last else [])),
        )
        if last:
            (sums,) = run(
                functools.partial(sum_kernel, scale),
                [(n_gz * n_xy, LANES)],
                [],
                marks, *partial,
                local,
                got0,
                got1,
            )
            sums = lax.all_to_all(sums.reshape(n_gz * n_xy, 1, LANES), ("gz", "xy"), 0, 0)
            sums = sums.reshape(n_gz * n_xy, LANES)
        (field_next,) = run(
            step_kernel, [field_shape], [], *(marks, field, base, own_lanes, own_high, *prev, local, got0, got1)
        )
        basis.append(field)
        field = field_next
        if not last:
            local, to0, to1, *edges = run(
                functools.partial(send_kernel, two),
                common[1:],
                [left(2)],
                *(marks, field, own_lanes, own_high, prev[1], prev[4]),
            )
    basis.append(field)
    solution_field, residual = call(finish_kernel, [VMEM] * (1 + len(basis)), [field_shape] * 2)(sums, *basis)
    return solution_field[:, None], residual[:, None]


def solution(mesh):
    in_specs = (
        P(None, "gz", "xy", None),
        P("gz", "xy", None),
        P("gz", "xy", None),
        P("gz", "xy", None),
        P("gz", "xy", None),
        P("gz", "xy", None),
        P(None, "gz", "xy", None),
        P("gz", "xy"),
    )
    out_specs = (P(None, "gz", "xy", None), P(None, "gz", "xy", None))
    return jax.shard_map(body, mesh=mesh, in_specs=in_specs, out_specs=out_specs, check_vma=False)
```
